16 devices in a mesh: data: 16 (over z, y, x, core).
Axes of the slice: x: 2, y: 2, z: 2, core: 2. Of those that a mesh axis runs over, the one named last changes fastest.
Arguments:
- x_in: bfloat16 [384, 64, 1280], P('data')
- g_out: bfloat16 [384, 64, 1280], P('data')
- step_emb: bfloat16 [2, 1280], replicated
- w_q: bfloat16 [1280, 20, 64], replicated
- w_k: bfloat16 [1280, 20, 64], replicated
- w_v: bfloat16 [1280, 20, 64], replicated
- w_o: bfloat16 [20, 64, 1280], replicated
- w_up: bfloat16 [1280, 5120], replicated
- w_down: bfloat16 [5120, 1280], replicated
Outputs:
- output 1: float32 [1280, 20, 64], replicated
- output 2: float32 [1280, 20, 64], replicated
- output 3: float32 [1280, 20, 64], replicated
- output 4: float32 [20, 64, 1280], replicated
- output 5: float32 [1280, 5120], replicated
- output 6: float32 [5120, 1280], replicated
- output 7: bfloat16 [384, 64, 1280], P('data')
All inputs are finite; a program needn't handle non-finite values.
Results may differ from the reference program's by a relative error of at most 0.02.
Values are sent between devices in bfloat16 or wider.
A program may use at most 1 GiB of HBM per device.

```python
import math
import functools
import jax
import jax.numpy as jnp
from jax import lax

D = 1280
FF = 5120
HEADS = 20
SEQ = 64
LAYERS = 2
BATCH = 384
HEAD = D // HEADS
NORM_EPS = 1e-6


def setup_inputs(seed: int = 0) -> dict:
    sub_keys = jax.random.split(jax.random.key(seed), 9)
    out_gain = 2.0 / math.sqrt(LAYERS)
    x_in = jax.random.normal(sub_keys[0], (BATCH, SEQ, D), jnp.float32)
    g_out = jax.random.normal(sub_keys[1], (BATCH, SEQ, D), jnp.float32)
    step_emb = jax.random.normal(sub_keys[2], (LAYERS, D), jnp.float32) / math.sqrt(LAYERS)
    w_q = jax.random.normal(sub_keys[3], (D, HEADS, HEAD), jnp.float32) * D ** -0.5
    w_k = jax.random.normal(sub_keys[4], (D, HEADS, HEAD), jnp.float32) * D ** -0.5
    w_v = jax.random.normal(sub_keys[5], (D, HEADS, HEAD), jnp.float32) * D ** -0.5
    w_o = jax.random.normal(sub_keys[6], (HEADS, HEAD, D), jnp.float32) * (D ** -0.5 * out_gain)
    w_up = jax.random.normal(sub_keys[7], (D, FF), jnp.float32) * D ** -0.5
    w_down = jax.random.normal(sub_keys[8], (FF, D), jnp.float32) * (FF ** -0.5 * out_gain)
    return {
        'x_in': x_in.astype(jnp.bfloat16),
        'g_out': g_out.astype(jnp.bfloat16),
        'step_emb': step_emb.astype(jnp.bfloat16),
        'w_q': w_q.astype(jnp.bfloat16),
        'w_k': w_k.astype(jnp.bfloat16),
        'w_v': w_v.astype(jnp.bfloat16),
        'w_o': w_o.astype(jnp.bfloat16),
        'w_up': w_up.astype(jnp.bfloat16),
        'w_down': w_down.astype(jnp.bfloat16),
    }


def rms_norm(x_val):
    x_f32 = x_val.astype(jnp.float32)
    return (x_f32 * lax.rsqrt(jnp.mean(x_f32 * x_f32, axis=-1, keepdims=True) + NORM_EPS)).astype(jnp.bfloat16)


def shared_block(weight_set, x_prev, step_vec):
    w_q, w_k, w_v, w_o, w_up, w_down = weight_set
    x_cur = x_prev + step_vec
    u_norm = rms_norm(x_cur).astype(jnp.float32)
    q_heads = jnp.einsum('sd,dhe->she', u_norm, w_q).astype(jnp.bfloat16)
    k_heads = jnp.einsum('sd,dhe->she', u_norm, w_k).astype(jnp.bfloat16)
    v_heads = jnp.einsum('sd,dhe->she', u_norm, w_v).astype(jnp.bfloat16)
    scores = jnp.einsum('qhe,khe->hqk', q_heads.astype(jnp.float32), k_heads.astype(jnp.float32)).astype(jnp.bfloat16)
    prob_mat = jax.nn.softmax(scores.astype(jnp.float32) * HEAD ** -0.5, axis=-1).astype(jnp.bfloat16)
    mix_heads = jnp.einsum('hqk,khe->qhe', prob_mat.astype(jnp.float32), v_heads.astype(jnp.float32)).astype(jnp.bfloat16)
    attn_out = jnp.einsum('qhe,hed->qd', mix_heads.astype(jnp.float32), w_o).astype(jnp.bfloat16)
    h_mid = x_cur + attn_out
    m_norm = rms_norm(h_mid).astype(jnp.float32)
    z_up = jnp.dot(m_norm, w_up, preferred_element_type=jnp.float32).astype(jnp.bfloat16)
    g_act = jax.nn.gelu(z_up.astype(jnp.float32), approximate=True).astype(jnp.bfloat16)
    y_down = jnp.dot(g_act.astype(jnp.float32), w_down, preferred_element_type=jnp.float32).astype(jnp.bfloat16)
    return h_mid + y_down


def run_stack(weight_set, x_seq, step_emb):
    def layer_step(x_cur, step_vec):
        return jax.checkpoint(shared_block)(weight_set, x_cur, step_vec), None
    x_out, unused = lax.scan(layer_step, x_seq, step_emb)
    return x_out


def reference(x_in, g_out, step_emb, w_q, w_k, w_v, w_o, w_up, w_down):
    weight_set = tuple(w.astype(jnp.float32) for w in (w_q, w_k, w_v, w_o, w_up, w_down))

    def seq_grads(grad_acc, seq_pair):
        x_seq, g_seq = seq_pair
        x_out, pull_back = jax.vjp(functools.partial(run_stack, step_emb=step_emb), weight_set, x_seq)
        d_weights, d_x = pull_back(g_seq)
        return tuple(a + b for a, b in zip(grad_acc, d_weights)), d_x

    zero_acc = tuple(jnp.zeros_like(w) for w in weight_set)
    grad_sums, grad_x = lax.scan(seq_grads, zero_acc, (x_in, g_out))
    return (grad_sums[0], grad_sums[1], grad_sums[2], grad_sums[3], grad_sums[4], grad_sums[5], grad_x)
```

```python
import jax
import jax.numpy as jnp
from jax import lax
from jax.sharding import PartitionSpec as P
import functools

NORM_EPS = 1e-6


def rms_norm(x_val):
    x_f32 = x_val.astype(jnp.float32)
    return (x_f32 * lax.rsqrt(jnp.mean(x_f32 * x_f32, axis=-1, keepdims=True) + NORM_EPS)).astype(jnp.bfloat16)


def gelu_act(z_val):
    return jax.nn.gelu(z_val.astype(jnp.float32), approximate=True).astype(jnp.bfloat16)


def attn_probs(scores, attn_scale):
    return jax.nn.softmax(scores.astype(jnp.float32) * attn_scale, axis=-1).astype(jnp.bfloat16)


def mm(spec, a, b):
    return jnp.einsum(spec, a, b, preferred_element_type=jnp.float32).astype(jnp.bfloat16)


def layer_fwd(x_prev, step_vec, weights, scale):
    w_q, w_k, w_v, w_o, w_up, w_down = weights
    x_cur = x_prev + step_vec
    u = rms_norm(x_cur)
    q, k, v = (mm('bsd,dhe->bhse', u, w) for w in (w_q, w_k, w_v))
    scores = mm('bhqe,bhke->bhqk', q, k)
    prob = attn_probs(scores, scale)
    mix = mm('bhqk,bhke->bhqe', prob, v)
    h = x_cur + mm('bhqe,hed->bqd', mix, w_o)
    z = mm('bsd,df->bsf', rms_norm(h), w_up)
    y = mm('bsf,fd->bsd', gelu_act(z), w_down)
    return h + y, (x_cur, q, k, v, scores, mix, h, z)


def solution(mesh):
    batch_spec = P('data', None, None)

    def per_device(x_loc, g_loc, step_emb, w_q, w_k, w_v, w_o, w_up, w_down):
        scale = w_q.shape[2] ** -0.5
        weights = (w_q, w_k, w_v, w_o, w_up, w_down)
        n_layers = step_emb.shape[0]
        x, saved = x_loc, []
        for l in range(n_layers):
            x, s = layer_fwd(x, step_emb[l], weights, scale)
            saved.append(s)
        d_out = g_loc
        acts = {k: [] for k in ('down', 'up', 'o', 'q', 'k', 'v')}
        for l in reversed(range(n_layers)):
            x_cur, q, k, v, scores, mix, h, z = saved[l]
            g_act, gelu_pull = jax.vjp(gelu_act, z)
            acts['down'].append((g_act, d_out))
            (d_up,) = gelu_pull(mm('bsd,fd->bsf', d_out, w_down))
            m, pull_h = jax.vjp(rms_norm, h)
            acts['up'].append((m, d_up))
            (d_h,) = pull_h(mm('bsf,df->bsd', d_up, w_up))
            d_mid = d_out + d_h
            acts['o'].append((mix, d_mid))
            d_mix = mm('bqd,hed->bhqe', d_mid, w_o)
            prob, prob_pull = jax.vjp(functools.partial(attn_probs, attn_scale=scale), scores)
            d_v = mm('bhqk,bhqe->bhke', prob, d_mix)
            (d_s,) = prob_pull(mm('bhqe,bhke->bhqk', d_mix, v))
            d_q = mm('bhqk,bhke->bhqe', d_s, k)
            d_k = mm('bhqk,bhqe->bhke', d_s, q)
            u, pull_x = jax.vjp(rms_norm, x_cur)
            for n, d in (('q', d_q), ('k', d_k), ('v', d_v)):
                acts[n].append((u, d))
            d_u = (jnp.einsum('bhse,dhe->bsd', d_q, w_q, preferred_element_type=jnp.float32)
                   + jnp.einsum('bhse,dhe->bsd', d_k, w_k, preferred_element_type=jnp.float32)
                   + jnp.einsum('bhse,dhe->bsd', d_v, w_v, preferred_element_type=jnp.float32))
            (d_x,) = pull_x(d_u.astype(jnp.bfloat16))
            d_out = d_mid + d_x

        def wgrad(spec, pairs):
            return sum(jnp.einsum(spec, a, b, preferred_element_type=jnp.float32) for a, b in pairs)

        def reduce(g):
            flat = g.reshape(-1, g.shape[-1])
            part = lax.psum_scatter(flat, 'data', scatter_dimension=0, tiled=True)
            return lax.all_gather(part, 'data', axis=0, tiled=True).reshape(g.shape)

        grad_down = reduce(wgrad('bsf,bsd->fd', acts['down']))
        grad_up = reduce(wgrad('bsd,bsf->df', acts['up']))
        grad_o = reduce(wgrad('bhse,bsd->hed', acts['o']))
        gq, gk, gv = (reduce(wgrad('bsd,bhse->hed', acts[n])).transpose(2, 0, 1) for n in 'qkv')
        return gq, gk, gv, grad_o, grad_up, grad_down, d_out

    return jax.shard_map(per_device, mesh=mesh, in_specs=(batch_spec, batch_spec, P(), P(), P(), P(), P(), P(), P()), out_specs=(P(), P(), P(), P(), P(), P(), batch_spec), check_vma=False)
```

```python
import functools
import math

import jax
import jax.numpy as jnp
from jax import lax
from jax.experimental import pallas as pl
from jax.experimental.pallas import tpu as pltpu
from jax.sharding import PartitionSpec as P


NORM_EPS = 1e-6
GELU_C = math.sqrt(2.0 / math.pi)
GELU_A = 0.044715
BF16 = jnp.bfloat16
F32 = jnp.float32
VMEM_LIMIT = 60 * 1024 * 1024

NN = (((1,), (0,)), ((), ()))
NT = (((1,), (1,)), ((), ()))
TN = (((0,), (0,)), ((), ()))
MESH = pl.DeviceIdType.MESH


def dot(a, b, dims=NN):
    return lax.dot_general(a, b, dims, preferred_element_type=F32)


def rms_scale(x_f32):
    return lax.rsqrt(jnp.mean(x_f32 * x_f32, axis=-1, keepdims=True) + NORM_EPS)


def rms_pull(x_bf16, d_bf16):
    x = x_bf16.astype(F32)
    d = d_bf16.astype(F32)
    r = rms_scale(x)
    dot_dx = jnp.mean(d * x, axis=-1, keepdims=True)
    return (d * r - x * (r * r * r * dot_dx)).astype(BF16)


def gelu_tanh(z):
    return jnp.tanh(GELU_C * (z + GELU_A * (z * z * z)))


def gelu_slope(z):
    t = gelu_tanh(z)
    return 0.5 * (1.0 + t) + (0.5 * z) * ((1.0 - t * t) * (GELU_C * (1.0 + (3.0 * GELU_A) * (z * z))))


def block_diag(a, mask):
    return jnp.concatenate([a, a, a, a], axis=0) * mask


def diag_blocks(full, seq, lane_lo):
    left = jnp.where(lane_lo, full[0:seq, 0:128], full[seq:2 * seq, 0:128])
    right = jnp.where(lane_lo, full[2 * seq:3 * seq, 128:256], full[3 * seq:4 * seq, 128:256])
    return jnp.concatenate([left, right], axis=1)


def softmax_t(scores_t, scale):
    s = scores_t * scale
    e = jnp.exp(s - jnp.max(s, axis=0, keepdims=True))
    return e / jnp.sum(e, axis=0, keepdims=True)


def in_chunks(n, body, rows=32):
    def step(i, _):
        body(pl.ds(pl.multiple_of(i * rows, rows), rows))
        return 0

    lax.fori_loop(0, n // rows, step, 0, unroll=2)


def attn_fwd_kernel(seq, scale, x_ref, e_ref, wq_ref, wk_ref, wv_ref, wo_ref, mask_ref,
                    xc_ref, u_ref, q_ref, k_ref, v_ref, mix_ref, h_ref, m_ref, mt_ref):
    def enter(rows):
        x = (x_ref[rows, :].astype(F32) + e_ref[...].astype(F32)).astype(BF16)
        xc_ref[rows, :] = x
        x_f32 = x.astype(F32)
        u_ref[rows, :] = (x_f32 * rms_scale(x_f32)).astype(BF16)

    in_chunks(x_ref.shape[0], enter)
    for w_ref, o_ref in ((wq_ref, q_ref), (wk_ref, k_ref), (wv_ref, v_ref)):
        o_ref[...] = dot(u_ref[...], w_ref[...], NT).astype(BF16)

    n_groups = x_ref.shape[1] // 256
    lane_lo = lax.broadcasted_iota(jnp.int32, (seq, 128), 1) < 64

    def one_seq(s, _):
        rows = pl.ds(pl.multiple_of(s * seq, seq), seq)
        cols = [pl.ds(g * 256, 256) for g in range(n_groups)]
        mask = mask_ref[...]
        st = [dot(k_ref[rows, c], block_diag(q_ref[rows, c], mask), NT).astype(BF16).astype(F32) for c in cols]
        pb = [softmax_t(t, scale).astype(BF16) for t in st]
        for c, p in zip(cols, pb):
            mix_ref[rows, c] = diag_blocks(dot(p, v_ref[rows, c], TN), seq, lane_lo).astype(BF16)
        return 0

    lax.fori_loop(0, x_ref.shape[0] // seq, one_seq, 0, unroll=2)
    h_ref[...] = dot(mix_ref[...], wo_ref[...]).astype(BF16)

    def leave(rows):
        h = (xc_ref[rows, :].astype(F32) + h_ref[rows, :].astype(F32)).astype(BF16)
        h_ref[rows, :] = h
        h_f32 = h.astype(F32)
        m_ref[rows, :] = (h_f32 * rms_scale(h_f32)).astype(BF16)

    in_chunks(x_ref.shape[0], leave)
    mt_ref[...] = m_ref[...].T


def attn_bwd_kernel(seq, scale, dmid_ref, q_ref, k_ref, v_ref, xc_ref, wq_ref, wk_ref, wv_ref, wo_ref, mask_ref,
                    dq_ref, dk_ref, dv_ref, dprev_ref, dmix_ref):
    dmix_ref[...] = dot(dmid_ref[...], wo_ref[...], NT).astype(BF16)
    n_groups = xc_ref.shape[1] // 256
    lane_lo = lax.broadcasted_iota(jnp.int32, (seq, 128), 1) < 64

    def one_seq(s, _):
        rows = pl.ds(pl.multiple_of(s * seq, seq), seq)
        cols = [pl.ds(g * 256, 256) for g in range(n_groups)]
        mask = mask_ref[...]
        qbd = [block_diag(q_ref[rows, c], mask) for c in cols]
        dbd = [block_diag(dmix_ref[rows, c], mask) for c in cols]
        st = [dot(k_ref[rows, c], t, NT).astype(BF16).astype(F32) for c, t in zip(cols, qbd)]
        dp = [dot(v_ref[rows, c], t, NT).astype(BF16).astype(F32) for c, t in zip(cols, dbd)]
        p = [softmax_t(t, scale) for t in st]
        for c, a, t in zip(cols, p, dbd):
            dv_ref[rows, c] = dot(a.astype(BF16), t).astype(BF16)
        ds = [((a * (t - jnp.sum(a * t, axis=0, keepdims=True))) * scale).astype(BF16) for a, t in zip(p, dp)]
        for c, a, t in zip(cols, ds, qbd):
            dk_ref[rows, c] = dot(a, t).astype(BF16)
            dq_ref[rows, c] = diag_blocks(dot(a, k_ref[rows, c], TN), seq, lane_lo).astype(BF16)
        return 0

    lax.fori_loop(0, xc_ref.shape[0] // seq, one_seq, 0, unroll=2)
    du = dot(dq_ref[...], wq_ref[...]) + dot(dk_ref[...], wk_ref[...]) + dot(dv_ref[...], wv_ref[...])
    dmix_ref[...] = du.astype(BF16)

    def leave(rows):
        dx = rms_pull(xc_ref[rows, :], dmix_ref[rows, :])
        dprev_ref[rows, :] = (dmid_ref[rows, :].astype(F32) + dx.astype(F32)).astype(BF16)

    in_chunks(xc_ref.shape[0], leave)


def mlp_fwd_kernel(sub, m_ref, wup_ref, wdown_ref, h_ref, z_ref, g_ref, y_ref, acc_ref):
    step = pl.program_id(0)

    @pl.when(step == 0)
    def _():
        acc_ref[...] = jnp.zeros_like(acc_ref)

    for r in range(m_ref.shape[0] // sub):
        rows = pl.ds(r * sub, sub)
        zb = dot(m_ref[rows, :], wup_ref[...]).astype(BF16)
        z_ref[rows, :] = zb
        z = zb.astype(F32)
        g = ((0.5 * z) * (1.0 + gelu_tanh(z))).astype(BF16)
        g_ref[rows, :] = g
        acc_ref[rows, :] += dot(g, wdown_ref[...])

    @pl.when(step == pl.num_programs(0) - 1)
    def _():
        def finish(rows):
            y = acc_ref[rows, :].astype(BF16)
            y_ref[rows, :] = (h_ref[rows, :].astype(F32) + y.astype(F32)).astype(BF16)

        in_chunks(m_ref.shape[0], finish)


def mlp_bwd_kernel(sub, d_ref, wup_ref, wdown_ref, z_ref, h_ref, dup_ref, dmid_ref, acc_ref):
    step = pl.program_id(0)

    @pl.when(step == 0)
    def _():
        acc_ref[...] = jnp.zeros_like(acc_ref)

    for r in range(d_ref.shape[0] // sub):
        rows = pl.ds(r * sub, sub)
        da = dot(d_ref[rows, :], wdown_ref[...], NT).astype(BF16).astype(F32)
        du = (da * gelu_slope(z_ref[rows, :].astype(F32))).astype(BF16)
        dup_ref[rows, :] = du
        acc_ref[rows, :] += dot(du, wup_ref[...], NT)

    @pl.when(step == pl.num_programs(0) - 1)
    def _():
        def finish(rows):
            dh = rms_pull(h_ref[rows, :], acc_ref[rows, :].astype(BF16))
            dmid_ref[rows, :] = (d_ref[rows, :].astype(F32) + dh.astype(F32)).astype(BF16)

        in_chunks(d_ref.shape[0], finish)


def params(**kw):
    return pltpu.CompilerParams(dimension_semantics=("arbitrary",), vmem_limit_bytes=VMEM_LIMIT, **kw)


def cost(flops, nbytes, trans=0):
    return pl.CostEstimate(flops=int(flops), bytes_accessed=int(nbytes), transcendentals=int(trans))


def whole(shape):
    return pl.BlockSpec(shape, lambda i: (0,) * len(shape))


def attn_fwd(x, step_vec, wq, wk, wv, wo, mask, seq, scale, tile):
    n, d = x.shape
    row = pl.BlockSpec((tile, d), lambda i: (i, 0))
    return pl.pallas_call(
        functools.partial(attn_fwd_kernel, seq, scale),
        grid=(n // tile,),
        in_specs=[row, whole((1, d))] + [whole(w.shape) for w in (wq, wk, wv, wo, mask)],
        out_specs=[row] * 8 + [pl.BlockSpec((d, tile), lambda i: (0, i))],
        out_shape=[jax.ShapeDtypeStruct((n, d), BF16)] * 8 + [jax.ShapeDtypeStruct((d, n), BF16)],
        compiler_params=params(),
        cost_estimate=cost(8 * n * d * d, 20 * n * d, n * d),
        name="attn_fwd",
    )(x, step_vec, wq, wk, wv, wo, mask)


def attn_bwd(dmid, q, k, v, xc, wq, wk, wv, wo, mask, seq, scale, tile):
    n, d = xc.shape
    row = pl.BlockSpec((tile, d), lambda i: (i, 0))
    return pl.pallas_call(
        functools.partial(attn_bwd_kernel, seq, scale),
        grid=(n // tile,),
        in_specs=[row] * 5 + [whole(w.shape) for w in (wq, wk, wv, wo, mask)],
        out_specs=[row] * 4,
        out_shape=[jax.ShapeDtypeStruct((n, d), BF16)] * 4,
        scratch_shapes=[pltpu.VMEM((tile, d), BF16)],
        compiler_params=params(),
        cost_estimate=cost(8 * n * d * d, 20 * n * d, n * d),
        name="attn_bwd",
    )(dmid, q, k, v, xc, wq, wk, wv, wo, mask)


def mlp_fwd(m, w_up, w_down, h, tile, sub):
    n, d = m.shape
    f = w_up.shape[1]
    col = pl.BlockSpec((n, tile), lambda i: (0, i))
    return pl.pallas_call(
        functools.partial(mlp_fwd_kernel, sub),
        grid=(f // tile,),
        in_specs=[whole((n, d)), pl.BlockSpec((d, tile), lambda i: (0, i)), pl.BlockSpec((tile, d), lambda i: (i, 0)), whole((n, d))],
        out_specs=[col, col, whole((n, d))],
        out_shape=[jax.ShapeDtypeStruct((n, f), BF16)] * 2 + [jax.ShapeDtypeStruct((n, d), BF16)],
        scratch_shapes=[pltpu.VMEM((n, d), F32)],
        compiler_params=params(),
        cost_estimate=cost(4 * n * d * f, 4 * n * f, n * f),
        name="mlp_fwd",
    )(m, w_up, w_down, h)


def mlp_bwd(d_out, w_up, w_down, z, h, tile, sub):
    n, d = d_out.shape
    f = w_up.shape[1]
    col = pl.BlockSpec((n, tile), lambda i: (0, i))
    return pl.pallas_call(
        functools.partial(mlp_bwd_kernel, sub),
        grid=(f // tile,),
        in_specs=[whole((n, d)), pl.BlockSpec((d, tile), lambda i: (0, i)), pl.BlockSpec((tile, d), lambda i: (i, 0)), col, whole((n, d))],
        out_specs=[col, whole((n, d))],
        out_shape=[jax.ShapeDtypeStruct((n, f), BF16), jax.ShapeDtypeStruct((n, d), BF16)],
        scratch_shapes=[pltpu.VMEM((n, d), F32)],
        compiler_params=params(),
        cost_estimate=cost(4 * n * d * f, 4 * n * f, n * f),
        name="mlp_bwd",
    )(d_out, w_up, w_down, z, h)


def peer_of(me, power):
    return me + power * (1 - 2 * ((me // power) % 2))


def enter_barrier(me):
    barrier = pltpu.get_barrier_semaphore()
    for power in (1, 2, 4, 8):
        pl.semaphore_signal(barrier, inc=1, device_id=(peer_of(me, power),), device_id_type=MESH)
    pl.semaphore_wait(barrier, 4)


def stream_scratch(half, width, slots):
    return [pltpu.VMEM((slots, half // k, width), F32) for k in (1, 2, 4, 8)] + [
        pltpu.SemaphoreType.DMA((4, slots)), pltpu.SemaphoreType.DMA((4, slots))]


def reduce_stage(s, j, shift, half, g_ref, out_ref, bufs, me):
    h0, h1, h2, h3, send_sem, recv_sem = bufs
    slots = h0.shape[0]
    slot, g = j % slots, g_ref.at[j % g_ref.shape[0]]
    core = me % 2
    powers, bits = [], []
    for k in range(3):
        r = (j + k + shift) % 3
        powers.append(2 + r + r * r)
        bits.append((me // powers[k]) % 2)
    held = (g, h0.at[slot], h1.at[slot], h2.at[slot], h3.at[slot])
    keep = (half * core,) + tuple((half >> (k + 1)) * bits[k] for k in range(3))
    away = (half * (1 - core),) + tuple((half >> (k + 1)) * (1 - bits[k]) for k in range(3))

    def part(ref, start, size):
        return ref.at[pl.ds(pl.multiple_of(start, 8), size)]

    def copy(k):
        peer = peer_of(me, 1) if k == 0 else peer_of(me, powers[k - 1])
        return pltpu.make_async_remote_copy(
            src_ref=part(held[k], away[k], half >> k), dst_ref=held[k + 1], send_sem=send_sem.at[k, slot],
            recv_sem=recv_sem.at[k, slot], device_id=(peer,), device_id_type=MESH)

    if s > 0:
        before = copy(s - 1)
        before.wait_recv()
        before.wait_send()
        own = held[s - 1][pl.ds(pl.multiple_of(keep[s - 1], 8), half >> (s - 1)), :]
        if s == 4:
            out_ref[0] = held[4][...] + own
        else:
            held[s][...] = held[s][...] + own
    if s < 4:
        copy(s).start()


def reduce_step(i, n, lags, streams, me):
    for stream in streams:
        for s in (4, 3, 2, 1, 0):
            j = i - lags[s]

            @pl.when((j >= 0) & (j < n))
            def _():
                reduce_stage(s, j, *stream, me)


def mlp_grads_kernel(n, lags, sub, d0_ref, d1_ref, m0t_ref, m1t_ref, h_ref, z_ref, g0_ref, g1_ref, dup1_ref, wup_ref, wdown_ref,
                     sd_ref, su_ref, dmid_ref, acc_ref, du_ref, gd_ref, gu_ref, *bufs):
    me = lax.axis_index('data')
    i = pl.program_id(0)

    @pl.when(i == 0)
    def _():
        enter_barrier(me)
        acc_ref[...] = jnp.zeros_like(acc_ref)

    @pl.when(i < n)
    def _():
        for r in range(d0_ref.shape[0] // sub):
            rows = pl.ds(r * sub, sub)
            da = dot(d0_ref[rows, :], wdown_ref[...], NT).astype(BF16).astype(F32)
            du = (da * gelu_slope(z_ref[rows, :].astype(F32))).astype(BF16)
            du_ref[rows, :] = du
            acc_ref[rows, :] += dot(du, wup_ref[...], NT)
        gd_ref[i % 2] = dot(g0_ref[...], d0_ref[...], TN) + dot(g1_ref[...], d1_ref[...], TN)
        gu_ref[i % 2] = dot(m0t_ref[...], du_ref[...]) + dot(m1t_ref[...], dup1_ref[...])

    @pl.when(i == n - 1)
    def _():
        def finish(rows):
            dh = rms_pull(h_ref[rows, :], acc_ref[rows, :].astype(BF16))
            dmid_ref[rows, :] = (d0_ref[rows, :].astype(F32) + dh.astype(F32)).astype(BF16)

        in_chunks(d0_ref.shape[0], finish)

    reduce_step(i, n, lags, ((0, gd_ref.shape[1] // 2, gd_ref, sd_ref, bufs[:6]), (2, gu_ref.shape[1] // 2, gu_ref, su_ref, bufs[6:])), me)


def attn_grads_kernel(n, lags, *refs):
    xs, (u0, u1, m0, m1), out_ref, g_ref, bufs = refs[:8], refs[8:12], refs[12], refs[13], refs[14:]
    me = lax.axis_index('data')
    i = pl.program_id(0)

    @pl.when(i == 0)
    def _():
        enter_barrier(me)

    per = n // 4
    for w in range(4):
        @pl.when((i >= w * per) & (i < (w + 1) * per))
        def _():
            y0, y1 = (u0, u1) if w < 3 else (m0, m1)
            g_ref[i % 4] = dot(xs[2 * w][...], y0[...], TN) + dot(xs[2 * w + 1][...], y1[...], TN)

    reduce_step(i, n, lags, ((0, g_ref.shape[1] // 2, g_ref, out_ref, bufs),), me)


MLP_LAGS, MLP_SLOTS = (0, 1, 3, 4, 5), 6
ATTN_LAGS, ATTN_SLOTS = (0, 2, 4, 6, 8), 8


def kept(shape):
    return pl.BlockSpec(shape, lambda i: (0,) * len(shape), pipeline_mode=pl.Buffered(1))


def mlp_grads(ds, mts, h, z, gs, dup1, w_up, w_down, tile, sub):
    rows, d = h.shape
    n = w_up.shape[1] // tile
    at = lambda i: jnp.minimum(i, n - 1)
    col = pl.BlockSpec((rows, tile), lambda i: (0, at(i)))
    share = lambda i: (jnp.maximum(i - MLP_LAGS[4], 0), 0, 0)
    return pl.pallas_call(
        functools.partial(mlp_grads_kernel, n, MLP_LAGS, sub),
        grid=(n + MLP_LAGS[4],),
        in_specs=[kept((rows, d))] * 2 + [kept((d, rows))] * 2 + [kept((rows, d))] + [col] * 4 + [
            pl.BlockSpec((d, tile), lambda i: (0, at(i))), pl.BlockSpec((tile, d), lambda i: (at(i), 0))],
        out_specs=[pl.BlockSpec((1, tile // 16, d), share), pl.BlockSpec((1, d // 16, tile), share), kept((rows, d))],
        out_shape=[jax.ShapeDtypeStruct((n, tile // 16, d), F32), jax.ShapeDtypeStruct((n, d // 16, tile), F32),
                   jax.ShapeDtypeStruct((rows, d), BF16)],
        scratch_shapes=[pltpu.VMEM((rows, d), F32), pltpu.VMEM((rows, tile), BF16), pltpu.VMEM((2, tile, d), F32),
                        pltpu.VMEM((2, d, tile), F32)] + stream_scratch(tile // 2, d, MLP_SLOTS) + stream_scratch(d // 2, tile, MLP_SLOTS),
        compiler_params=pltpu.CompilerParams(dimension_semantics=("arbitrary",), collective_id=0, has_side_effects=True,
                                             vmem_limit_bytes=63 * 1024 * 1024),
        cost_estimate=cost(12 * rows * d * n * tile, 10 * rows * n * tile),
        name="mlp_grads",
    )(*ds, *mts, h, z, *gs, dup1, w_up, w_down)


def attn_grads(xs, ys, tile):
    rows, d = ys[0].shape
    per = d // tile
    n = 4 * per
    cols = [pl.BlockSpec((rows, tile), lambda i, w=w: (0, jnp.clip(i - w * per, 0, per - 1))) for w in range(4) for _ in range(2)]
    return pl.pallas_call(
        functools.partial(attn_grads_kernel, n, ATTN_LAGS),
        grid=(n + ATTN_LAGS[4],),
        in_specs=cols + [kept((rows, d))] * 4,
        out_specs=pl.BlockSpec((1, tile // 16, d), lambda i: (jnp.maximum(i - ATTN_LAGS[4], 0), 0, 0)),
        out_shape=jax.ShapeDtypeStruct((n, tile // 16, d), F32),
        scratch_shapes=[pltpu.VMEM((4, tile, d), F32)] + stream_scratch(tile // 2, d, ATTN_SLOTS),
        compiler_params=pltpu.CompilerParams(dimension_semantics=("arbitrary",), collective_id=1, has_side_effects=True,
                                             vmem_limit_bytes=VMEM_LIMIT),
        cost_estimate=cost(16 * rows * d * d, 24 * rows * d),
        name="attn_grads",
    )(*[x for pair in xs for x in pair], *ys)


def place_kernel(shift, first, in_ref, out_ref):
    j = pl.program_id(0) + first
    half, piece = out_ref.shape[0] // 2, in_ref.shape[2]
    for v in range(3):
        @pl.when((j + shift) % 3 == v)
        def _():
            for dev in range(16):
                bits = [(dev >> (1 + (v + k) % 3)) & 1 for k in range(3)]
                at = half * (dev & 1) + sum((half >> (k + 1)) * bits[k] for k in range(3))
                out_ref[at:at + piece, :] = in_ref[dev, 0]


def place(shares, shift, first, count, by_cols):
    _, _, piece, width = shares.shape
    high = 16 * piece
    out = (high, width * count) if by_cols else (high * count, width)
    return pl.pallas_call(
        functools.partial(place_kernel, shift, first),
        grid=(count,),
        in_specs=[pl.BlockSpec((16, 1, piece, width), lambda i: (0, i + first, 0, 0))],
        out_specs=pl.BlockSpec((high, width), (lambda i: (0, i)) if by_cols else (lambda i: (i, 0))),
        out_shape=jax.ShapeDtypeStruct(out, F32),
        compiler_params=params(),
        cost_estimate=cost(shares.size // 2, 8 * high * width * count),
        name="place",
    )(shares)


def solution(mesh):
    batch_spec = P('data', None, None)

    def per_device(x_loc, g_loc, step_emb, w_q, w_k, w_v, w_o, w_up, w_down):
        d, n_heads, head = w_q.shape
        scale = head ** -0.5
        n_seq, seq, _ = x_loc.shape
        n = n_seq * seq
        wq, wk, wv = (w.transpose(1, 2, 0).reshape(n_heads * head, d) for w in (w_q, w_k, w_v))
        wo = w_o.reshape(n_heads * head, d)
        head_of = jnp.arange(256) // 64
        mask = (head_of[:, None] == head_of[None, :]).astype(BF16)
        x = x_loc.reshape(n, d)
        saved = []
        for l in range(2):
            xc, u, q, k, v, mix, h, m, mt = attn_fwd(x, step_emb[l:l + 1], wq, wk, wv, wo, mask, seq, scale, 512)
            z, g, x = mlp_fwd(m, w_up, w_down, h, 512, 512)
            saved.append((xc, u, q, k, v, mix, h, mt, z, g))
        (_, u0, _, _, _, mix0, h0, mt0, z0, g0), (_, u1, _, _, _, mix1, h1, mt1, z1, g1) = saved

        def attn_back(l, dmid):
            xc, _, q, k, v = saved[l][:5]
            return attn_bwd(dmid, q, k, v, xc, wq, wk, wv, wo, mask, seq, scale, 512)

        do1 = g_loc.reshape(n, d)
        dup1, dmid1 = mlp_bwd(do1, w_up, w_down, z1, h1, 512, 512)
        dq1, dk1, dv1, do0 = attn_back(1, dmid1)
        s_down, s_up, dmid0 = mlp_grads((do0, do1), (mt0, mt1), h0, z0, (g0, g1), dup1, w_up, w_down, 256, 512)
        a_down = lax.all_gather(s_down, 'data')
        a_up = lax.all_gather(s_up, 'data')
        dq0, dk0, dv0, d_out = attn_back(0, dmid0)
        s_attn = attn_grads([(dq0, dq1), (dk0, dk1), (dv0, dv1), (mix0, mix1)], (u0, u1, dmid0, dmid1), 256)
        a_attn = lax.all_gather(s_attn, 'data')
        n_tiles = s_down.shape[0]
        g_down = place(a_down, 0, 0, n_tiles, False)
        g_up = place(a_up, 2, 0, n_tiles, True)
        per = s_attn.shape[0] // 4
        g_q, g_k, g_v, g_o = (place(a_attn, 0, w * per, per, False) for w in range(4))
        heads = lambda a: a.reshape(n_heads, head, d).transpose(2, 0, 1)
        return heads(g_q), heads(g_k), heads(g_v), g_o.reshape(w_o.shape), g_up, g_down, d_out.reshape(x_loc.shape)

    return jax.shard_map(per_device, mesh=mesh, in_specs=(batch_spec, batch_spec, P(), P(), P(), P(), P(), P(), P()), out_specs=(P(), P(), P(), P(), P(), P(), batch_spec), check_vma=False)
```

```python
import functools
import math

import jax
import jax.numpy as jnp
from jax import lax
from jax.experimental import pallas as pl
from jax.experimental.pallas import tpu as pltpu
from jax.sharding import PartitionSpec as P


NORM_EPS = 1e-6
GELU_C = math.sqrt(2.0 / math.pi)
GELU_A = 0.044715
BF16 = jnp.bfloat16
F32 = jnp.float32
VMEM_LIMIT = 60 * 1024 * 1024

NN = (((1,), (0,)), ((), ()))
NT = (((1,), (1,)), ((), ()))
TN = (((0,), (0,)), ((), ()))
MESH = pl.DeviceIdType.MESH


def dot(a, b, dims=NN):
    return lax.dot_general(a, b, dims, preferred_element_type=F32)


def rms_scale(x_f32):
    return lax.rsqrt(jnp.mean(x_f32 * x_f32, axis=-1, keepdims=True) + NORM_EPS)


def rms_pull(x_bf16, d_bf16):
    x = x_bf16.astype(F32)
    d = d_bf16.astype(F32)
    r = rms_scale(x)
    dot_dx = jnp.mean(d * x, axis=-1, keepdims=True)
    return (d * r - x * (r * r * r * dot_dx)).astype(BF16)


def gelu_tanh(z):
    return jnp.tanh(GELU_C * (z + GELU_A * (z * z * z)))


def gelu_slope(z):
    t = gelu_tanh(z)
    return 0.5 * (1.0 + t) + (0.5 * z) * ((1.0 - t * t) * (GELU_C * (1.0 + (3.0 * GELU_A) * (z * z))))


def block_diag(a, mask):
    return jnp.concatenate([a, a, a, a], axis=0) * mask


def diag_blocks(full, seq, lane_lo):
    left = jnp.where(lane_lo, full[0:seq, 0:128], full[seq:2 * seq, 0:128])
    right = jnp.where(lane_lo, full[2 * seq:3 * seq, 128:256], full[3 * seq:4 * seq, 128:256])
    return jnp.concatenate([left, right], axis=1)


def softmax_t(scores_t, scale):
    s = scores_t * scale
    e = jnp.exp(s - jnp.max(s, axis=0, keepdims=True))
    return e / jnp.sum(e, axis=0, keepdims=True)


def in_chunks(n, body, rows=32):
    def step(i, _):
        body(pl.ds(pl.multiple_of(i * rows, rows), rows))
        return 0

    lax.fori_loop(0, n // rows, step, 0, unroll=2)


def loads(refs, bufs, sems):
    return [pltpu.make_async_copy(r, b, sems.at[k]) for k, (r, b) in enumerate(zip(refs, bufs))]


def at_step(step, *actions):
    @pl.when(pl.program_id(0) == step)
    def _():
        for act in actions:
            act()


def attn_fwd_kernel(seq, scale, x_ref, e_ref, mask_ref, wq_hbm, wk_hbm, wv_hbm, wo_hbm,
                    xc_ref, u_ref, q_ref, k_ref, v_ref, mix_ref, h_ref, m_ref, mt_ref, wq_ref, wk_ref, wv_ref, wo_ref, sems):
    load = loads((wq_hbm, wk_hbm, wv_hbm, wo_hbm), (wq_ref, wk_ref, wv_ref, wo_ref), sems)
    at_step(0, *(c.start for c in load))
    n_rows = x_ref.shape[0]
    blocks = [pl.ds(r * (n_rows // 2), n_rows // 2) for r in range(2)]
    at_step(0, *(c.wait for c in load[:3]))
    for rows in blocks:
        x = (x_ref[rows, :].astype(F32) + e_ref[...].astype(F32)).astype(BF16)
        xc_ref[rows, :] = x
        x_f32 = x.astype(F32)
        u_ref[rows, :] = (x_f32 * rms_scale(x_f32)).astype(BF16)
        for w_ref, o_ref in ((wq_ref, q_ref), (wk_ref, k_ref), (wv_ref, v_ref)):
            o_ref[rows, :] = dot(u_ref[rows, :], w_ref[...], NT).astype(BF16)

    n_groups = x_ref.shape[1] // 256
    lane_lo = lax.broadcasted_iota(jnp.int32, (seq, 128), 1) < 64

    def one_seq(s, _):
        rows = pl.ds(pl.multiple_of(s * seq, seq), seq)
        cols = [pl.ds(g * 256, 256) for g in range(n_groups)]
        mask = mask_ref[...]
        st = [dot(k_ref[rows, c], block_diag(q_ref[rows, c], mask), NT).astype(BF16).astype(F32) for c in cols]
        pb = [softmax_t(t, scale).astype(BF16) for t in st]
        for c, p in zip(cols, pb):
            mix_ref[rows, c] = diag_blocks(dot(p, v_ref[rows, c], TN), seq, lane_lo).astype(BF16)
        return 0

    lax.fori_loop(0, x_ref.shape[0] // seq, one_seq, 0, unroll=2)
    at_step(0, load[3].wait)
    for rows in blocks:
        h = (xc_ref[rows, :].astype(F32) + dot(mix_ref[rows, :], wo_ref[...]).astype(BF16).astype(F32)).astype(BF16)
        h_ref[rows, :] = h
        h_f32 = h.astype(F32)
        m_ref[rows, :] = (h_f32 * rms_scale(h_f32)).astype(BF16)
    mt_ref[...] = m_ref[...].T


def attn_bwd_kernel(seq, scale, dmid_ref, q_ref, k_ref, v_ref, xc_ref, mask_ref, wo_hbm, wq_hbm, wk_hbm, wv_hbm,
                    dq_ref, dk_ref, dv_ref, dprev_ref, dmix_ref, wo_ref, wq_ref, wk_ref, wv_ref, sems):
    load = loads((wo_hbm, wq_hbm, wk_hbm, wv_hbm), (wo_ref, wq_ref, wk_ref, wv_ref), sems)
    at_step(0, *(c.start for c in load), load[0].wait)
    dmix_ref[...] = dot(dmid_ref[...], wo_ref[...], NT).astype(BF16)
    n_groups = xc_ref.shape[1] // 256
    lane_lo = lax.broadcasted_iota(jnp.int32, (seq, 128), 1) < 64

    def one_seq(s, _):
        rows = pl.ds(pl.multiple_of(s * seq, seq), seq)
        cols = [pl.ds(g * 256, 256) for g in range(n_groups)]
        mask = mask_ref[...]
        qbd = [block_diag(q_ref[rows, c], mask) for c in cols]
        dbd = [block_diag(dmix_ref[rows, c], mask) for c in cols]
        st = [dot(k_ref[rows, c], t, NT).astype(BF16).astype(F32) for c, t in zip(cols, qbd)]
        dp = [dot(v_ref[rows, c], t, NT).astype(BF16).astype(F32) for c, t in zip(cols, dbd)]
        p = [softmax_t(t, scale) for t in st]
        for c, a, t in zip(cols, p, dbd):
            dv_ref[rows, c] = dot(a.astype(BF16), t).astype(BF16)
        ds = [((a * (t - jnp.sum(a * t, axis=0, keepdims=True))) * scale).astype(BF16) for a, t in zip(p, dp)]
        for c, a, t in zip(cols, ds, qbd):
            dk_ref[rows, c] = dot(a, t).astype(BF16)
            dq_ref[rows, c] = diag_blocks(dot(a, k_ref[rows, c], TN), seq, lane_lo).astype(BF16)
        return 0

    lax.fori_loop(0, xc_ref.shape[0] // seq, one_seq, 0, unroll=2)
    at_step(0, *(c.wait for c in load[1:]))
    n_rows = xc_ref.shape[0]
    for rows in [pl.ds(r * (n_rows // 2), n_rows // 2) for r in range(2)]:
        du = dot(dq_ref[rows, :], wq_ref[...]) + dot(dk_ref[rows, :], wk_ref[...]) + dot(dv_ref[rows, :], wv_ref[...])
        dx = rms_pull(xc_ref[rows, :], du.astype(BF16))
        dprev_ref[rows, :] = (dmid_ref[rows, :].astype(F32) + dx.astype(F32)).astype(BF16)


def mlp_fwd_kernel(sub, m_ref, wup_ref, wdown_ref, h_hbm, z_ref, g_ref, y_ref, acc_ref, h_ref, sem):
    step = pl.program_id(0)
    load = pltpu.make_async_copy(h_hbm, h_ref, sem)
    at_step(0, load.start)

    @pl.when(step == 0)
    def _():
        acc_ref[...] = jnp.zeros_like(acc_ref)

    for r in range(m_ref.shape[0] // sub):
        rows = pl.ds(r * sub, sub)
        zb = dot(m_ref[rows, :], wup_ref[...]).astype(BF16)
        z_ref[rows, :] = zb
        z = zb.astype(F32)
        g = ((0.5 * z) * (1.0 + gelu_tanh(z))).astype(BF16)
        g_ref[rows, :] = g
        acc_ref[rows, :] += dot(g, wdown_ref[...])

    @pl.when(step == pl.num_programs(0) - 1)
    def _():
        load.wait()

        def finish(rows):
            y = acc_ref[rows, :].astype(BF16)
            y_ref[rows, :] = (h_ref[rows, :].astype(F32) + y.astype(F32)).astype(BF16)

        in_chunks(m_ref.shape[0], finish)


def mlp_bwd_kernel(sub, d_ref, wup_ref, wdown_ref, z_ref, h_hbm, dup_ref, dmid_ref, acc_ref, h_ref, sem):
    step = pl.program_id(0)
    load = pltpu.make_async_copy(h_hbm, h_ref, sem)
    at_step(0, load.start)

    @pl.when(step == 0)
    def _():
        acc_ref[...] = jnp.zeros_like(acc_ref)

    for r in range(d_ref.shape[0] // sub):
        rows = pl.ds(r * sub, sub)
        da = dot(d_ref[rows, :], wdown_ref[...], NT).astype(BF16).astype(F32)
        du = (da * gelu_slope(z_ref[rows, :].astype(F32))).astype(BF16)
        dup_ref[rows, :] = du
        acc_ref[rows, :] += dot(du, wup_ref[...], NT)

    @pl.when(step == pl.num_programs(0) - 1)
    def _():
        load.wait()

        def finish(rows):
            dh = rms_pull(h_ref[rows, :], acc_ref[rows, :].astype(BF16))
            dmid_ref[rows, :] = (d_ref[rows, :].astype(F32) + dh.astype(F32)).astype(BF16)

        in_chunks(d_ref.shape[0], finish)


def params(**kw):
    return pltpu.CompilerParams(dimension_semantics=("arbitrary",), vmem_limit_bytes=VMEM_LIMIT, **kw)


def cost(flops, nbytes, trans=0):
    return pl.CostEstimate(flops=int(flops), bytes_accessed=int(nbytes), transcendentals=int(trans))


def whole(shape):
    return pl.BlockSpec(shape, lambda i: (0,) * len(shape))


def attn_fwd(x, step_vec, wq, wk, wv, wo, mask, seq, scale, tile):
    n, d = x.shape
    row = pl.BlockSpec((tile, d), lambda i: (i, 0))
    return pl.pallas_call(
        functools.partial(attn_fwd_kernel, seq, scale),
        grid=(n // tile,),
        in_specs=[row, whole((1, d)), whole(mask.shape)] + [pl.BlockSpec(memory_space=pl.ANY)] * 4,
        out_specs=[row] * 8 + [pl.BlockSpec((d, tile), lambda i: (0, i))],
        out_shape=[jax.ShapeDtypeStruct((n, d), BF16)] * 8 + [jax.ShapeDtypeStruct((d, n), BF16)],
        scratch_shapes=[pltpu.VMEM(w.shape, BF16) for w in (wq, wk, wv, wo)] + [pltpu.SemaphoreType.DMA((4,))],
        compiler_params=params(),
        cost_estimate=cost(8 * n * d * d, 20 * n * d, n * d),
        name="attn_fwd",
    )(x, step_vec, mask, wq, wk, wv, wo)


def attn_bwd(dmid, q, k, v, xc, wq, wk, wv, wo, mask, seq, scale, tile):
    n, d = xc.shape
    row = pl.BlockSpec((tile, d), lambda i: (i, 0))
    return pl.pallas_call(
        functools.partial(attn_bwd_kernel, seq, scale),
        grid=(n // tile,),
        in_specs=[row] * 5 + [whole(mask.shape)] + [pl.BlockSpec(memory_space=pl.ANY)] * 4,
        out_specs=[row] * 4,
        out_shape=[jax.ShapeDtypeStruct((n, d), BF16)] * 4,
        scratch_shapes=[pltpu.VMEM((tile, d), BF16)] + [pltpu.VMEM(w.shape, BF16) for w in (wo, wq, wk, wv)] + [pltpu.SemaphoreType.DMA((4,))],
        compiler_params=params(),
        cost_estimate=cost(8 * n * d * d, 20 * n * d, n * d),
        name="attn_bwd",
    )(dmid, q, k, v, xc, mask, wo, wq, wk, wv)


def mlp_fwd(m, w_up, w_down, h, tile, sub):
    n, d = m.shape
    f = w_up.shape[1]
    col = pl.BlockSpec((n, tile), lambda i: (0, i))
    return pl.pallas_call(
        functools.partial(mlp_fwd_kernel, sub),
        grid=(f // tile,),
        in_specs=[kept((n, d)), pl.BlockSpec((d, tile), lambda i: (0, i)), pl.BlockSpec((tile, d), lambda i: (i, 0)), pl.BlockSpec(memory_space=pl.ANY)],
        out_specs=[col, col, kept((n, d))],
        out_shape=[jax.ShapeDtypeStruct((n, f), BF16)] * 2 + [jax.ShapeDtypeStruct((n, d), BF16)],
        scratch_shapes=[pltpu.VMEM((n, d), F32), pltpu.VMEM((n, d), BF16), pltpu.SemaphoreType.DMA(())],
        compiler_params=params(),
        cost_estimate=cost(4 * n * d * f, 4 * n * f, n * f),
        name="mlp_fwd",
    )(m, w_up, w_down, h)


def mlp_bwd(d_out, w_up, w_down, z, h, tile, sub):
    n, d = d_out.shape
    f = w_up.shape[1]
    col = pl.BlockSpec((n, tile), lambda i: (0, i))
    return pl.pallas_call(
        functools.partial(mlp_bwd_kernel, sub),
        grid=(f // tile,),
        in_specs=[kept((n, d)), pl.BlockSpec((d, tile), lambda i: (0, i)), pl.BlockSpec((tile, d), lambda i: (i, 0)), col, pl.BlockSpec(memory_space=pl.ANY)],
        out_specs=[col, kept((n, d))],
        out_shape=[jax.ShapeDtypeStruct((n, f), BF16), jax.ShapeDtypeStruct((n, d), BF16)],
        scratch_shapes=[pltpu.VMEM((n, d), F32), pltpu.VMEM((n, d), BF16), pltpu.SemaphoreType.DMA(())],
        compiler_params=params(),
        cost_estimate=cost(4 * n * d * f, 4 * n * f, n * f),
        name="mlp_bwd",
    )(d_out, w_up, w_down, z, h)


def peer_of(me, power):
    return me + power * (1 - 2 * ((me // power) % 2))


def enter_barrier(me):
    barrier = pltpu.get_barrier_semaphore()
    for power in (1, 2, 4, 8):
        pl.semaphore_signal(barrier, inc=1, device_id=(peer_of(me, power),), device_id_type=MESH)
    pl.semaphore_wait(barrier, 4)


def stream_scratch(half, width, slots):
    return [pltpu.VMEM((slots, half // k, width), F32) for k in (1, 2, 4, 8)] + [
        pltpu.SemaphoreType.DMA((4, slots)), pltpu.SemaphoreType.DMA((4, slots))]


def reduce_stage(s, j, shift, half, g_ref, out_ref, bufs, me):
    h0, h1, h2, h3, send_sem, recv_sem = bufs
    slots = h0.shape[0]
    slot, g = j % slots, g_ref.at[j % g_ref.shape[0]]
    core = me % 2
    powers, bits = [], []
    for k in range(3):
        r = (j + k + shift) % 3
        powers.append(2 + r + r * r)
        bits.append((me // powers[k]) % 2)
    held = (g, h0.at[slot], h1.at[slot], h2.at[slot], h3.at[slot])
    keep = (half * core,) + tuple((half >> (k + 1)) * bits[k] for k in range(3))
    away = (half * (1 - core),) + tuple((half >> (k + 1)) * (1 - bits[k]) for k in range(3))

    def part(ref, start, size):
        return ref.at[pl.ds(pl.multiple_of(start, 8), size)]

    def copy(k):
        peer = peer_of(me, 1) if k == 0 else peer_of(me, powers[k - 1])
        return pltpu.make_async_remote_copy(
            src_ref=part(held[k], away[k], half >> k), dst_ref=held[k + 1], send_sem=send_sem.at[k, slot],
            recv_sem=recv_sem.at[k, slot], device_id=(peer,), device_id_type=MESH)

    if s > 0:
        before = copy(s - 1)
        before.wait_recv()
        before.wait_send()
        own = held[s - 1][pl.ds(pl.multiple_of(keep[s - 1], 8), half >> (s - 1)), :]
        if s == 4:
            out_ref[...] = held[4][...] + own
        else:
            held[s][...] = held[s][...] + own
    if s < 4:
        copy(s).start()


def reduce_step(i, n, lags, streams, me):
    for stream in streams:
        for s in (4, 3, 2, 1, 0):
            j = i - lags[s]

            @pl.when((j >= 0) & (j < n))
            def _():
                reduce_stage(s, j, *stream, me)


def mlp_grads_kernel(n, lags, sub, d0_hbm, d1_hbm, m0t_hbm, m1t_hbm, h_hbm, z_ref, g0_ref, g1_ref, dup1_ref, wup_ref, wdown_ref,
                     share_ref, dmid_ref, acc_ref, du_ref, gd_ref, gu_ref, su_ref, d0_ref, d1_ref, m0t_ref, m1t_ref, h_ref, sems, *bufs):
    me = lax.axis_index('data')
    i = pl.program_id(0)

    load = loads((d0_hbm, d1_hbm, m0t_hbm, m1t_hbm, h_hbm), (d0_ref, d1_ref, m0t_ref, m1t_ref, h_ref), sems)

    @pl.when(i == 0)
    def _():
        for c in load:
            c.start()
        enter_barrier(me)
        acc_ref[...] = jnp.zeros_like(acc_ref)
        load[0].wait()

    @pl.when(i < n)
    def _():
        for r in range(d0_ref.shape[0] // sub):
            rows = pl.ds(r * sub, sub)
            da = dot(d0_ref[rows, :], wdown_ref[...], NT).astype(BF16).astype(F32)
            du = (da * gelu_slope(z_ref[rows, :].astype(F32))).astype(BF16)
            du_ref[rows, :] = du
            acc_ref[rows, :] += dot(du, wup_ref[...], NT)
        at_step(0, *(c.wait for c in load[1:4]))
        gd_ref[i % 2] = dot(g0_ref[...], d0_ref[...], TN) + dot(g1_ref[...], d1_ref[...], TN)
        gu_ref[i % 2] = dot(m0t_ref[...], du_ref[...]) + dot(m1t_ref[...], dup1_ref[...])

    @pl.when(i == n - 1)
    def _():
        load[4].wait()

        def finish(rows):
            dh = rms_pull(h_ref[rows, :], acc_ref[rows, :].astype(BF16))
            dmid_ref[rows, :] = (d0_ref[rows, :].astype(F32) + dh.astype(F32)).astype(BF16)

        in_chunks(d0_ref.shape[0], finish)

    reduce_step(i, n, lags, ((0, gd_ref.shape[1] // 2, gd_ref, share_ref.at[0, 0], bufs[:6]),
                             (2, gu_ref.shape[1] // 2, gu_ref, su_ref, bufs[6:])), me)

    @pl.when(i >= lags[4])
    def _():
        piece, width = share_ref.shape[2], su_ref.shape[1]
        for k in range(su_ref.shape[0] // piece):
            share_ref[0, 1, :, k * width:(k + 1) * width] = su_ref[k * piece:(k + 1) * piece, :]


def attn_grads_kernel(n, lags, *refs):
    xs, (u0, u1, m0, m1), out_ref, g_ref, bufs = refs[:8], refs[8:12], refs[12], refs[13], refs[14:]
    me = lax.axis_index('data')
    i = pl.program_id(0)

    @pl.when(i == 0)
    def _():
        enter_barrier(me)

    per = n // 4
    for w in range(4):
        @pl.when((i >= w * per) & (i < (w + 1) * per))
        def _():
            y0, y1 = (u0, u1) if w < 3 else (m0, m1)
            g_ref[i % 4] = dot(xs[2 * w][...], y0[...], TN) + dot(xs[2 * w + 1][...], y1[...], TN)

    reduce_step(i, n, lags, ((0, g_ref.shape[1] // 2, g_ref, out_ref.at[0], bufs),), me)


MLP_LAGS, MLP_SLOTS = (0, 1, 3, 4, 5), 6
ATTN_LAGS, ATTN_SLOTS = (0, 2, 4, 6, 8), 8


def kept(shape):
    return pl.BlockSpec(shape, lambda i: (0,) * len(shape), pipeline_mode=pl.Buffered(1))


def mlp_grads(ds, mts, h, z, gs, dup1, w_up, w_down, tile, sub):
    rows, d = h.shape
    n = w_up.shape[1] // tile
    at = lambda i: jnp.minimum(i, n - 1)
    col = pl.BlockSpec((rows, tile), lambda i: (0, at(i)))
    share = lambda i: (jnp.maximum(i - MLP_LAGS[4], 0), 0, 0, 0)
    anywhere = pl.BlockSpec(memory_space=pl.ANY)
    return pl.pallas_call(
        functools.partial(mlp_grads_kernel, n, MLP_LAGS, sub),
        grid=(n + MLP_LAGS[4],),
        in_specs=[anywhere] * 5 + [col] * 4 + [
            pl.BlockSpec((d, tile), lambda i: (0, at(i))), pl.BlockSpec((tile, d), lambda i: (at(i), 0))],
        out_specs=[pl.BlockSpec((1, 2, tile // 16, d), share), kept((rows, d))],
        out_shape=[jax.ShapeDtypeStruct((n, 2, tile // 16, d), F32), jax.ShapeDtypeStruct((rows, d), BF16)],
        scratch_shapes=[pltpu.VMEM((rows, d), F32), pltpu.VMEM((rows, tile), BF16), pltpu.VMEM((2, tile, d), F32),
                        pltpu.VMEM((2, d, tile), F32), pltpu.VMEM((d // 16, tile), F32)] + [
                            pltpu.VMEM(a.shape, BF16) for a in (*ds, *mts, h)] + [pltpu.SemaphoreType.DMA((5,))] + stream_scratch(tile // 2, d, MLP_SLOTS) + stream_scratch(d // 2, tile, MLP_SLOTS),
        compiler_params=pltpu.CompilerParams(dimension_semantics=("arbitrary",), collective_id=0, has_side_effects=True,
                                             vmem_limit_bytes=63 * 1024 * 1024),
        cost_estimate=cost(12 * rows * d * n * tile, 10 * rows * n * tile),
        name="mlp_grads",
    )(*ds, *mts, h, z, *gs, dup1, w_up, w_down)


def attn_grads(xs, ys, tile):
    rows, d = ys[0].shape
    per = d // tile
    n = 4 * per
    cols = [pl.BlockSpec((rows, tile), lambda i, w=w: (0, jnp.clip(i - w * per, 0, per - 1))) for w in range(4) for _ in range(2)]
    return pl.pallas_call(
        functools.partial(attn_grads_kernel, n, ATTN_LAGS),
        grid=(n + ATTN_LAGS[4],),
        in_specs=cols + [kept((rows, d))] * 4,
        out_specs=pl.BlockSpec((1, tile // 16, d), lambda i: (jnp.maximum(i - ATTN_LAGS[4], 0), 0, 0)),
        out_shape=jax.ShapeDtypeStruct((n, tile // 16, d), F32),
        scratch_shapes=[pltpu.VMEM((4, tile, d), F32)] + stream_scratch(tile // 2, d, ATTN_SLOTS),
        compiler_params=pltpu.CompilerParams(dimension_semantics=("arbitrary",), collective_id=1, has_side_effects=True,
                                             vmem_limit_bytes=VMEM_LIMIT),
        cost_estimate=cost(16 * rows * d * d, 24 * rows * d),
        name="attn_grads",
    )(*[x for pair in xs for x in pair], *ys)


def put_in_place(j, shift, in_ref, out_ref, bands):
    half = out_ref.shape[0] // 2
    piece, width = in_ref.shape[1], out_ref.shape[1]
    for v in range(3):
        @pl.when((j + shift) % 3 == v)
        def _():
            for dev in range(16):
                bits = [(dev >> (1 + (v + k) % 3)) & 1 for k in range(3)]
                at = half * (dev & 1) + sum((half >> (k + 1)) * bits[k] for k in range(3))
                for k in range(bands):
                    out_ref[at + k * piece:at + (k + 1) * piece, :] = in_ref[dev, :, k * width:(k + 1) * width]


def place_mlp_kernel(group, down_in, up_in, down_ref, up_ref):
    high, width = down_ref.shape[0] // group, up_ref.shape[1] // group
    for c in range(group):
        j = pl.program_id(0) * group + c
        put_in_place(j, 0, down_in.at[:, c, 0], down_ref.at[pl.ds(c * high, high)], 1)
        put_in_place(j, 2, up_in.at[:, c, 0], up_ref.at[:, pl.ds(c * width, width)], up_ref.shape[0] // (16 * up_in.shape[3]))


def place_mlp(shares, tile, group):
    _, n, _, piece, d = shares.shape
    block = lambda w: pl.BlockSpec((16, group, 1, piece, d), lambda i: (0, i, w, 0, 0))
    return pl.pallas_call(
        functools.partial(place_mlp_kernel, group),
        grid=(n // group,),
        in_specs=[block(0), block(1)],
        out_specs=[pl.BlockSpec((group * tile, d), lambda i: (i, 0)), pl.BlockSpec((d, group * tile), lambda i: (0, i))],
        out_shape=[jax.ShapeDtypeStruct((n * tile, d), F32), jax.ShapeDtypeStruct((d, n * tile), F32)],
        compiler_params=params(),
        cost_estimate=cost(shares.size // 2, 8 * shares.size),
        name="place_mlp",
    )(shares, shares)


def place_attn_kernel(per, in_ref, *outs):
    i = pl.program_id(0)
    for w in range(4):
        @pl.when((i >= w * per) & (i < (w + 1) * per))
        def _():
            put_in_place(i, 0, in_ref.at[:, 0], outs[w], 1)


def place_attn(shares):
    _, n, piece, d = shares.shape
    per = n // 4
    return pl.pallas_call(
        functools.partial(place_attn_kernel, per),
        grid=(n,),
        in_specs=[pl.BlockSpec((16, 1, piece, d), lambda i: (0, i, 0, 0))],
        out_specs=[pl.BlockSpec((16 * piece, d), lambda i, w=w: (jnp.clip(i - w * per, 0, per - 1), 0)) for w in range(4)],
        out_shape=[jax.ShapeDtypeStruct((per * 16 * piece, d), F32)] * 4,
        compiler_params=params(),
        cost_estimate=cost(shares.size // 2, 8 * shares.size),
        name="place_attn",
    )(shares)


def solution(mesh):
    batch_spec = P('data', None, None)

    def per_device(x_loc, g_loc, step_emb, w_q, w_k, w_v, w_o, w_up, w_down):
        d, n_heads, head = w_q.shape
        scale = head ** -0.5
        n_seq, seq, _ = x_loc.shape
        n = n_seq * seq
        wq, wk, wv = (w.transpose(1, 2, 0).reshape(n_heads * head, d) for w in (w_q, w_k, w_v))
        wo = w_o.reshape(n_heads * head, d)
        head_of = jnp.arange(256) // 64
        mask = (head_of[:, None] == head_of[None, :]).astype(BF16)
        x = x_loc.reshape(n, d)
        saved = []
        for l in range(2):
            xc, u, q, k, v, mix, h, m, mt = attn_fwd(x, step_emb[l:l + 1], wq, wk, wv, wo, mask, seq, scale, 512)
            z, g, x = mlp_fwd(m, w_up, w_down, h, 1024, 512)
            saved.append((xc, u, q, k, v, mix, h, mt, z, g))
        (_, u0, _, _, _, mix0, h0, mt0, z0, g0), (_, u1, _, _, _, mix1, h1, mt1, z1, g1) = saved

        def attn_back(l, dmid):
            xc, _, q, k, v = saved[l][:5]
            return attn_bwd(dmid, q, k, v, xc, wq, wk, wv, wo, mask, seq, scale, 512)

        do1 = g_loc.reshape(n, d)
        dup1, dmid1 = mlp_bwd(do1, w_up, w_down, z1, h1, 1024, 512)
        dq1, dk1, dv1, do0 = attn_back(1, dmid1)
        s_mlp, dmid0 = mlp_grads((do0, do1), (mt0, mt1), h0, z0, (g0, g1), dup1, w_up, w_down, 256, 256)
        a_mlp = lax.all_gather(s_mlp, 'data')
        dq0, dk0, dv0, d_out = attn_back(0, dmid0)
        s_attn = attn_grads([(dq0, dq1), (dk0, dk1), (dv0, dv1), (mix0, mix1)], (u0, u1, dmid0, dmid1), 256)
        a_attn = lax.all_gather(s_attn, 'data')
        g_down, g_up = place_mlp(a_mlp, 256, 2)
        g_q, g_k, g_v, g_o = place_attn(a_attn)
        heads = lambda a: a.reshape(n_heads, head, d).transpose(2, 0, 1)
        return heads(g_q), heads(g_k), heads(g_v), g_o.reshape(w_o.shape), g_up, g_down, d_out.reshape(x_loc.shape)

    return jax.shard_map(per_device, mesh=mesh, in_specs=(batch_spec, batch_spec, P(), P(), P(), P(), P(), P(), P()), out_specs=(P(), P(), P(), P(), P(), P(), batch_spec), check_vma=False)
```

```python
import functools
import math

import jax
import jax.numpy as jnp
import numpy as np
from jax import lax
from jax.experimental import pallas as pl
from jax.experimental.pallas import tpu as pltpu
from jax.sharding import PartitionSpec as P


NORM_EPS = 1e-6
GELU_C = math.sqrt(2.0 / math.pi)
GELU_A = 0.044715
BF16 = jnp.bfloat16
F32 = jnp.float32
VMEM_LIMIT = 60 * 1024 * 1024

NN = (((1,), (0,)), ((), ()))
NT = (((1,), (1,)), ((), ()))
TN = (((0,), (0,)), ((), ()))
MESH = pl.DeviceIdType.MESH


def dot(a, b, dims=NN):
    return lax.dot_general(a, b, dims, preferred_element_type=F32)


def rms_scale(x_f32):
    return lax.rsqrt(jnp.mean(x_f32 * x_f32, axis=-1, keepdims=True) + NORM_EPS)


def rms_pull(x_bf16, d_bf16):
    x = x_bf16.astype(F32)
    d = d_bf16.astype(F32)
    r = rms_scale(x)
    dot_dx = jnp.mean(d * x, axis=-1, keepdims=True)
    return (d * r - x * (r * r * r * dot_dx)).astype(BF16)


def gelu_tanh(z):
    return jnp.tanh(GELU_C * (z + GELU_A * (z * z * z)))


def gelu_slope(z):
    t = gelu_tanh(z)
    return 0.5 * (1.0 + t) + (0.5 * z) * ((1.0 - t * t) * (GELU_C * (1.0 + (3.0 * GELU_A) * (z * z))))


def block_diag(a, mask):
    return jnp.concatenate([a, a, a, a], axis=0) * mask


def diag_blocks(full, seq, lane_lo):
    left = jnp.where(lane_lo, full[0:seq, 0:128], full[seq:2 * seq, 0:128])
    right = jnp.where(lane_lo, full[2 * seq:3 * seq, 128:256], full[3 * seq:4 * seq, 128:256])
    return jnp.concatenate([left, right], axis=1)


def softmax_t(scores_t, scale):
    s = scores_t * scale
    e = jnp.exp(s - jnp.max(s, axis=0, keepdims=True))
    return e / jnp.sum(e, axis=0, keepdims=True)


def in_chunks(n, body, rows=32):
    def step(i, _):
        body(pl.ds(pl.multiple_of(i * rows, rows), rows))
        return 0

    lax.fori_loop(0, n // rows, step, 0, unroll=2)


def loads(refs, bufs, sems):
    return [pltpu.make_async_copy(r, b, sems.at[k]) for k, (r, b) in enumerate(zip(refs, bufs))]


def at_step(step, *actions):
    @pl.when(pl.program_id(0) == step)
    def _():
        for act in actions:
            act()


def attn_fwd_kernel(layer, seq, scale, x_ref, e_ref, mask_ref, wq_hbm, wk_hbm, wv_hbm, wo_hbm,
                    xc_ref, u_ref, q_ref, k_ref, v_ref, mix_ref, h_ref, m_ref, mt_ref, wq_ref, wk_ref, wv_ref, wo_ref, sems):
    load = loads((wq_hbm, wk_hbm, wv_hbm, wo_hbm), (wq_ref, wk_ref, wv_ref, wo_ref), sems)
    at_step(0, *(c.start for c in load))
    n_rows = x_ref.shape[0]
    blocks = [pl.ds(r * (n_rows // 2), n_rows // 2) for r in range(2)]
    at_step(0, *(c.wait for c in load))
    for rows in blocks:
        x = (x_ref[rows, :].astype(F32) + e_ref[layer:layer + 1, :].astype(F32)).astype(BF16)
        xc_ref[rows, :] = x
        x_f32 = x.astype(F32)
        u_ref[rows, :] = (x_f32 * rms_scale(x_f32)).astype(BF16)
        for w_ref, o_ref in ((wq_ref, q_ref), (wk_ref, k_ref), (wv_ref, v_ref)):
            o_ref[rows, :] = dot(u_ref[rows, :], w_ref[...], NT).astype(BF16)

    n_groups = x_ref.shape[1] // 256
    lane_lo = lax.broadcasted_iota(jnp.int32, (seq, 128), 1) < 64

    def one_seq(s):
        rows = pl.ds(s * seq, seq)
        cols = [pl.ds(g * 256, 256) for g in range(n_groups)]
        mask = mask_ref[...]
        st = [dot(k_ref[rows, c], block_diag(q_ref[rows, c], mask), NT).astype(BF16).astype(F32) for c in cols]
        pb = [softmax_t(t, scale).astype(BF16) for t in st]
        for c, p in zip(cols, pb):
            mix_ref[rows, c] = diag_blocks(dot(p, v_ref[rows, c], TN), seq, lane_lo).astype(BF16)

    for s in range(x_ref.shape[0] // seq):
        one_seq(s)
    for rows in blocks:
        h = (xc_ref[rows, :].astype(F32) + dot(mix_ref[rows, :], wo_ref[...]).astype(BF16).astype(F32)).astype(BF16)
        h_ref[rows, :] = h
        h_f32 = h.astype(F32)
        m_ref[rows, :] = (h_f32 * rms_scale(h_f32)).astype(BF16)
    mt_ref[...] = m_ref[...].T


def attn_bwd_kernel(seq, scale, dmid_ref, q_ref, k_ref, v_ref, xc_ref, mask_ref, wo_hbm, wq_hbm, wk_hbm, wv_hbm,
                    dq_ref, dk_ref, dv_ref, dprev_ref, dmix_ref, wo_ref, wq_ref, wk_ref, wv_ref, sems):
    load = loads((wo_hbm, wq_hbm, wk_hbm, wv_hbm), (wo_ref, wq_ref, wk_ref, wv_ref), sems)
    at_step(0, *(c.start for c in load), load[0].wait)
    dmix_ref[...] = dot(dmid_ref[...], wo_ref[...], NT).astype(BF16)
    n_groups = xc_ref.shape[1] // 256
    lane_lo = lax.broadcasted_iota(jnp.int32, (seq, 128), 1) < 64

    def one_seq(s, _):
        rows = pl.ds(pl.multiple_of(s * seq, seq), seq)
        cols = [pl.ds(g * 256, 256) for g in range(n_groups)]
        mask = mask_ref[...]
        qbd = [block_diag(q_ref[rows, c], mask) for c in cols]
        dbd = [block_diag(dmix_ref[rows, c], mask) for c in cols]
        st = [dot(k_ref[rows, c], t, NT).astype(BF16).astype(F32) for c, t in zip(cols, qbd)]
        dp = [dot(v_ref[rows, c], t, NT).astype(BF16).astype(F32) for c, t in zip(cols, dbd)]
        p = [softmax_t(t, scale) for t in st]
        for c, a, t in zip(cols, p, dbd):
            dv_ref[rows, c] = dot(a.astype(BF16), t).astype(BF16)
        ds = [((a * (t - jnp.sum(a * t, axis=0, keepdims=True))) * scale).astype(BF16) for a, t in zip(p, dp)]
        for c, a, t in zip(cols, ds, qbd):
            dk_ref[rows, c] = dot(a, t).astype(BF16)
            dq_ref[rows, c] = diag_blocks(dot(a, k_ref[rows, c], TN), seq, lane_lo).astype(BF16)
        return 0

    lax.fori_loop(0, xc_ref.shape[0] // seq, one_seq, 0, unroll=4)
    at_step(0, *(c.wait for c in load[1:]))
    n_rows = xc_ref.shape[0]
    for rows in [pl.ds(r * (n_rows // 2), n_rows // 2) for r in range(2)]:
        du = dot(dq_ref[rows, :], wq_ref[...]) + dot(dk_ref[rows, :], wk_ref[...]) + dot(dv_ref[rows, :], wv_ref[...])
        dx = rms_pull(xc_ref[rows, :], du.astype(BF16))
        dprev_ref[rows, :] = (dmid_ref[rows, :].astype(F32) + dx.astype(F32)).astype(BF16)


def mlp_fwd_kernel(sub, m_ref, wup_ref, wdown_ref, h_hbm, z_ref, g_ref, y_ref, acc_ref, h_ref, sem):
    step = pl.program_id(0)
    load = pltpu.make_async_copy(h_hbm, h_ref, sem)
    at_step(0, load.start)

    @pl.when(step == 0)
    def _():
        acc_ref[...] = jnp.zeros_like(acc_ref)

    for r in range(m_ref.shape[0] // sub):
        rows = pl.ds(r * sub, sub)
        zb = dot(m_ref[rows, :], wup_ref[...]).astype(BF16)
        z_ref[rows, :] = zb
        z = zb.astype(F32)
        g = ((0.5 * z) * (1.0 + gelu_tanh(z))).astype(BF16)
        g_ref[rows, :] = g
        acc_ref[rows, :] += dot(g, wdown_ref[...])

    @pl.when(step == pl.num_programs(0) - 1)
    def _():
        load.wait()

        def finish(rows):
            y = acc_ref[rows, :].astype(BF16)
            y_ref[rows, :] = (h_ref[rows, :].astype(F32) + y.astype(F32)).astype(BF16)

        in_chunks(m_ref.shape[0], finish)


def mlp_bwd_kernel(sub, d_ref, wup_ref, wdown_ref, z_ref, h_hbm, dup_ref, dmid_ref, acc_ref, h_ref, sem):
    step = pl.program_id(0)
    load = pltpu.make_async_copy(h_hbm, h_ref, sem)
    at_step(0, load.start)

    @pl.when(step == 0)
    def _():
        acc_ref[...] = jnp.zeros_like(acc_ref)

    for r in range(d_ref.shape[0] // sub):
        rows = pl.ds(r * sub, sub)
        da = dot(d_ref[rows, :], wdown_ref[...], NT).astype(BF16).astype(F32)
        du = (da * gelu_slope(z_ref[rows, :].astype(F32))).astype(BF16)
        dup_ref[rows, :] = du
        acc_ref[rows, :] += dot(du, wup_ref[...], NT)

    @pl.when(step == pl.num_programs(0) - 1)
    def _():
        load.wait()

        def finish(rows):
            dh = rms_pull(h_ref[rows, :], acc_ref[rows, :].astype(BF16))
            dmid_ref[rows, :] = (d_ref[rows, :].astype(F32) + dh.astype(F32)).astype(BF16)

        in_chunks(d_ref.shape[0], finish)


def params(**kw):
    return pltpu.CompilerParams(dimension_semantics=("arbitrary",), vmem_limit_bytes=VMEM_LIMIT, **kw)


def cost(flops, nbytes, trans=0):
    return pl.CostEstimate(flops=int(flops), bytes_accessed=int(nbytes), transcendentals=int(trans))


def whole(shape):
    return pl.BlockSpec(shape, lambda i: (0,) * len(shape))


def attn_fwd(x, step_emb, layer, wq, wk, wv, wo, mask, seq, scale, tile):
    n, d = x.shape
    row = pl.BlockSpec((tile, d), lambda i: (i, 0))
    return pl.pallas_call(
        functools.partial(attn_fwd_kernel, layer, seq, scale),
        grid=(n // tile,),
        in_specs=[row, whole(step_emb.shape), whole(mask.shape)] + [pl.BlockSpec(memory_space=pl.ANY)] * 4,
        out_specs=[row] * 8 + [pl.BlockSpec((d, tile), lambda i: (0, i))],
        out_shape=[jax.ShapeDtypeStruct((n, d), BF16)] * 8 + [jax.ShapeDtypeStruct((d, n), BF16)],
        scratch_shapes=[pltpu.VMEM(w.shape, BF16) for w in (wq, wk, wv, wo)] + [pltpu.SemaphoreType.DMA((4,))],
        compiler_params=params(),
        cost_estimate=cost(8 * n * d * d, 20 * n * d, n * d),
        name="attn_fwd",
    )(x, step_emb, mask, wq, wk, wv, wo)


def attn_bwd(dmid, q, k, v, xc, wq, wk, wv, wo, mask, seq, scale, tile):
    n, d = xc.shape
    row = pl.BlockSpec((tile, d), lambda i: (i, 0))
    return pl.pallas_call(
        functools.partial(attn_bwd_kernel, seq, scale),
        grid=(n // tile,),
        in_specs=[row] * 5 + [whole(mask.shape)] + [pl.BlockSpec(memory_space=pl.ANY)] * 4,
        out_specs=[row] * 4,
        out_shape=[jax.ShapeDtypeStruct((n, d), BF16)] * 4,
        scratch_shapes=[pltpu.VMEM((tile, d), BF16)] + [pltpu.VMEM(w.shape, BF16) for w in (wo, wq, wk, wv)] + [pltpu.SemaphoreType.DMA((4,))],
        compiler_params=params(),
        cost_estimate=cost(8 * n * d * d, 20 * n * d, n * d),
        name="attn_bwd",
    )(dmid, q, k, v, xc, mask, wo, wq, wk, wv)


def mlp_fwd(m, w_up, w_down, h, tile, sub):
    n, d = m.shape
    f = w_up.shape[1]
    col = pl.BlockSpec((n, tile), lambda i: (0, i))
    return pl.pallas_call(
        functools.partial(mlp_fwd_kernel, sub),
        grid=(f // tile,),
        in_specs=[kept((n, d)), pl.BlockSpec((d, tile), lambda i: (0, i)), pl.BlockSpec((tile, d), lambda i: (i, 0)), pl.BlockSpec(memory_space=pl.ANY)],
        out_specs=[col, col, kept((n, d))],
        out_shape=[jax.ShapeDtypeStruct((n, f), BF16)] * 2 + [jax.ShapeDtypeStruct((n, d), BF16)],
        scratch_shapes=[pltpu.VMEM((n, d), F32), pltpu.VMEM((n, d), BF16), pltpu.SemaphoreType.DMA(())],
        compiler_params=params(),
        cost_estimate=cost(4 * n * d * f, 4 * n * f, n * f),
        name="mlp_fwd",
    )(m, w_up, w_down, h)


def mlp_bwd(d_out, w_up, w_down, z, h, tile, sub):
    n, d = d_out.shape
    f = w_up.shape[1]
    col = pl.BlockSpec((n, tile), lambda i: (0, i))
    return pl.pallas_call(
        functools.partial(mlp_bwd_kernel, sub),
        grid=(f // tile,),
        in_specs=[kept((n, d)), pl.BlockSpec((d, tile), lambda i: (0, i)), pl.BlockSpec((tile, d), lambda i: (i, 0)), col, pl.BlockSpec(memory_space=pl.ANY)],
        out_specs=[col, kept((n, d))],
        out_shape=[jax.ShapeDtypeStruct((n, f), BF16), jax.ShapeDtypeStruct((n, d), BF16)],
        scratch_shapes=[pltpu.VMEM((n, d), F32), pltpu.VMEM((n, d), BF16), pltpu.SemaphoreType.DMA(())],
        compiler_params=params(),
        cost_estimate=cost(4 * n * d * f, 4 * n * f, n * f),
        name="mlp_bwd",
    )(d_out, w_up, w_down, z, h)


def peer_of(me, power):
    return me + power * (1 - 2 * ((me // power) % 2))


def enter_barrier(me):
    barrier = pltpu.get_barrier_semaphore()
    for power in (1, 2, 4, 8):
        pl.semaphore_signal(barrier, inc=1, device_id=(peer_of(me, power),), device_id_type=MESH)
    pl.semaphore_wait(barrier, 4)


def stream_scratch(half, width, slots):
    return [pltpu.VMEM((slots, half // k, width), F32) for k in (1, 2, 4, 8)] + [
        pltpu.SemaphoreType.DMA((4, slots)), pltpu.SemaphoreType.DMA((4, slots))]


def put(ref, value):
    ref[0] = value


def reduce_stage(s, j, shift, half, g_ref, sink, bufs, me):
    h0, h1, h2, h3, send_sem, recv_sem = bufs
    slots = h0.shape[0]
    slot, g = j % slots, g_ref.at[j % g_ref.shape[0]]
    core = me % 2
    powers, bits = [], []
    for k in range(3):
        r = (j + k + shift) % 3
        powers.append(2 + r + r * r)
        bits.append((me // powers[k]) % 2)
    held = (g, h0.at[slot], h1.at[slot], h2.at[slot], h3.at[slot])
    keep = (half * core,) + tuple((half >> (k + 1)) * bits[k] for k in range(3))
    away = (half * (1 - core),) + tuple((half >> (k + 1)) * (1 - bits[k]) for k in range(3))

    def part(ref, start, size):
        return ref.at[pl.ds(pl.multiple_of(start, 8), size)]

    def copy(k):
        peer = peer_of(me, 1) if k == 0 else peer_of(me, powers[k - 1])
        return pltpu.make_async_remote_copy(
            src_ref=part(held[k], away[k], half >> k), dst_ref=held[k + 1], send_sem=send_sem.at[k, slot],
            recv_sem=recv_sem.at[k, slot], device_id=(peer,), device_id_type=MESH)

    if s > 0:
        before = copy(s - 1)
        before.wait_recv()
        before.wait_send()
        own = held[s - 1][pl.ds(pl.multiple_of(keep[s - 1], 8), half >> (s - 1)), :]
        if s == 4:
            sink(j, held[4][...] + own)
        else:
            held[s][...] = held[s][...] + own
    if s < 4:
        copy(s).start()


def reduce_step(i, lags, streams, me):
    for n, *stream in streams:
        for s in (4, 3, 2, 1, 0):
            j = i - lags[s]

            @pl.when((j >= 0) & (j < n))
            def _():
                reduce_stage(s, j, *stream, me)


def mlp_grads_kernel(n, n_o, lags, sub, d0_hbm, d1_hbm, m0t_hbm, m1t_hbm, h_hbm, dmid1_hbm, z_ref, g0_ref, g1_ref, dup1_ref,
                     wup_ref, wdown_ref, mix0_ref, mix1_ref, share_hbm, dmid_ref, acc_ref, du_ref, gd_ref, gu_ref, d0_ref, d1_ref,
                     m0t_ref, m1t_ref, out_d, out_u, load_sem, out_sem, *bufs):
    me = lax.axis_index('data')
    i = pl.program_id(0)
    load = loads((d0_hbm, d1_hbm, m0t_hbm, m1t_hbm, h_hbm, dmid1_hbm), (d0_ref, d1_ref, m0t_ref, m1t_ref, d1_ref, d1_ref), load_sem)

    @pl.when(i == 0)
    def _():
        for c in load[:4]:
            c.start()
        enter_barrier(me)
        acc_ref[...] = jnp.zeros_like(acc_ref)
        load[0].wait()

    @pl.when(i < n)
    def _():
        for r in range(d0_ref.shape[0] // sub):
            rows = pl.ds(r * sub, sub)
            da = dot(d0_ref[rows, :], wdown_ref[...], NT).astype(BF16).astype(F32)
            du = (da * gelu_slope(z_ref[rows, :].astype(F32))).astype(BF16)
            du_ref[rows, :] = du
            acc_ref[rows, :] += dot(du, wup_ref[...], NT)
        at_step(0, *(c.wait for c in load[1:4]))
        gd_ref[i % 2] = dot(g0_ref[...], d0_ref[...], TN) + dot(g1_ref[...], d1_ref[...], TN)
        gu_ref[i % 2] = dot(m0t_ref[...], du_ref[...]) + dot(m1t_ref[...], dup1_ref[...])

    @pl.when(i == n - 1)
    def _():
        load[4].start()
        load[4].wait()

        def finish(rows):
            dh = rms_pull(d1_ref[rows, :], acc_ref[rows, :].astype(BF16))
            dmid_ref[rows, :] = (d0_ref[rows, :].astype(F32) + dh.astype(F32)).astype(BF16)

        in_chunks(d0_ref.shape[0], finish)
        load[5].start()

    @pl.when(i == n)
    def _():
        load[5].wait()

    @pl.when((i >= n) & (i < n + n_o))
    def _():
        gd_ref[i % 2] = dot(mix0_ref[...], dmid_ref[...], TN) + dot(mix1_ref[...], d1_ref[...], TN)

    def out_copy(k, j, row):
        return pltpu.make_async_copy((out_d, out_u)[k].at[j % 2], share_hbm.at[row], out_sem.at[k, j % 2])

    def sink_down(j, share):
        @pl.when(j >= 2)
        def _():
            out_copy(0, j, 0).wait()

        out_d[j % 2] = share
        out_copy(0, j, jnp.where(j < n, 2 * j, n + j)).start()

    def sink_up(j, share):
        @pl.when(j >= 2)
        def _():
            out_copy(1, j, 0).wait()

        piece, width = out_u.shape[1], share.shape[1]
        for k in range(share.shape[0] // piece):
            out_u[j % 2, :, k * width:(k + 1) * width] = share[k * piece:(k + 1) * piece, :]
        out_copy(1, j, 2 * j + 1).start()

    reduce_step(i, lags, ((n + n_o, 0, gd_ref.shape[1] // 2, gd_ref, sink_down, bufs[:6]),
                          (n, 2, gu_ref.shape[1] // 2, gu_ref, sink_up, bufs[6:])), me)

    @pl.when(i == n + n_o + lags[4] - 1)
    def _():
        for k in range(2):
            for j in range(2):
                out_copy(k, j, 0).wait()


def attn_grads_kernel(n, lags, *refs):
    xs, (y0, y1), out_ref, g_ref, bufs = refs[:6], refs[6:8], refs[8], refs[9], refs[10:]
    me = lax.axis_index('data')
    i = pl.program_id(0)

    @pl.when(i == 0)
    def _():
        enter_barrier(me)

    per = n // 3
    for w in range(3):
        @pl.when((i >= w * per) & (i < (w + 1) * per))
        def _():
            g_ref[i % 4] = dot(xs[2 * w][...], y0[...], TN) + dot(xs[2 * w + 1][...], y1[...], TN)

    reduce_step(i, lags, ((n, 0, g_ref.shape[1] // 2, g_ref, lambda j, share: put(out_ref, share), bufs),), me)


MLP_LAGS, MLP_SLOTS = (0, 1, 3, 4, 5), 6
ATTN_LAGS, ATTN_SLOTS = (0, 2, 4, 6, 8), 8


def kept(shape):
    return pl.BlockSpec(shape, lambda i: (0,) * len(shape), pipeline_mode=pl.Buffered(1))


def mlp_grads(ds, mts, h, dmid1, mixes, z, gs, dup1, w_up, w_down, tile, sub):
    rows, d = h.shape
    n, n_o = w_up.shape[1] // tile, d // tile
    at = lambda i: jnp.minimum(i, n - 1)
    col = pl.BlockSpec((rows, tile), lambda i: (0, at(i)))
    mix = pl.BlockSpec((rows, tile), lambda i: (0, jnp.clip(i - n, 0, n_o - 1)))
    anywhere = pl.BlockSpec(memory_space=pl.ANY)
    piece = tile // 16
    return pl.pallas_call(
        functools.partial(mlp_grads_kernel, n, n_o, MLP_LAGS, sub),
        grid=(n + n_o + MLP_LAGS[4],),
        in_specs=[anywhere] * 6 + [col] * 4 + [
            pl.BlockSpec((d, tile), lambda i: (0, at(i))), pl.BlockSpec((tile, d), lambda i: (at(i), 0)), mix, mix],
        out_specs=[anywhere, kept((rows, d))],
        out_shape=[jax.ShapeDtypeStruct((2 * n + n_o, piece, d), F32), jax.ShapeDtypeStruct((rows, d), BF16)],
        scratch_shapes=[pltpu.VMEM((rows, d), F32), pltpu.VMEM((rows, tile), BF16), pltpu.VMEM((2, tile, d), F32),
                        pltpu.VMEM((2, d, tile), F32)] + [pltpu.VMEM(a.shape, BF16) for a in (*ds, *mts)] + [
                            pltpu.VMEM((2, piece, d), F32), pltpu.VMEM((2, piece, d), F32), pltpu.SemaphoreType.DMA((6,)),
                            pltpu.SemaphoreType.DMA((2, 2))] + stream_scratch(tile // 2, d, MLP_SLOTS) + stream_scratch(d // 2, tile, MLP_SLOTS),
        compiler_params=pltpu.CompilerParams(dimension_semantics=("arbitrary",), collective_id=0, has_side_effects=True,
                                             vmem_limit_bytes=63 * 1024 * 1024),
        cost_estimate=cost(12 * rows * d * n * tile, 10 * rows * n * tile),
        name="mlp_grads",
    )(*ds, *mts, h, dmid1, z, *gs, dup1, w_up, w_down, *mixes)


def attn_grads(xs, ys, tile):
    rows, d = ys[0].shape
    per = d // tile
    n = 3 * per
    cols = [pl.BlockSpec((rows, tile), lambda i, w=w: (0, jnp.clip(i - w * per, 0, per - 1))) for w in range(3) for _ in range(2)]
    return pl.pallas_call(
        functools.partial(attn_grads_kernel, n, ATTN_LAGS),
        grid=(n + ATTN_LAGS[4],),
        in_specs=cols + [kept((rows, d))] * 2,
        out_specs=pl.BlockSpec((1, tile // 16, d), lambda i: (jnp.maximum(i - ATTN_LAGS[4], 0), 0, 0)),
        out_shape=jax.ShapeDtypeStruct((n, tile // 16, d), F32),
        scratch_shapes=[pltpu.VMEM((4, tile, d), F32)] + stream_scratch(tile // 2, d, ATTN_SLOTS),
        compiler_params=pltpu.CompilerParams(dimension_semantics=("arbitrary",), collective_id=1, has_side_effects=True,
                                             vmem_limit_bytes=VMEM_LIMIT),
        cost_estimate=cost(12 * rows * d * d, 24 * rows * d),
        name="attn_grads",
    )(*[x for pair in xs for x in pair], *ys)


def put_in_place(j, shift, in_ref, out_ref, bands):
    half = out_ref.shape[0] // 2
    piece, width = in_ref.shape[1], out_ref.shape[1]

    def variant(v):
        for dev in range(16):
            bits = [(dev >> (1 + (v + k) % 3)) & 1 for k in range(3)]
            at = half * (dev & 1) + sum((half >> (k + 1)) * bits[k] for k in range(3))
            for k in range(bands):
                out_ref[at + k * piece:at + (k + 1) * piece, :] = in_ref[dev, :, k * width:(k + 1) * width]

    if isinstance(j, int):
        variant((j + shift) % 3)
    else:
        for v in range(3):
            pl.when((j + shift) % 3 == v)(functools.partial(variant, v))


def place_mlp_kernel(group, in_ref, down_ref, up_ref):
    high, width = down_ref.shape[0] // group, up_ref.shape[1] // group
    for c in range(group):
        j = pl.program_id(0) * group + c
        put_in_place(j, 0, in_ref.at[:, 2 * c], down_ref.at[pl.ds(c * high, high)], 1)
        put_in_place(j, 2, in_ref.at[:, 2 * c + 1], up_ref.at[:, pl.ds(c * width, width)], up_ref.shape[0] // (16 * in_ref.shape[2]))


def place_mlp(shares, n, tile, group):
    _, _, piece, d = shares.shape
    return pl.pallas_call(
        functools.partial(place_mlp_kernel, group),
        grid=(n // group,),
        in_specs=[pl.BlockSpec((16, 2 * group, piece, d), lambda i: (0, i, 0, 0))],
        out_specs=[pl.BlockSpec((group * tile, d), lambda i: (i, 0)), pl.BlockSpec((d, group * tile), lambda i: (0, i))],
        out_shape=[jax.ShapeDtypeStruct((n * tile, d), F32), jax.ShapeDtypeStruct((d, n * tile), F32)],
        compiler_params=params(),
        cost_estimate=cost(shares.size // 2, 8 * shares.size),
        name="place_mlp",
    )(shares)


def place_rows_kernel(first, turn, per, in_ref, *refs):
    outs, (in_buf, out_buf, in_sem, out_sem) = refs[:-4], refs[-4:]
    depth, high = in_buf.shape[0], out_buf.shape[1]
    total = per * len(outs)

    def fetch(t):
        return pltpu.make_async_copy(in_ref.at[:, first + t], in_buf.at[t % depth], in_sem.at[t % depth])

    def store(t):
        at = t % per * high
        return pltpu.make_async_copy(out_buf.at[t % depth], outs[t // per].at[pl.ds(at, high)], out_sem.at[t % depth])

    for t in range(min(depth, total)):
        fetch(t).start()
    for t in range(total):
        fetch(t).wait()
        if t >= depth:
            store(t - depth).wait()
        put_in_place(turn + t, 0, in_buf.at[t % depth], out_buf.at[t % depth], 1)
        store(t).start()
        if t + depth < total:
            fetch(t + depth).start()
    for t in range(max(total - depth, 0), total):
        store(t).wait()


def place_rows(shares, first, turn, per, n_out, depth):
    _, _, piece, d = shares.shape
    anywhere = pl.BlockSpec(memory_space=pl.ANY)
    return pl.pallas_call(
        functools.partial(place_rows_kernel, first, turn, per),
        in_specs=[anywhere],
        out_specs=[anywhere] * n_out,
        out_shape=[jax.ShapeDtypeStruct((per * 16 * piece, d), F32)] * n_out,
        scratch_shapes=[pltpu.VMEM((depth, 16, piece, d), F32), pltpu.VMEM((depth, 16 * piece, d), F32),
                        pltpu.SemaphoreType.DMA((depth,)), pltpu.SemaphoreType.DMA((depth,))],
        compiler_params=pltpu.CompilerParams(vmem_limit_bytes=VMEM_LIMIT),
        cost_estimate=cost(per * n_out * piece * d * 16, per * n_out * piece * d * 128),
        name="place_rows",
    )(shares)


def solution(mesh):
    batch_spec = P('data', None, None)

    def per_device(x_loc, g_loc, step_emb, w_q, w_k, w_v, w_o, w_up, w_down):
        d, n_heads, head = w_q.shape
        scale = head ** -0.5
        n_seq, seq, _ = x_loc.shape
        n = n_seq * seq
        wq, wk, wv = (w.transpose(1, 2, 0).reshape(n_heads * head, d) for w in (w_q, w_k, w_v))
        wo = w_o.reshape(n_heads * head, d)
        mask = np.kron(np.eye(4), np.ones((64, 64))).astype(BF16)
        x = x_loc.reshape(n, d)
        saved = []
        for l in range(2):
            xc, u, q, k, v, mix, h, m, mt = attn_fwd(x, step_emb, l, wq, wk, wv, wo, mask, seq, scale, 512)
            z, g, x = mlp_fwd(m, w_up, w_down, h, 1024, 512)
            saved.append((xc, u, q, k, v, mix, h, mt, z, g))
        (_, u0, _, _, _, mix0, h0, mt0, z0, g0), (_, u1, _, _, _, mix1, h1, mt1, z1, g1) = saved

        def attn_back(l, dmid):
            xc, _, q, k, v = saved[l][:5]
            return attn_bwd(dmid, q, k, v, xc, wq, wk, wv, wo, mask, seq, scale, 512)

        do1 = g_loc.reshape(n, d)
        dup1, dmid1 = mlp_bwd(do1, w_up, w_down, z1, h1, 1024, 512)
        dq1, dk1, dv1, do0 = attn_back(1, dmid1)
        s_mlp, dmid0 = mlp_grads((do0, do1), (mt0, mt1), h0, dmid1, (mix0, mix1), z0, (g0, g1), dup1, w_up, w_down, 256, 256)
        n_tiles, n_blocks = w_up.shape[1] // 256, d // 256
        a_mlp = lax.all_gather(s_mlp, 'data')
        dq0, dk0, dv0, d_out = attn_back(0, dmid0)
        s_attn = attn_grads([(dq0, dq1), (dk0, dk1), (dv0, dv1)], (u0, u1), 256)
        a_attn = lax.all_gather(s_attn, 'data')
        g_down, g_up = place_mlp(a_mlp, n_tiles, 256, 2)
        (g_o,) = place_rows(a_mlp, 2 * n_tiles, n_tiles, n_blocks, 1, 5)
        g_q, g_k, g_v = place_rows(a_attn, 0, 0, n_blocks, 3, 6)
        heads = lambda a: a.reshape(n_heads, head, d).transpose(2, 0, 1)
        return heads(g_q), heads(g_k), heads(g_v), g_o.reshape(w_o.shape), g_up, g_down, d_out.reshape(x_loc.shape)

    return jax.shard_map(per_device, mesh=mesh, in_specs=(batch_spec, batch_spec, P(), P(), P(), P(), P(), P(), P()), out_specs=(P(), P(), P(), P(), P(), P(), batch_spec), check_vma=False)
```

```python
import functools
import math

import jax
import jax.numpy as jnp
import numpy as np
from jax import lax
from jax.experimental import pallas as pl
from jax.experimental.pallas import tpu as pltpu
from jax.sharding import PartitionSpec as P


NORM_EPS = 1e-6
GELU_C = math.sqrt(2.0 / math.pi)
GELU_A = 0.044715
BF16 = jnp.bfloat16
F32 = jnp.float32
VMEM_LIMIT = 60 * 1024 * 1024

NN = (((1,), (0,)), ((), ()))
NT = (((1,), (1,)), ((), ()))
TN = (((0,), (0,)), ((), ()))
MESH = pl.DeviceIdType.MESH


def dot(a, b, dims=NN):
    return lax.dot_general(a, b, dims, preferred_element_type=F32)


def rms_scale(x_f32):
    return lax.rsqrt(jnp.mean(x_f32 * x_f32, axis=-1, keepdims=True) + NORM_EPS)


def rms_pull(x_bf16, d_bf16):
    x = x_bf16.astype(F32)
    d = d_bf16.astype(F32)
    r = rms_scale(x)
    dot_dx = jnp.mean(d * x, axis=-1, keepdims=True)
    return (d * r - x * (r * r * r * dot_dx)).astype(BF16)


def gelu_tanh(z):
    return jnp.tanh(GELU_C * (z + GELU_A * (z * z * z)))


def gelu_slope(z):
    t = gelu_tanh(z)
    return 0.5 * (1.0 + t) + (0.5 * z) * ((1.0 - t * t) * (GELU_C * (1.0 + (3.0 * GELU_A) * (z * z))))


def block_diag(a, mask):
    return jnp.concatenate([a, a, a, a], axis=0) * mask


def diag_blocks(full, seq, lane_lo):
    left = jnp.where(lane_lo, full[0:seq, 0:128], full[seq:2 * seq, 0:128])
    right = jnp.where(lane_lo, full[2 * seq:3 * seq, 128:256], full[3 * seq:4 * seq, 128:256])
    return jnp.concatenate([left, right], axis=1)


def softmax_t(scores_t, scale):
    s = scores_t * scale
    e = jnp.exp(s - jnp.max(s, axis=0, keepdims=True))
    return e / jnp.sum(e, axis=0, keepdims=True)


def in_chunks(n, body, rows=32):
    def step(i, _):
        body(pl.ds(pl.multiple_of(i * rows, rows), rows))
        return 0

    lax.fori_loop(0, n // rows, step, 0, unroll=2)


def loads(refs, bufs, sems):
    return [pltpu.make_async_copy(r, b, sems.at[k]) for k, (r, b) in enumerate(zip(refs, bufs))]


def at_step(step, *actions):
    @pl.when(pl.program_id(0) == step)
    def _():
        for act in actions:
            act()


def attn_fwd_kernel(layer, seq, scale, x_ref, e_ref, mask_ref, wq_hbm, wk_hbm, wv_hbm, wo_hbm,
                    xc_ref, u_ref, q_ref, k_ref, v_ref, mix_ref, h_ref, m_ref, mt_ref, wq_ref, wk_ref, wv_ref, wo_ref, sems):
    load = loads((wq_hbm, wk_hbm, wv_hbm, wo_hbm), (wq_ref, wk_ref, wv_ref, wo_ref), sems)
    at_step(0, *(c.start for c in load))
    n_rows = x_ref.shape[0]
    blocks = [pl.ds(r * (n_rows // 2), n_rows // 2) for r in range(2)]
    at_step(0, *(c.wait for c in load))
    for rows in blocks:
        x = (x_ref[rows, :].astype(F32) + e_ref[layer:layer + 1, :].astype(F32)).astype(BF16)
        xc_ref[rows, :] = x
        x_f32 = x.astype(F32)
        u_ref[rows, :] = (x_f32 * rms_scale(x_f32)).astype(BF16)
        for w_ref, o_ref in ((wq_ref, q_ref), (wk_ref, k_ref), (wv_ref, v_ref)):
            o_ref[rows, :] = dot(u_ref[rows, :], w_ref[...], NT).astype(BF16)

    n_groups = x_ref.shape[1] // 256
    lane_lo = lax.broadcasted_iota(jnp.int32, (seq, 128), 1) < 64

    def one_seq(s):
        rows = pl.ds(s * seq, seq)
        cols = [pl.ds(g * 256, 256) for g in range(n_groups)]
        mask = mask_ref[...]
        st = [dot(k_ref[rows, c], block_diag(q_ref[rows, c], mask), NT).astype(BF16).astype(F32) for c in cols]
        pb = [softmax_t(t, scale).astype(BF16) for t in st]
        for c, p in zip(cols, pb):
            mix_ref[rows, c] = diag_blocks(dot(p, v_ref[rows, c], TN), seq, lane_lo).astype(BF16)

    for s in range(x_ref.shape[0] // seq):
        one_seq(s)
    for rows in blocks:
        h = (xc_ref[rows, :].astype(F32) + dot(mix_ref[rows, :], wo_ref[...]).astype(BF16).astype(F32)).astype(BF16)
        h_ref[rows, :] = h
        h_f32 = h.astype(F32)
        m_ref[rows, :] = (h_f32 * rms_scale(h_f32)).astype(BF16)
    mt_ref[...] = m_ref[...].T


def attn_bwd_kernel(seq, scale, dmid_ref, q_ref, k_ref, v_ref, xc_ref, mask_ref, wo_hbm, wq_hbm, wk_hbm, wv_hbm,
                    dq_ref, dk_ref, dv_ref, dprev_ref, dmix_ref, wo_ref, wq_ref, wk_ref, wv_ref, sems):
    load = loads((wo_hbm, wq_hbm, wk_hbm, wv_hbm), (wo_ref, wq_ref, wk_ref, wv_ref), sems)
    at_step(0, *(c.start for c in load), load[0].wait)
    dmix_ref[...] = dot(dmid_ref[...], wo_ref[...], NT).astype(BF16)
    n_groups = xc_ref.shape[1] // 256
    lane_lo = lax.broadcasted_iota(jnp.int32, (seq, 128), 1) < 64

    def one_seq(s, _):
        rows = pl.ds(pl.multiple_of(s * seq, seq), seq)
        cols = [pl.ds(g * 256, 256) for g in range(n_groups)]
        mask = mask_ref[...]
        qbd = [block_diag(q_ref[rows, c], mask) for c in cols]
        dbd = [block_diag(dmix_ref[rows, c], mask) for c in cols]
        st = [dot(k_ref[rows, c], t, NT).astype(BF16).astype(F32) for c, t in zip(cols, qbd)]
        dp = [dot(v_ref[rows, c], t, NT).astype(BF16).astype(F32) for c, t in zip(cols, dbd)]
        p = [softmax_t(t, scale) for t in st]
        for c, a, t in zip(cols, p, dbd):
            dv_ref[rows, c] = dot(a.astype(BF16), t).astype(BF16)
        ds = [((a * (t - jnp.sum(a * t, axis=0, keepdims=True))) * scale).astype(BF16) for a, t in zip(p, dp)]
        for c, a, t in zip(cols, ds, qbd):
            dk_ref[rows, c] = dot(a, t).astype(BF16)
            dq_ref[rows, c] = diag_blocks(dot(a, k_ref[rows, c], TN), seq, lane_lo).astype(BF16)
        return 0

    lax.fori_loop(0, xc_ref.shape[0] // seq, one_seq, 0, unroll=4)
    at_step(0, *(c.wait for c in load[1:]))
    n_rows = xc_ref.shape[0]
    for rows in [pl.ds(r * (n_rows // 2), n_rows // 2) for r in range(2)]:
        du = dot(dq_ref[rows, :], wq_ref[...]) + dot(dk_ref[rows, :], wk_ref[...]) + dot(dv_ref[rows, :], wv_ref[...])
        dx = rms_pull(xc_ref[rows, :], du.astype(BF16))
        dprev_ref[rows, :] = (dmid_ref[rows, :].astype(F32) + dx.astype(F32)).astype(BF16)


def mlp_fwd_kernel(sub, m_ref, wup_ref, wdown_ref, h_hbm, z_ref, g_ref, y_ref, acc_ref, h_ref, sem):
    step = pl.program_id(0)
    load = pltpu.make_async_copy(h_hbm, h_ref, sem)
    at_step(0, load.start)

    @pl.when(step == 0)
    def _():
        acc_ref[...] = jnp.zeros_like(acc_ref)

    for r in range(m_ref.shape[0] // sub):
        rows = pl.ds(r * sub, sub)
        zb = dot(m_ref[rows, :], wup_ref[...]).astype(BF16)
        z_ref[rows, :] = zb
        z = zb.astype(F32)
        g = ((0.5 * z) * (1.0 + gelu_tanh(z))).astype(BF16)
        g_ref[rows, :] = g
        acc_ref[rows, :] += dot(g, wdown_ref[...])

    @pl.when(step == pl.num_programs(0) - 1)
    def _():
        load.wait()

        def finish(rows):
            y = acc_ref[rows, :].astype(BF16)
            y_ref[rows, :] = (h_ref[rows, :].astype(F32) + y.astype(F32)).astype(BF16)

        in_chunks(m_ref.shape[0], finish)


def mlp_bwd_kernel(sub, d_ref, wup_ref, wdown_ref, z_ref, h_hbm, dup_ref, dmid_ref, acc_ref, h_ref, sem):
    step = pl.program_id(0)
    load = pltpu.make_async_copy(h_hbm, h_ref, sem)
    at_step(0, load.start)

    @pl.when(step == 0)
    def _():
        acc_ref[...] = jnp.zeros_like(acc_ref)

    for r in range(d_ref.shape[0] // sub):
        rows = pl.ds(r * sub, sub)
        da = dot(d_ref[rows, :], wdown_ref[...], NT).astype(BF16).astype(F32)
        du = (da * gelu_slope(z_ref[rows, :].astype(F32))).astype(BF16)
        dup_ref[rows, :] = du
        acc_ref[rows, :] += dot(du, wup_ref[...], NT)

    @pl.when(step == pl.num_programs(0) - 1)
    def _():
        load.wait()

        def finish(rows):
            dh = rms_pull(h_ref[rows, :], acc_ref[rows, :].astype(BF16))
            dmid_ref[rows, :] = (d_ref[rows, :].astype(F32) + dh.astype(F32)).astype(BF16)

        in_chunks(d_ref.shape[0], finish)


def params(**kw):
    return pltpu.CompilerParams(dimension_semantics=("arbitrary",), vmem_limit_bytes=VMEM_LIMIT, **kw)


def cost(flops, nbytes, trans=0):
    return pl.CostEstimate(flops=int(flops), bytes_accessed=int(nbytes), transcendentals=int(trans))


def whole(shape):
    return pl.BlockSpec(shape, lambda i: (0,) * len(shape))


def attn_fwd(x, step_emb, layer, wq, wk, wv, wo, mask, seq, scale, tile):
    n, d = x.shape
    row = pl.BlockSpec((tile, d), lambda i: (i, 0))
    return pl.pallas_call(
        functools.partial(attn_fwd_kernel, layer, seq, scale),
        grid=(n // tile,),
        in_specs=[row, whole(step_emb.shape), whole(mask.shape)] + [pl.BlockSpec(memory_space=pl.ANY)] * 4,
        out_specs=[row] * 8 + [pl.BlockSpec((d, tile), lambda i: (0, i))],
        out_shape=[jax.ShapeDtypeStruct((n, d), BF16)] * 8 + [jax.ShapeDtypeStruct((d, n), BF16)],
        scratch_shapes=[pltpu.VMEM(w.shape, BF16) for w in (wq, wk, wv, wo)] + [pltpu.SemaphoreType.DMA((4,))],
        compiler_params=params(),
        cost_estimate=cost(8 * n * d * d, 20 * n * d, n * d),
        name="attn_fwd",
    )(x, step_emb, mask, wq, wk, wv, wo)


def attn_bwd(dmid, q, k, v, xc, wq, wk, wv, wo, mask, seq, scale, tile):
    n, d = xc.shape
    row = pl.BlockSpec((tile, d), lambda i: (i, 0))
    return pl.pallas_call(
        functools.partial(attn_bwd_kernel, seq, scale),
        grid=(n // tile,),
        in_specs=[row] * 5 + [whole(mask.shape)] + [pl.BlockSpec(memory_space=pl.ANY)] * 4,
        out_specs=[row] * 4,
        out_shape=[jax.ShapeDtypeStruct((n, d), BF16)] * 4,
        scratch_shapes=[pltpu.VMEM((tile, d), BF16)] + [pltpu.VMEM(w.shape, BF16) for w in (wo, wq, wk, wv)] + [pltpu.SemaphoreType.DMA((4,))],
        compiler_params=params(),
        cost_estimate=cost(8 * n * d * d, 20 * n * d, n * d),
        name="attn_bwd",
    )(dmid, q, k, v, xc, mask, wo, wq, wk, wv)


def mlp_fwd(m, w_up, w_down, h, tile, sub):
    n, d = m.shape
    f = w_up.shape[1]
    col = pl.BlockSpec((n, tile), lambda i: (0, i))
    return pl.pallas_call(
        functools.partial(mlp_fwd_kernel, sub),
        grid=(f // tile,),
        in_specs=[kept((n, d)), pl.BlockSpec((d, tile), lambda i: (0, i)), pl.BlockSpec((tile, d), lambda i: (i, 0)), pl.BlockSpec(memory_space=pl.ANY)],
        out_specs=[col, col, kept((n, d))],
        out_shape=[jax.ShapeDtypeStruct((n, f), BF16)] * 2 + [jax.ShapeDtypeStruct((n, d), BF16)],
        scratch_shapes=[pltpu.VMEM((n, d), F32), pltpu.VMEM((n, d), BF16), pltpu.SemaphoreType.DMA(())],
        compiler_params=params(),
        cost_estimate=cost(4 * n * d * f, 4 * n * f, n * f),
        name="mlp_fwd",
    )(m, w_up, w_down, h)


def mlp_bwd(d_out, w_up, w_down, z, h, tile, sub):
    n, d = d_out.shape
    f = w_up.shape[1]
    col = pl.BlockSpec((n, tile), lambda i: (0, i))
    return pl.pallas_call(
        functools.partial(mlp_bwd_kernel, sub),
        grid=(f // tile,),
        in_specs=[kept((n, d)), pl.BlockSpec((d, tile), lambda i: (0, i)), pl.BlockSpec((tile, d), lambda i: (i, 0)), col, pl.BlockSpec(memory_space=pl.ANY)],
        out_specs=[col, kept((n, d))],
        out_shape=[jax.ShapeDtypeStruct((n, f), BF16), jax.ShapeDtypeStruct((n, d), BF16)],
        scratch_shapes=[pltpu.VMEM((n, d), F32), pltpu.VMEM((n, d), BF16), pltpu.SemaphoreType.DMA(())],
        compiler_params=params(),
        cost_estimate=cost(4 * n * d * f, 4 * n * f, n * f),
        name="mlp_bwd",
    )(d_out, w_up, w_down, z, h)


def peer_of(me, power):
    return me + power * (1 - 2 * ((me // power) % 2))


def enter_barrier(me):
    barrier = pltpu.get_barrier_semaphore()
    for power in (1, 2, 4, 8):
        pl.semaphore_signal(barrier, inc=1, device_id=(peer_of(me, power),), device_id_type=MESH)
    pl.semaphore_wait(barrier, 4)


def stream_scratch(half, width, slots):
    return [pltpu.VMEM((slots, half // k, width), F32) for k in (1, 2, 4, 8)] + [
        pltpu.SemaphoreType.DMA((4, slots)), pltpu.SemaphoreType.DMA((4, slots))]


def put(ref, value):
    ref[0] = value


def reduce_stage(s, j, shift, half, g_ref, sink, bufs, me):
    h0, h1, h2, h3, send_sem, recv_sem = bufs
    slots = h0.shape[0]
    slot, g = j % slots, g_ref.at[j % g_ref.shape[0]]
    core = me % 2
    powers, bits = [], []
    for k in range(3):
        r = (j + k + shift) % 3
        powers.append(2 + r + r * r)
        bits.append((me // powers[k]) % 2)
    held = (g, h0.at[slot], h1.at[slot], h2.at[slot], h3.at[slot])
    keep = (half * core,) + tuple((half >> (k + 1)) * bits[k] for k in range(3))
    away = (half * (1 - core),) + tuple((half >> (k + 1)) * (1 - bits[k]) for k in range(3))

    def part(ref, start, size):
        return ref.at[pl.ds(pl.multiple_of(start, 8), size)]

    def copy(k):
        peer = peer_of(me, 1) if k == 0 else peer_of(me, powers[k - 1])
        return pltpu.make_async_remote_copy(
            src_ref=part(held[k], away[k], half >> k), dst_ref=held[k + 1], send_sem=send_sem.at[k, slot],
            recv_sem=recv_sem.at[k, slot], device_id=(peer,), device_id_type=MESH)

    if s > 0:
        before = copy(s - 1)
        before.wait_recv()
        before.wait_send()
        own = held[s - 1][pl.ds(pl.multiple_of(keep[s - 1], 8), half >> (s - 1)), :]
        if s == 4:
            sink(j, held[4][...] + own)
        else:
            held[s][...] = held[s][...] + own
    if s < 4:
        copy(s).start()


def reduce_step(i, lags, streams, me):
    for n, *stream in streams:
        for s in (4, 3, 2, 1, 0):
            j = i - lags[s]

            @pl.when((j >= 0) & (j < n))
            def _():
                reduce_stage(s, j, *stream, me)


def mlp_grads_kernel(n, lags, sub, d0_hbm, d1_hbm, m0t_hbm, m1t_hbm, z_ref, g0_ref, g1_ref, dup1_ref, wdown_ref,
                     share_ref, du_ref, gd_ref, gu_ref, d0_ref, d1_ref, m0t_ref, m1t_ref, sems, *bufs):
    me = lax.axis_index('data')
    i = pl.program_id(0)
    load = loads((d0_hbm, d1_hbm, m0t_hbm, m1t_hbm), (d0_ref, d1_ref, m0t_ref, m1t_ref), sems)

    @pl.when(i == 0)
    def _():
        for c in load:
            c.start()
        enter_barrier(me)
        for c in load:
            c.wait()

    @pl.when(i < n)
    def _():
        gd_ref[i % 2] = dot(g0_ref[...], d0_ref[...], TN) + dot(g1_ref[...], d1_ref[...], TN)
        for r in range(d0_ref.shape[0] // sub):
            rows = pl.ds(r * sub, sub)
            da = dot(d0_ref[rows, :], wdown_ref[...], NT).astype(BF16).astype(F32)
            du_ref[rows, :] = (da * gelu_slope(z_ref[rows, :].astype(F32))).astype(BF16)
        gu_ref[i % 2] = dot(m0t_ref[...], du_ref[...]) + dot(m1t_ref[...], dup1_ref[...])

    def share_up(j, share):
        piece, width = share_ref.shape[1], share.shape[1]
        for k in range(share.shape[0] // piece):
            share_ref[1, :, k * width:(k + 1) * width] = share[k * piece:(k + 1) * piece, :]

    reduce_step(i, lags, ((n, 0, gd_ref.shape[1] // 2, gd_ref, lambda j, share: put(share_ref, share), bufs[:6]),
                          (n, 2, gu_ref.shape[1] // 2, gu_ref, share_up, bufs[6:])), me)


def mlp_back_kernel(sub, du_ref, wup_ref, d_hbm, h_hbm, dmid_ref, acc_ref, d_ref, h_ref, sems):
    step = pl.program_id(0)
    load = loads((d_hbm, h_hbm), (d_ref, h_ref), sems)
    at_step(0, *(c.start for c in load))

    @pl.when(step == 0)
    def _():
        acc_ref[...] = jnp.zeros_like(acc_ref)

    for r in range(du_ref.shape[0] // sub):
        rows = pl.ds(r * sub, sub)
        acc_ref[rows, :] += dot(du_ref[rows, :], wup_ref[...], NT)

    @pl.when(step == pl.num_programs(0) - 1)
    def _():
        for c in load:
            c.wait()

        def finish(rows):
            dh = rms_pull(h_ref[rows, :], acc_ref[rows, :].astype(BF16))
            dmid_ref[rows, :] = (d_ref[rows, :].astype(F32) + dh.astype(F32)).astype(BF16)

        in_chunks(d_ref.shape[0], finish)


def attn_grads_kernel(n, lags, *refs):
    xs, (u0, u1, m0, m1), out_ref, g_ref, bufs = refs[:8], refs[8:12], refs[12], refs[13], refs[14:]
    me = lax.axis_index('data')
    i = pl.program_id(0)

    @pl.when(i == 0)
    def _():
        enter_barrier(me)

    per = n // 4
    for w in range(4):
        @pl.when((i >= w * per) & (i < (w + 1) * per))
        def _():
            y0, y1 = (u0, u1) if w < 3 else (m0, m1)
            g_ref[i % 4] = dot(xs[2 * w][...], y0[...], TN) + dot(xs[2 * w + 1][...], y1[...], TN)

    reduce_step(i, lags, ((n, 0, g_ref.shape[1] // 2, g_ref, lambda j, share: put(out_ref, share), bufs),), me)


MLP_LAGS, MLP_SLOTS = (0, 1, 3, 4, 5), 6
ATTN_LAGS, ATTN_SLOTS = (0, 2, 4, 6, 8), 8


def kept(shape):
    return pl.BlockSpec(shape, lambda i: (0,) * len(shape), pipeline_mode=pl.Buffered(1))


def mlp_grads(ds, mts, z, gs, dup1, w_down, tile, sub):
    rows, d = ds[0].shape
    n = w_down.shape[0] // tile
    at = lambda i: jnp.minimum(i, n - 1)
    col = pl.BlockSpec((rows, tile), lambda i: (0, at(i)))
    anywhere = pl.BlockSpec(memory_space=pl.ANY)
    piece = tile // 16
    return pl.pallas_call(
        functools.partial(mlp_grads_kernel, n, MLP_LAGS, sub),
        grid=(n + MLP_LAGS[4],),
        in_specs=[anywhere] * 4 + [col] * 4 + [pl.BlockSpec((tile, d), lambda i: (at(i), 0))],
        out_specs=[pl.BlockSpec((2, piece, d), lambda i: (jnp.maximum(i - MLP_LAGS[4], 0), 0, 0)), col],
        out_shape=[jax.ShapeDtypeStruct((2 * n, piece, d), F32), jax.ShapeDtypeStruct((rows, n * tile), BF16)],
        scratch_shapes=[pltpu.VMEM((2, tile, d), F32), pltpu.VMEM((2, d, tile), F32)] + [pltpu.VMEM(a.shape, BF16) for a in (*ds, *mts)] + [
            pltpu.SemaphoreType.DMA((4,))] + stream_scratch(tile // 2, d, MLP_SLOTS) + stream_scratch(d // 2, tile, MLP_SLOTS),
        compiler_params=pltpu.CompilerParams(dimension_semantics=("arbitrary",), collective_id=0, has_side_effects=True,
                                             vmem_limit_bytes=VMEM_LIMIT),
        cost_estimate=cost(10 * rows * d * n * tile, 10 * rows * n * tile),
        name="mlp_grads",
    )(*ds, *mts, z, *gs, dup1, w_down)


def mlp_back(du, w_up, d_out, h, tile, sub):
    n, d = d_out.shape
    f = w_up.shape[1]
    anywhere = pl.BlockSpec(memory_space=pl.ANY)
    return pl.pallas_call(
        functools.partial(mlp_back_kernel, sub),
        grid=(f // tile,),
        in_specs=[pl.BlockSpec((n, tile), lambda i: (0, i)), pl.BlockSpec((d, tile), lambda i: (0, i)), anywhere, anywhere],
        out_specs=kept((n, d)),
        out_shape=jax.ShapeDtypeStruct((n, d), BF16),
        scratch_shapes=[pltpu.VMEM((n, d), F32), pltpu.VMEM((n, d), BF16), pltpu.VMEM((n, d), BF16), pltpu.SemaphoreType.DMA((2,))],
        compiler_params=params(),
        cost_estimate=cost(2 * n * d * f, 2 * n * f),
        name="mlp_back",
    )(du, w_up, d_out, h)


def attn_grads(xs, ys, tile):
    rows, d = ys[0].shape
    per = d // tile
    n = 4 * per
    cols = [pl.BlockSpec((rows, tile), lambda i, w=w: (0, jnp.clip(i - w * per, 0, per - 1))) for w in range(4) for _ in range(2)]
    return pl.pallas_call(
        functools.partial(attn_grads_kernel, n, ATTN_LAGS),
        grid=(n + ATTN_LAGS[4],),
        in_specs=cols + [kept((rows, d))] * 4,
        out_specs=pl.BlockSpec((1, tile // 16, d), lambda i: (jnp.maximum(i - ATTN_LAGS[4], 0), 0, 0)),
        out_shape=jax.ShapeDtypeStruct((n, tile // 16, d), F32),
        scratch_shapes=[pltpu.VMEM((4, tile, d), F32)] + stream_scratch(tile // 2, d, ATTN_SLOTS),
        compiler_params=pltpu.CompilerParams(dimension_semantics=("arbitrary",), collective_id=1, has_side_effects=True,
                                             vmem_limit_bytes=VMEM_LIMIT),
        cost_estimate=cost(16 * rows * d * d, 24 * rows * d),
        name="attn_grads",
    )(*[x for pair in xs for x in pair], *ys)


def put_in_place(j, shift, in_ref, out_ref, bands):
    half = out_ref.shape[0] // 2
    piece, width = in_ref.shape[1], out_ref.shape[1]

    def variant(v):
        for dev in range(16):
            bits = [(dev >> (1 + (v + k) % 3)) & 1 for k in range(3)]
            at = half * (dev & 1) + sum((half >> (k + 1)) * bits[k] for k in range(3))
            for k in range(bands):
                out_ref[at + k * piece:at + (k + 1) * piece, :] = in_ref[dev, :, k * width:(k + 1) * width]

    if isinstance(j, int):
        variant((j + shift) % 3)
    else:
        for v in range(3):
            pl.when((j + shift) % 3 == v)(functools.partial(variant, v))


def place_mlp_kernel(group, in_ref, down_ref, up_ref):
    high, width = down_ref.shape[0] // group, up_ref.shape[1] // group
    for c in range(group):
        j = pl.program_id(0) * group + c
        put_in_place(j, 0, in_ref.at[:, 2 * c], down_ref.at[pl.ds(c * high, high)], 1)
        put_in_place(j, 2, in_ref.at[:, 2 * c + 1], up_ref.at[:, pl.ds(c * width, width)], up_ref.shape[0] // (16 * in_ref.shape[2]))


def place_mlp(shares, n, tile, group):
    _, _, piece, d = shares.shape
    return pl.pallas_call(
        functools.partial(place_mlp_kernel, group),
        grid=(n // group,),
        in_specs=[pl.BlockSpec((16, 2 * group, piece, d), lambda i: (0, i, 0, 0))],
        out_specs=[pl.BlockSpec((group * tile, d), lambda i: (i, 0)), pl.BlockSpec((d, group * tile), lambda i: (0, i))],
        out_shape=[jax.ShapeDtypeStruct((n * tile, d), F32), jax.ShapeDtypeStruct((d, n * tile), F32)],
        compiler_params=params(),
        cost_estimate=cost(shares.size // 2, 8 * shares.size),
        name="place_mlp",
    )(shares)


def place_rows_kernel(first, turn, per, in_ref, *refs):
    outs, (in_buf, out_buf, in_sem, out_sem) = refs[:-4], refs[-4:]
    depth, high = in_buf.shape[0], out_buf.shape[1]
    total = per * len(outs)

    def fetch(t):
        return pltpu.make_async_copy(in_ref.at[:, first + t], in_buf.at[t % depth], in_sem.at[t % depth])

    def store(t):
        at = t % per * high
        return pltpu.make_async_copy(out_buf.at[t % depth], outs[t // per].at[pl.ds(at, high)], out_sem.at[t % depth])

    for t in range(min(depth, total)):
        fetch(t).start()
    for t in range(total):
        fetch(t).wait()
        if t >= depth:
            store(t - depth).wait()
        put_in_place(turn + t, 0, in_buf.at[t % depth], out_buf.at[t % depth], 1)
        store(t).start()
        if t + depth < total:
            fetch(t + depth).start()
    for t in range(max(total - depth, 0), total):
        store(t).wait()


def place_rows(shares, first, turn, per, n_out, depth):
    _, _, piece, d = shares.shape
    anywhere = pl.BlockSpec(memory_space=pl.ANY)
    return pl.pallas_call(
        functools.partial(place_rows_kernel, first, turn, per),
        in_specs=[anywhere],
        out_specs=[anywhere] * n_out,
        out_shape=[jax.ShapeDtypeStruct((per * 16 * piece, d), F32)] * n_out,
        scratch_shapes=[pltpu.VMEM((depth, 16, piece, d), F32), pltpu.VMEM((depth, 16 * piece, d), F32),
                        pltpu.SemaphoreType.DMA((depth,)), pltpu.SemaphoreType.DMA((depth,))],
        compiler_params=pltpu.CompilerParams(vmem_limit_bytes=VMEM_LIMIT),
        cost_estimate=cost(per * n_out * piece * d * 16, per * n_out * piece * d * 128),
        name="place_rows",
    )(shares)


def solution(mesh):
    batch_spec = P('data', None, None)

    def per_device(x_loc, g_loc, step_emb, w_q, w_k, w_v, w_o, w_up, w_down):
        d, n_heads, head = w_q.shape
        scale = head ** -0.5
        n_seq, seq, _ = x_loc.shape
        n = n_seq * seq
        wq, wk, wv = (w.transpose(1, 2, 0).reshape(n_heads * head, d) for w in (w_q, w_k, w_v))
        wo = w_o.reshape(n_heads * head, d)
        mask = np.kron(np.eye(4), np.ones((64, 64))).astype(BF16)
        x = x_loc.reshape(n, d)
        saved = []
        for l in range(2):
            xc, u, q, k, v, mix, h, m, mt = attn_fwd(x, step_emb, l, wq, wk, wv, wo, mask, seq, scale, 512)
            z, g, x = mlp_fwd(m, w_up, w_down, h, 1024, 512)
            saved.append((xc, u, q, k, v, mix, h, mt, z, g))
        (_, u0, _, _, _, mix0, h0, mt0, z0, g0), (_, u1, _, _, _, mix1, h1, mt1, z1, g1) = saved

        def attn_back(l, dmid):
            xc, _, q, k, v = saved[l][:5]
            return attn_bwd(dmid, q, k, v, xc, wq, wk, wv, wo, mask, seq, scale, 512)

        do1 = g_loc.reshape(n, d)
        dup1, dmid1 = mlp_bwd(do1, w_up, w_down, z1, h1, 1024, 512)
        dq1, dk1, dv1, do0 = attn_back(1, dmid1)
        s_mlp, dup0 = mlp_grads((do0, do1), (mt0, mt1), z0, (g0, g1), dup1, w_down, 256, 256)
        n_tiles, n_blocks = w_up.shape[1] // 256, d // 256
        a_mlp = lax.all_gather(s_mlp, 'data')
        dmid0 = mlp_back(dup0, w_up, do0, h0, 1024, 512)
        dq0, dk0, dv0, d_out = attn_back(0, dmid0)
        s_attn = attn_grads([(dq0, dq1), (dk0, dk1), (dv0, dv1), (mix0, mix1)], (u0, u1, dmid0, dmid1), 256)
        a_attn = lax.all_gather(s_attn, 'data')
        g_down, g_up = place_mlp(a_mlp, n_tiles, 256, 2)
        g_q, g_k, g_v, g_o = place_rows(a_attn, 0, 0, n_blocks, 4, 6)
        heads = lambda a: a.reshape(n_heads, head, d).transpose(2, 0, 1)
        return heads(g_q), heads(g_k), heads(g_v), g_o.reshape(w_o.shape), g_up, g_down, d_out.reshape(x_loc.shape)

    return jax.shard_map(per_device, mesh=mesh, in_specs=(batch_spec, batch_spec, P(), P(), P(), P(), P(), P(), P()), out_specs=(P(), P(), P(), P(), P(), P(), batch_spec), check_vma=False)
```

```python
import functools
import math

import jax
import jax.numpy as jnp
import numpy as np
from jax import lax
from jax.experimental import pallas as pl
from jax.experimental.pallas import tpu as pltpu
from jax.sharding import PartitionSpec as P


NORM_EPS = 1e-6
GELU_C = math.sqrt(2.0 / math.pi)
GELU_A = 0.044715
BF16 = jnp.bfloat16
F32 = jnp.float32
VMEM_LIMIT = 60 * 1024 * 1024

NN = (((1,), (0,)), ((), ()))
NT = (((1,), (1,)), ((), ()))
TN = (((0,), (0,)), ((), ()))
MESH = pl.DeviceIdType.MESH


def dot(a, b, dims=NN):
    return lax.dot_general(a, b, dims, preferred_element_type=F32)


def rms_scale(x_f32):
    return lax.rsqrt(jnp.mean(x_f32 * x_f32, axis=-1, keepdims=True) + NORM_EPS)


def rms_pull(x_bf16, d_bf16):
    x = x_bf16.astype(F32)
    d = d_bf16.astype(F32)
    r = rms_scale(x)
    dot_dx = jnp.mean(d * x, axis=-1, keepdims=True)
    return (d * r - x * (r * r * r * dot_dx)).astype(BF16)


def gelu_tanh(z):
    return jnp.tanh(GELU_C * (z + GELU_A * (z * z * z)))


def gelu_slope(z, t):
    return 0.5 * (1.0 + t) + (0.5 * z) * ((1.0 - t * t) * (GELU_C * (1.0 + (3.0 * GELU_A) * (z * z))))


def block_diag(a, mask):
    return jnp.concatenate([a, a, a, a], axis=0) * mask


def diag_blocks(full, seq, lane_lo):
    left = jnp.where(lane_lo, full[0:seq, 0:128], full[seq:2 * seq, 0:128])
    right = jnp.where(lane_lo, full[2 * seq:3 * seq, 128:256], full[3 * seq:4 * seq, 128:256])
    return jnp.concatenate([left, right], axis=1)


def softmax_t(scores_t, scale):
    s = scores_t * scale
    e = jnp.exp(s - jnp.max(s, axis=0, keepdims=True))
    return e / jnp.sum(e, axis=0, keepdims=True)


def in_chunks(n, body, rows=32):
    def step(i, _):
        body(pl.ds(pl.multiple_of(i * rows, rows), rows))
        return 0

    lax.fori_loop(0, n // rows, step, 0, unroll=2)


def loads(refs, bufs, sems):
    return [pltpu.make_async_copy(r, b, sems.at[k]) for k, (r, b) in enumerate(zip(refs, bufs))]


def at_step(step, *actions):
    @pl.when(pl.program_id(0) == step)
    def _():
        for act in actions:
            act()


def attn_fwd_kernel(layer, seq, scale, x_ref, e_ref, mask_ref, wq_hbm, wk_hbm, wv_hbm, wo_hbm,
                    xc_ref, u_ref, q_ref, k_ref, v_ref, mix_ref, h_ref, m_ref, mt_ref, wq_ref, wk_ref, wv_ref, wo_ref, sems):
    load = loads((wq_hbm, wk_hbm, wv_hbm, wo_hbm), (wq_ref, wk_ref, wv_ref, wo_ref), sems)
    at_step(0, *(c.start for c in load))
    n_rows = x_ref.shape[0]
    blocks = [pl.ds(r * (n_rows // 2), n_rows // 2) for r in range(2)]
    at_step(0, *(c.wait for c in load))
    for rows in blocks:
        x = (x_ref[rows, :].astype(F32) + e_ref[layer:layer + 1, :].astype(F32)).astype(BF16)
        xc_ref[rows, :] = x
        x_f32 = x.astype(F32)
        u_ref[rows, :] = (x_f32 * rms_scale(x_f32)).astype(BF16)
        for w_ref, o_ref in ((wq_ref, q_ref), (wk_ref, k_ref), (wv_ref, v_ref)):
            o_ref[rows, :] = dot(u_ref[rows, :], w_ref[...], NT).astype(BF16)

    n_groups = x_ref.shape[1] // 256
    lane_lo = lax.broadcasted_iota(jnp.int32, (seq, 128), 1) < 64

    def one_seq(s):
        rows = pl.ds(s * seq, seq)
        cols = [pl.ds(g * 256, 256) for g in range(n_groups)]
        mask = mask_ref[...]
        st = [dot(k_ref[rows, c], block_diag(q_ref[rows, c], mask), NT).astype(BF16).astype(F32) for c in cols]
        pb = [softmax_t(t, scale).astype(BF16) for t in st]
        for c, p in zip(cols, pb):
            mix_ref[rows, c] = diag_blocks(dot(p, v_ref[rows, c], TN), seq, lane_lo).astype(BF16)

    for s in range(x_ref.shape[0] // seq):
        one_seq(s)
    for rows in blocks:
        h = (xc_ref[rows, :].astype(F32) + dot(mix_ref[rows, :], wo_ref[...]).astype(BF16).astype(F32)).astype(BF16)
        h_ref[rows, :] = h
        h_f32 = h.astype(F32)
        m_ref[rows, :] = (h_f32 * rms_scale(h_f32)).astype(BF16)
    mt_ref[...] = m_ref[...].T


def attn_bwd_kernel(seq, scale, dmid_ref, q_ref, k_ref, v_ref, xc_ref, mask_ref, wo_hbm, wq_hbm, wk_hbm, wv_hbm,
                    dq_ref, dk_ref, dv_ref, dprev_ref, dmix_ref, wo_ref, wq_ref, wk_ref, wv_ref, sems):
    load = loads((wo_hbm, wq_hbm, wk_hbm, wv_hbm), (wo_ref, wq_ref, wk_ref, wv_ref), sems)
    at_step(0, *(c.start for c in load), load[0].wait)
    dmix_ref[...] = dot(dmid_ref[...], wo_ref[...], NT).astype(BF16)
    n_groups = xc_ref.shape[1] // 256
    lane_lo = lax.broadcasted_iota(jnp.int32, (seq, 128), 1) < 64

    def one_seq(s, _):
        rows = pl.ds(pl.multiple_of(s * seq, seq), seq)
        cols = [pl.ds(g * 256, 256) for g in range(n_groups)]
        mask = mask_ref[...]
        qbd = [block_diag(q_ref[rows, c], mask) for c in cols]
        dbd = [block_diag(dmix_ref[rows, c], mask) for c in cols]
        st = [dot(k_ref[rows, c], t, NT).astype(BF16).astype(F32) for c, t in zip(cols, qbd)]
        dp = [dot(v_ref[rows, c], t, NT).astype(BF16).astype(F32) for c, t in zip(cols, dbd)]
        p = [softmax_t(t, scale) for t in st]
        for c, a, t in zip(cols, p, dbd):
            dv_ref[rows, c] = dot(a.astype(BF16), t).astype(BF16)
        ds = [((a * (t - jnp.sum(a * t, axis=0, keepdims=True))) * scale).astype(BF16) for a, t in zip(p, dp)]
        for c, a, t in zip(cols, ds, qbd):
            dk_ref[rows, c] = dot(a, t).astype(BF16)
            dq_ref[rows, c] = diag_blocks(dot(a, k_ref[rows, c], TN), seq, lane_lo).astype(BF16)
        return 0

    lax.fori_loop(0, xc_ref.shape[0] // seq, one_seq, 0, unroll=4)
    at_step(0, *(c.wait for c in load[1:]))
    n_rows = xc_ref.shape[0]
    for rows in [pl.ds(r * (n_rows // 2), n_rows // 2) for r in range(2)]:
        du = dot(dq_ref[rows, :], wq_ref[...]) + dot(dk_ref[rows, :], wk_ref[...]) + dot(dv_ref[rows, :], wv_ref[...])
        dx = rms_pull(xc_ref[rows, :], du.astype(BF16))
        dprev_ref[rows, :] = (dmid_ref[rows, :].astype(F32) + dx.astype(F32)).astype(BF16)


def mlp_fwd_kernel(sub, m_ref, wup_ref, wdown_ref, h_hbm, z_ref, g_ref, y_ref, acc_ref, h_ref, sem):
    step = pl.program_id(0)
    load = pltpu.make_async_copy(h_hbm, h_ref, sem)
    at_step(0, load.start)

    @pl.when(step == 0)
    def _():
        acc_ref[...] = jnp.zeros_like(acc_ref)

    for r in range(m_ref.shape[0] // sub):
        rows = pl.ds(r * sub, sub)
        zb = dot(m_ref[rows, :], wup_ref[...]).astype(BF16)
        z_ref[rows, :] = zb
        z = zb.astype(F32)
        g = ((0.5 * z) * (1.0 + gelu_tanh(z))).astype(BF16)
        g_ref[rows, :] = g
        acc_ref[rows, :] += dot(g, wdown_ref[...])

    @pl.when(step == pl.num_programs(0) - 1)
    def _():
        load.wait()

        def finish(rows):
            y = acc_ref[rows, :].astype(BF16)
            y_ref[rows, :] = (h_ref[rows, :].astype(F32) + y.astype(F32)).astype(BF16)

        in_chunks(m_ref.shape[0], finish)


def mlp_last_kernel(sub, m_ref, d_ref, wup_ref, wdown_ref, h_hbm, g_ref, dup_ref, dmid_ref, acc_ref, h_ref, sem):
    step = pl.program_id(0)
    load = pltpu.make_async_copy(h_hbm, h_ref, sem)
    at_step(0, load.start)

    @pl.when(step == 0)
    def _():
        acc_ref[...] = jnp.zeros_like(acc_ref)

    for r in range(d_ref.shape[0] // sub):
        rows = pl.ds(r * sub, sub)
        z = dot(m_ref[rows, :], wup_ref[...]).astype(BF16).astype(F32)
        t = gelu_tanh(z)
        g_ref[rows, :] = ((0.5 * z) * (1.0 + t)).astype(BF16)
        da = dot(d_ref[rows, :], wdown_ref[...], NT).astype(BF16).astype(F32)
        dup_ref[rows, :] = (da * gelu_slope(z, t)).astype(BF16)
        acc_ref[rows, :] += dot(dup_ref[rows, :], wup_ref[...], NT)

    @pl.when(step == pl.num_programs(0) - 1)
    def _():
        load.wait()

        def finish(rows):
            dh = rms_pull(h_ref[rows, :], acc_ref[rows, :].astype(BF16))
            dmid_ref[rows, :] = (d_ref[rows, :].astype(F32) + dh.astype(F32)).astype(BF16)

        in_chunks(d_ref.shape[0], finish)


def params(**kw):
    return pltpu.CompilerParams(dimension_semantics=("arbitrary",), vmem_limit_bytes=VMEM_LIMIT, **kw)


def cost(flops, nbytes, trans=0):
    return pl.CostEstimate(flops=int(flops), bytes_accessed=int(nbytes), transcendentals=int(trans))


def whole(shape):
    return pl.BlockSpec(shape, lambda i: (0,) * len(shape))


def attn_fwd(x, step_emb, layer, wq, wk, wv, wo, mask, seq, scale, tile):
    n, d = x.shape
    row = pl.BlockSpec((tile, d), lambda i: (i, 0))
    return pl.pallas_call(
        functools.partial(attn_fwd_kernel, layer, seq, scale),
        grid=(n // tile,),
        in_specs=[row, whole(step_emb.shape), whole(mask.shape)] + [pl.BlockSpec(memory_space=pl.ANY)] * 4,
        out_specs=[row] * 8 + [pl.BlockSpec((d, tile), lambda i: (0, i))],
        out_shape=[jax.ShapeDtypeStruct((n, d), BF16)] * 8 + [jax.ShapeDtypeStruct((d, n), BF16)],
        scratch_shapes=[pltpu.VMEM(w.shape, BF16) for w in (wq, wk, wv, wo)] + [pltpu.SemaphoreType.DMA((4,))],
        compiler_params=params(),
        cost_estimate=cost(8 * n * d * d, 20 * n * d, n * d),
        name="attn_fwd",
    )(x, step_emb, mask, wq, wk, wv, wo)


def attn_bwd(dmid, q, k, v, xc, wq, wk, wv, wo, mask, seq, scale, tile):
    n, d = xc.shape
    row = pl.BlockSpec((tile, d), lambda i: (i, 0))
    return pl.pallas_call(
        functools.partial(attn_bwd_kernel, seq, scale),
        grid=(n // tile,),
        in_specs=[row] * 5 + [whole(mask.shape)] + [pl.BlockSpec(memory_space=pl.ANY)] * 4,
        out_specs=[row] * 4,
        out_shape=[jax.ShapeDtypeStruct((n, d), BF16)] * 4,
        scratch_shapes=[pltpu.VMEM((tile, d), BF16)] + [pltpu.VMEM(w.shape, BF16) for w in (wo, wq, wk, wv)] + [pltpu.SemaphoreType.DMA((4,))],
        compiler_params=params(),
        cost_estimate=cost(8 * n * d * d, 20 * n * d, n * d),
        name="attn_bwd",
    )(dmid, q, k, v, xc, mask, wo, wq, wk, wv)


def mlp_fwd(m, w_up, w_down, h, tile, sub):
    n, d = m.shape
    f = w_up.shape[1]
    col = pl.BlockSpec((n, tile), lambda i: (0, i))
    return pl.pallas_call(
        functools.partial(mlp_fwd_kernel, sub),
        grid=(f // tile,),
        in_specs=[kept((n, d)), pl.BlockSpec((d, tile), lambda i: (0, i)), pl.BlockSpec((tile, d), lambda i: (i, 0)), pl.BlockSpec(memory_space=pl.ANY)],
        out_specs=[col, col, kept((n, d))],
        out_shape=[jax.ShapeDtypeStruct((n, f), BF16)] * 2 + [jax.ShapeDtypeStruct((n, d), BF16)],
        scratch_shapes=[pltpu.VMEM((n, d), F32), pltpu.VMEM((n, d), BF16), pltpu.SemaphoreType.DMA(())],
        compiler_params=params(),
        cost_estimate=cost(4 * n * d * f, 4 * n * f, n * f),
        name="mlp_fwd",
    )(m, w_up, w_down, h)


def mlp_last(m, d_out, w_up, w_down, h, tile, sub):
    n, d = d_out.shape
    f = w_up.shape[1]
    col = pl.BlockSpec((n, tile), lambda i: (0, i))
    return pl.pallas_call(
        functools.partial(mlp_last_kernel, sub),
        grid=(f // tile,),
        in_specs=[kept((n, d)), kept((n, d)), pl.BlockSpec((d, tile), lambda i: (0, i)), pl.BlockSpec((tile, d), lambda i: (i, 0)),
                  pl.BlockSpec(memory_space=pl.ANY)],
        out_specs=[col, col, kept((n, d))],
        out_shape=[jax.ShapeDtypeStruct((n, f), BF16)] * 2 + [jax.ShapeDtypeStruct((n, d), BF16)],
        scratch_shapes=[pltpu.VMEM((n, d), F32), pltpu.VMEM((n, d), BF16), pltpu.SemaphoreType.DMA(())],
        compiler_params=params(),
        cost_estimate=cost(6 * n * d * f, 4 * n * f, n * f),
        name="mlp_last",
    )(m, d_out, w_up, w_down, h)


def peer_of(me, power):
    return me + power * (1 - 2 * ((me // power) % 2))


def enter_barrier(me):
    barrier = pltpu.get_barrier_semaphore()
    for power in (1, 2, 4, 8):
        pl.semaphore_signal(barrier, inc=1, device_id=(peer_of(me, power),), device_id_type=MESH)
    pl.semaphore_wait(barrier, 4)


def stream_scratch(half, width, slots):
    return [pltpu.VMEM((slots, half // k, width), F32) for k in (1, 2, 4, 8)] + [
        pltpu.SemaphoreType.DMA((4, slots)), pltpu.SemaphoreType.DMA((4, slots))]


def put(ref, value):
    ref[0] = value


def reduce_stage(s, j, shift, half, g_ref, sink, bufs, me):
    h0, h1, h2, h3, send_sem, recv_sem = bufs
    slots = h0.shape[0]
    slot, g = j % slots, g_ref.at[j % g_ref.shape[0]]
    core = me % 2
    powers, bits = [], []
    for k in range(3):
        r = (j + k + shift) % 3
        powers.append(2 + r + r * r)
        bits.append((me // powers[k]) % 2)
    held = (g, h0.at[slot], h1.at[slot], h2.at[slot], h3.at[slot])
    keep = (half * core,) + tuple((half >> (k + 1)) * bits[k] for k in range(3))
    away = (half * (1 - core),) + tuple((half >> (k + 1)) * (1 - bits[k]) for k in range(3))

    def part(ref, start, size):
        return ref.at[pl.ds(pl.multiple_of(start, 8), size)]

    def copy(k):
        peer = peer_of(me, 1) if k == 0 else peer_of(me, powers[k - 1])
        return pltpu.make_async_remote_copy(
            src_ref=part(held[k], away[k], half >> k), dst_ref=held[k + 1], send_sem=send_sem.at[k, slot],
            recv_sem=recv_sem.at[k, slot], device_id=(peer,), device_id_type=MESH)

    if s > 0:
        before = copy(s - 1)
        before.wait_recv()
        before.wait_send()
        own = held[s - 1][pl.ds(pl.multiple_of(keep[s - 1], 8), half >> (s - 1)), :]
        if s == 4:
            sink(j, held[4][...] + own)
        else:
            held[s][...] = held[s][...] + own
    if s < 4:
        copy(s).start()


def reduce_step(i, lags, streams, me):
    for n, *stream in streams:
        for s in (4, 3, 2, 1, 0):
            j = i - lags[s]

            @pl.when((j >= 0) & (j < n))
            def _():
                reduce_stage(s, j, *stream, me)


def mlp_grads_kernel(n, lags, sub, d0_hbm, d1_hbm, m0t_hbm, m1t_hbm, z_ref, g0_ref, g1_ref, dup1_ref, wdown_ref,
                     share_ref, du_ref, gd_ref, gu_ref, d0_ref, d1_ref, m0t_ref, m1t_ref, sems, *bufs):
    me = lax.axis_index('data')
    i = pl.program_id(0)
    load = loads((d0_hbm, d1_hbm, m0t_hbm, m1t_hbm), (d0_ref, d1_ref, m0t_ref, m1t_ref), sems)

    @pl.when(i == 0)
    def _():
        for c in load:
            c.start()
        enter_barrier(me)
        for c in load:
            c.wait()

    @pl.when(i < n)
    def _():
        gd_ref[i % 2] = dot(g0_ref[...], d0_ref[...], TN) + dot(g1_ref[...], d1_ref[...], TN)
        for r in range(d0_ref.shape[0] // sub):
            rows = pl.ds(r * sub, sub)
            da = dot(d0_ref[rows, :], wdown_ref[...], NT).astype(BF16).astype(F32)
            z = z_ref[rows, :].astype(F32)
            du_ref[rows, :] = (da * gelu_slope(z, gelu_tanh(z))).astype(BF16)
        gu_ref[i % 2] = dot(m0t_ref[...], du_ref[...]) + dot(m1t_ref[...], dup1_ref[...])

    def share_up(j, share):
        piece, width = share_ref.shape[1], share.shape[1]
        for k in range(share.shape[0] // piece):
            share_ref[1, :, k * width:(k + 1) * width] = share[k * piece:(k + 1) * piece, :]

    reduce_step(i, lags, ((n, 0, gd_ref.shape[1] // 2, gd_ref, lambda j, share: put(share_ref, share), bufs[:6]),
                          (n, 2, gu_ref.shape[1] // 2, gu_ref, share_up, bufs[6:])), me)


def mlp_back_kernel(sub, du_ref, wup_ref, d_hbm, h_hbm, dmid_ref, acc_ref, d_ref, h_ref, sems):
    step = pl.program_id(0)
    load = loads((d_hbm, h_hbm), (d_ref, h_ref), sems)
    at_step(0, *(c.start for c in load))

    @pl.when(step == 0)
    def _():
        acc_ref[...] = jnp.zeros_like(acc_ref)

    for r in range(du_ref.shape[0] // sub):
        rows = pl.ds(r * sub, sub)
        acc_ref[rows, :] += dot(du_ref[rows, :], wup_ref[...], NT)

    @pl.when(step == pl.num_programs(0) - 1)
    def _():
        for c in load:
            c.wait()

        def finish(rows):
            dh = rms_pull(h_ref[rows, :], acc_ref[rows, :].astype(BF16))
            dmid_ref[rows, :] = (d_ref[rows, :].astype(F32) + dh.astype(F32)).astype(BF16)

        in_chunks(d_ref.shape[0], finish)


def attn_grads_kernel(n, lags, *refs):
    xs, (u0, u1, m0, m1), out_ref, g_ref, bufs = refs[:8], refs[8:12], refs[12], refs[13], refs[14:]
    me = lax.axis_index('data')
    i = pl.program_id(0)

    @pl.when(i == 0)
    def _():
        enter_barrier(me)

    per = n // 4
    for w in range(4):
        @pl.when((i >= w * per) & (i < (w + 1) * per))
        def _():
            y0, y1 = (u0, u1) if w < 3 else (m0, m1)
            g_ref[i % 4] = dot(xs[2 * w][...], y0[...], TN) + dot(xs[2 * w + 1][...], y1[...], TN)

    reduce_step(i, lags, ((n, 0, g_ref.shape[1] // 2, g_ref, lambda j, share: put(out_ref, share), bufs),), me)


MLP_LAGS, MLP_SLOTS = (0, 1, 3, 4, 5), 6
ATTN_LAGS, ATTN_SLOTS = (0, 2, 4, 6, 8), 8


def kept(shape):
    return pl.BlockSpec(shape, lambda i: (0,) * len(shape), pipeline_mode=pl.Buffered(1))


def mlp_grads(ds, mts, z, gs, dup1, w_down, tile, sub):
    rows, d = ds[0].shape
    n = w_down.shape[0] // tile
    at = lambda i: jnp.minimum(i, n - 1)
    col = pl.BlockSpec((rows, tile), lambda i: (0, at(i)))
    anywhere = pl.BlockSpec(memory_space=pl.ANY)
    piece = tile // 16
    return pl.pallas_call(
        functools.partial(mlp_grads_kernel, n, MLP_LAGS, sub),
        grid=(n + MLP_LAGS[4],),
        in_specs=[anywhere] * 4 + [col] * 4 + [pl.BlockSpec((tile, d), lambda i: (at(i), 0))],
        out_specs=[pl.BlockSpec((2, piece, d), lambda i: (jnp.maximum(i - MLP_LAGS[4], 0), 0, 0)), col],
        out_shape=[jax.ShapeDtypeStruct((2 * n, piece, d), F32), jax.ShapeDtypeStruct((rows, n * tile), BF16)],
        scratch_shapes=[pltpu.VMEM((2, tile, d), F32), pltpu.VMEM((2, d, tile), F32)] + [pltpu.VMEM(a.shape, BF16) for a in (*ds, *mts)] + [
            pltpu.SemaphoreType.DMA((4,))] + stream_scratch(tile // 2, d, MLP_SLOTS) + stream_scratch(d // 2, tile, MLP_SLOTS),
        compiler_params=pltpu.CompilerParams(dimension_semantics=("arbitrary",), collective_id=0, has_side_effects=True,
                                             vmem_limit_bytes=VMEM_LIMIT),
        cost_estimate=cost(10 * rows * d * n * tile, 10 * rows * n * tile),
        name="mlp_grads",
    )(*ds, *mts, z, *gs, dup1, w_down)


def mlp_back(du, w_up, d_out, h, tile, sub):
    n, d = d_out.shape
    f = w_up.shape[1]
    anywhere = pl.BlockSpec(memory_space=pl.ANY)
    return pl.pallas_call(
        functools.partial(mlp_back_kernel, sub),
        grid=(f // tile,),
        in_specs=[pl.BlockSpec((n, tile), lambda i: (0, i)), pl.BlockSpec((d, tile), lambda i: (0, i)), anywhere, anywhere],
        out_specs=kept((n, d)),
        out_shape=jax.ShapeDtypeStruct((n, d), BF16),
        scratch_shapes=[pltpu.VMEM((n, d), F32), pltpu.VMEM((n, d), BF16), pltpu.VMEM((n, d), BF16), pltpu.SemaphoreType.DMA((2,))],
        compiler_params=params(),
        cost_estimate=cost(2 * n * d * f, 2 * n * f),
        name="mlp_back",
    )(du, w_up, d_out, h)


def attn_grads(xs, ys, tile):
    rows, d = ys[0].shape
    per = d // tile
    n = 4 * per
    cols = [pl.BlockSpec((rows, tile), lambda i, w=w: (0, jnp.clip(i - w * per, 0, per - 1))) for w in range(4) for _ in range(2)]
    return pl.pallas_call(
        functools.partial(attn_grads_kernel, n, ATTN_LAGS),
        grid=(n + ATTN_LAGS[4],),
        in_specs=cols + [kept((rows, d))] * 4,
        out_specs=pl.BlockSpec((1, tile // 16, d), lambda i: (jnp.maximum(i - ATTN_LAGS[4], 0), 0, 0)),
        out_shape=jax.ShapeDtypeStruct((n, tile // 16, d), F32),
        scratch_shapes=[pltpu.VMEM((4, tile, d), F32)] + stream_scratch(tile // 2, d, ATTN_SLOTS),
        compiler_params=pltpu.CompilerParams(dimension_semantics=("arbitrary",), collective_id=1, has_side_effects=True,
                                             vmem_limit_bytes=VMEM_LIMIT),
        cost_estimate=cost(16 * rows * d * d, 24 * rows * d),
        name="attn_grads",
    )(*[x for pair in xs for x in pair], *ys)


def put_in_place(j, shift, in_ref, out_ref, bands):
    half = out_ref.shape[0] // 2
    piece, width = in_ref.shape[1], out_ref.shape[1]

    def variant(v):
        for dev in range(16):
            bits = [(dev >> (1 + (v + k) % 3)) & 1 for k in range(3)]
            at = half * (dev & 1) + sum((half >> (k + 1)) * bits[k] for k in range(3))
            for k in range(bands):
                out_ref[at + k * piece:at + (k + 1) * piece, :] = in_ref[dev, :, k * width:(k + 1) * width]

    if isinstance(j, int):
        variant((j + shift) % 3)
    else:
        for v in range(3):
            pl.when((j + shift) % 3 == v)(functools.partial(variant, v))


def place_mlp_kernel(group, in_ref, down_ref, up_ref):
    high, width = down_ref.shape[0] // group, up_ref.shape[1] // group
    for c in range(group):
        j = pl.program_id(0) * group + c
        put_in_place(j, 0, in_ref.at[:, 2 * c], down_ref.at[pl.ds(c * high, high)], 1)
        put_in_place(j, 2, in_ref.at[:, 2 * c + 1], up_ref.at[:, pl.ds(c * width, width)], up_ref.shape[0] // (16 * in_ref.shape[2]))


def place_mlp(shares, n, tile, group):
    _, _, piece, d = shares.shape
    return pl.pallas_call(
        functools.partial(place_mlp_kernel, group),
        grid=(n // group,),
        in_specs=[pl.BlockSpec((16, 2 * group, piece, d), lambda i: (0, i, 0, 0))],
        out_specs=[pl.BlockSpec((group * tile, d), lambda i: (i, 0)), pl.BlockSpec((d, group * tile), lambda i: (0, i))],
        out_shape=[jax.ShapeDtypeStruct((n * tile, d), F32), jax.ShapeDtypeStruct((d, n * tile), F32)],
        compiler_params=params(),
        cost_estimate=cost(shares.size // 2, 8 * shares.size),
        name="place_mlp",
    )(shares)


def place_rows_kernel(first, turn, per, in_ref, *refs):
    outs, (in_buf, out_buf, in_sem, out_sem) = refs[:-4], refs[-4:]
    depth, high = in_buf.shape[0], out_buf.shape[1]
    total = per * len(outs)

    def fetch(t):
        return pltpu.make_async_copy(in_ref.at[:, first + t], in_buf.at[t % depth], in_sem.at[t % depth])

    def store(t):
        at = t % per * high
        return pltpu.make_async_copy(out_buf.at[t % depth], outs[t // per].at[pl.ds(at, high)], out_sem.at[t % depth])

    for t in range(min(depth, total)):
        fetch(t).start()
    for t in range(total):
        fetch(t).wait()
        if t >= depth:
            store(t - depth).wait()
        put_in_place(turn + t, 0, in_buf.at[t % depth], out_buf.at[t % depth], 1)
        store(t).start()
        if t + depth < total:
            fetch(t + depth).start()
    for t in range(max(total - depth, 0), total):
        store(t).wait()


def place_rows(shares, first, turn, per, n_out, depth):
    _, _, piece, d = shares.shape
    anywhere = pl.BlockSpec(memory_space=pl.ANY)
    return pl.pallas_call(
        functools.partial(place_rows_kernel, first, turn, per),
        in_specs=[anywhere],
        out_specs=[anywhere] * n_out,
        out_shape=[jax.ShapeDtypeStruct((per * 16 * piece, d), F32)] * n_out,
        scratch_shapes=[pltpu.VMEM((depth, 16, piece, d), F32), pltpu.VMEM((depth, 16 * piece, d), F32),
                        pltpu.SemaphoreType.DMA((depth,)), pltpu.SemaphoreType.DMA((depth,))],
        compiler_params=pltpu.CompilerParams(vmem_limit_bytes=VMEM_LIMIT),
        cost_estimate=cost(per * n_out * piece * d * 16, per * n_out * piece * d * 128),
        name="place_rows",
    )(shares)


def solution(mesh):
    batch_spec = P('data', None, None)

    def per_device(x_loc, g_loc, step_emb, w_q, w_k, w_v, w_o, w_up, w_down):
        d, n_heads, head = w_q.shape
        scale = head ** -0.5
        n_seq, seq, _ = x_loc.shape
        n = n_seq * seq
        wq, wk, wv = (w.transpose(1, 2, 0).reshape(n_heads * head, d) for w in (w_q, w_k, w_v))
        wo = w_o.reshape(n_heads * head, d)
        mask = np.kron(np.eye(4), np.ones((64, 64))).astype(BF16)

        def attn_back(dmid, *acts):
            return attn_bwd(dmid, *acts, wq, wk, wv, wo, mask, seq, scale, 512)

        x0, u0, q0, k0, v0, mix0, h0, m0, mt0 = attn_fwd(x_loc.reshape(n, d), step_emb, 0, wq, wk, wv, wo, mask, seq, scale, 512)
        z0, g0, x = mlp_fwd(m0, w_up, w_down, h0, 1024, 512)
        x1, u1, q1, k1, v1, mix1, h1, m1, mt1 = attn_fwd(x, step_emb, 1, wq, wk, wv, wo, mask, seq, scale, 512)
        do1 = g_loc.reshape(n, d)
        g1, dup1, dmid1 = mlp_last(m1, do1, w_up, w_down, h1, 1024, 512)
        dq1, dk1, dv1, do0 = attn_back(dmid1, q1, k1, v1, x1)
        s_mlp, dup0 = mlp_grads((do0, do1), (mt0, mt1), z0, (g0, g1), dup1, w_down, 256, 256)
        n_tiles, n_blocks = w_up.shape[1] // 256, d // 256
        a_mlp = lax.all_gather(s_mlp, 'data')
        dmid0 = mlp_back(dup0, w_up, do0, h0, 1024, 512)
        dq0, dk0, dv0, d_out = attn_back(dmid0, q0, k0, v0, x0)
        s_attn = attn_grads([(dq0, dq1), (dk0, dk1), (dv0, dv1), (mix0, mix1)], (u0, u1, dmid0, dmid1), 256)
        a_attn = lax.all_gather(s_attn, 'data')
        g_down, g_up = place_mlp(a_mlp, n_tiles, 256, 2)
        g_q, g_k, g_v, g_o = place_rows(a_attn, 0, 0, n_blocks, 4, 6)
        heads = lambda a: a.reshape(n_heads, head, d).transpose(2, 0, 1)
        return heads(g_q), heads(g_k), heads(g_v), g_o.reshape(w_o.shape), g_up, g_down, d_out.reshape(x_loc.shape)

    return jax.shard_map(per_device, mesh=mesh, in_specs=(batch_spec, batch_spec, P(), P(), P(), P(), P(), P(), P()), out_specs=(P(), P(), P(), P(), P(), P(), batch_spec), check_vma=False)
```

```python
import functools
import math

import jax
import jax.numpy as jnp
import numpy as np
from jax import lax
from jax.experimental import pallas as pl
from jax.experimental.pallas import tpu as pltpu
from jax.sharding import PartitionSpec as P


NORM_EPS = 1e-6
GELU_C = math.sqrt(2.0 / math.pi)
GELU_A = 0.044715
BF16 = jnp.bfloat16
F32 = jnp.float32
VMEM_LIMIT = 60 * 1024 * 1024

NN = (((1,), (0,)), ((), ()))
NT = (((1,), (1,)), ((), ()))
TN = (((0,), (0,)), ((), ()))
MESH = pl.DeviceIdType.MESH


def dot(a, b, dims=NN):
    return lax.dot_general(a, b, dims, preferred_element_type=F32)


def rms_scale(x_f32):
    return lax.rsqrt(jnp.mean(x_f32 * x_f32, axis=-1, keepdims=True) + NORM_EPS)


def rms_pull(x_bf16, d_bf16):
    x = x_bf16.astype(F32)
    d = d_bf16.astype(F32)
    r = rms_scale(x)
    dot_dx = jnp.mean(d * x, axis=-1, keepdims=True)
    return (d * r - x * (r * r * r * dot_dx)).astype(BF16)


def gelu_tanh(z):
    return jnp.tanh(GELU_C * (z + GELU_A * (z * z * z)))


def gelu_slope(z, t):
    return 0.5 * (1.0 + t) + (0.5 * z) * ((1.0 - t * t) * (GELU_C * (1.0 + (3.0 * GELU_A) * (z * z))))


def block_diag(a, mask):
    return jnp.concatenate([a, a, a, a], axis=0) * mask


def diag_blocks(full, seq, lane_lo):
    left = jnp.where(lane_lo, full[0:seq, 0:128], full[seq:2 * seq, 0:128])
    right = jnp.where(lane_lo, full[2 * seq:3 * seq, 128:256], full[3 * seq:4 * seq, 128:256])
    return jnp.concatenate([left, right], axis=1)


def softmax_t(scores_t, scale):
    s = scores_t * scale
    e = jnp.exp(s - jnp.max(s, axis=0, keepdims=True))
    return e / jnp.sum(e, axis=0, keepdims=True)


def in_chunks(n, body, rows=32):
    def step(i, _):
        body(pl.ds(pl.multiple_of(i * rows, rows), rows))
        return 0

    lax.fori_loop(0, n // rows, step, 0, unroll=2)


def loads(refs, bufs, sems):
    return [pltpu.make_async_copy(r, b, sems.at[k]) for k, (r, b) in enumerate(zip(refs, bufs))]


def at_step(step, *actions):
    @pl.when(pl.program_id(0) == step)
    def _():
        for act in actions:
            act()


def attn_fwd_kernel(layer, seq, scale, x_ref, e_ref, mask_ref, wq_hbm, wk_hbm, wv_hbm, wo_hbm,
                    xc_ref, u_ref, q_ref, k_ref, v_ref, mix_ref, h_ref, m_ref, mt_ref, wq_ref, wk_ref, wv_ref, wo_ref, sems):
    load = loads((wq_hbm, wk_hbm, wv_hbm, wo_hbm), (wq_ref, wk_ref, wv_ref, wo_ref), sems)
    at_step(0, *(c.start for c in load))
    n_rows = x_ref.shape[0]
    blocks = [pl.ds(r * (n_rows // 2), n_rows // 2) for r in range(2)]
    at_step(0, load[0].wait, load[1].wait)
    for k, rows in enumerate(blocks):
        x = (x_ref[rows, :].astype(F32) + e_ref[layer:layer + 1, :].astype(F32)).astype(BF16)
        xc_ref[rows, :] = x
        x_f32 = x.astype(F32)
        u_ref[rows, :] = (x_f32 * rms_scale(x_f32)).astype(BF16)
        for w_ref, o_ref in ((wq_ref, q_ref), (wk_ref, k_ref), (wv_ref, v_ref)):
            if k == 0 and w_ref is wv_ref:
                at_step(0, load[2].wait, load[3].wait)
            o_ref[rows, :] = dot(u_ref[rows, :], w_ref[...], NT).astype(BF16)

    n_groups = x_ref.shape[1] // 256
    lane_lo = lax.broadcasted_iota(jnp.int32, (seq, 128), 1) < 64

    def one_seq(s):
        rows = pl.ds(s * seq, seq)
        cols = [pl.ds(g * 256, 256) for g in range(n_groups)]
        mask = mask_ref[...]
        st = [dot(k_ref[rows, c], block_diag(q_ref[rows, c], mask), NT).astype(BF16).astype(F32) for c in cols]
        pb = [softmax_t(t, scale).astype(BF16) for t in st]
        for c, p in zip(cols, pb):
            mix_ref[rows, c] = diag_blocks(dot(p, v_ref[rows, c], TN), seq, lane_lo).astype(BF16)

    for s in range(x_ref.shape[0] // seq):
        one_seq(s)
    for rows in blocks:
        h = (xc_ref[rows, :].astype(F32) + dot(mix_ref[rows, :], wo_ref[...]).astype(BF16).astype(F32)).astype(BF16)
        h_ref[rows, :] = h
        h_f32 = h.astype(F32)
        m_ref[rows, :] = (h_f32 * rms_scale(h_f32)).astype(BF16)
    mt_ref[...] = m_ref[...].T


def attn_bwd_kernel(seq, scale, dmid_ref, q_ref, k_ref, v_ref, xc_ref, mask_ref, wo_hbm, wq_hbm, wk_hbm, wv_hbm,
                    dq_ref, dk_ref, dv_ref, dprev_ref, dmix_ref, wo_ref, wq_ref, wk_ref, wv_ref, sems):
    load = loads((wo_hbm, wq_hbm, wk_hbm, wv_hbm), (wo_ref, wq_ref, wk_ref, wv_ref), sems)
    at_step(0, *(c.start for c in load), load[0].wait)
    dmix_ref[...] = dot(dmid_ref[...], wo_ref[...], NT).astype(BF16)
    n_groups = xc_ref.shape[1] // 256
    lane_lo = lax.broadcasted_iota(jnp.int32, (seq, 128), 1) < 64

    def one_seq(s, _):
        rows = pl.ds(pl.multiple_of(s * seq, seq), seq)
        cols = [pl.ds(g * 256, 256) for g in range(n_groups)]
        mask = mask_ref[...]
        qbd = [block_diag(q_ref[rows, c], mask) for c in cols]
        dbd = [block_diag(dmix_ref[rows, c], mask) for c in cols]
        st = [dot(k_ref[rows, c], t, NT).astype(BF16).astype(F32) for c, t in zip(cols, qbd)]
        dp = [dot(v_ref[rows, c], t, NT).astype(BF16).astype(F32) for c, t in zip(cols, dbd)]
        p = [softmax_t(t, scale) for t in st]
        for c, a, t in zip(cols, p, dbd):
            dv_ref[rows, c] = dot(a.astype(BF16), t).astype(BF16)
        ds = [((a * (t - jnp.sum(a * t, axis=0, keepdims=True))) * scale).astype(BF16) for a, t in zip(p, dp)]
        for c, a, t in zip(cols, ds, qbd):
            dk_ref[rows, c] = dot(a, t).astype(BF16)
            dq_ref[rows, c] = diag_blocks(dot(a, k_ref[rows, c], TN), seq, lane_lo).astype(BF16)
        return 0

    lax.fori_loop(0, xc_ref.shape[0] // seq, one_seq, 0, unroll=4)
    at_step(0, *(c.wait for c in load[1:]))
    n_rows = xc_ref.shape[0]
    for rows in [pl.ds(r * (n_rows // 2), n_rows // 2) for r in range(2)]:
        du = dot(dq_ref[rows, :], wq_ref[...]) + dot(dk_ref[rows, :], wk_ref[...]) + dot(dv_ref[rows, :], wv_ref[...])
        dx = rms_pull(xc_ref[rows, :], du.astype(BF16))
        dprev_ref[rows, :] = (dmid_ref[rows, :].astype(F32) + dx.astype(F32)).astype(BF16)


def mlp_fwd_kernel(sub, m_ref, wup_ref, wdown_ref, h_hbm, z_ref, g_ref, y_ref, acc_ref, h_ref, sem):
    step = pl.program_id(0)
    load = pltpu.make_async_copy(h_hbm, h_ref, sem)
    at_step(0, load.start)

    @pl.when(step == 0)
    def _():
        acc_ref[...] = jnp.zeros_like(acc_ref)

    for r in range(m_ref.shape[0] // sub):
        rows = pl.ds(r * sub, sub)
        zb = dot(m_ref[rows, :], wup_ref[...]).astype(BF16)
        z_ref[rows, :] = zb
        z = zb.astype(F32)
        g = ((0.5 * z) * (1.0 + gelu_tanh(z))).astype(BF16)
        g_ref[rows, :] = g
        acc_ref[rows, :] += dot(g, wdown_ref[...])

    @pl.when(step == pl.num_programs(0) - 1)
    def _():
        load.wait()

        def finish(rows):
            y = acc_ref[rows, :].astype(BF16)
            y_ref[rows, :] = (h_ref[rows, :].astype(F32) + y.astype(F32)).astype(BF16)

        in_chunks(m_ref.shape[0], finish)


def mlp_last_kernel(sub, m_ref, d_ref, wup_ref, wdown_ref, h_hbm, g_ref, dup_ref, dmid_ref, acc_ref, h_ref, sem):
    step = pl.program_id(0)
    load = pltpu.make_async_copy(h_hbm, h_ref, sem)
    at_step(0, load.start)

    @pl.when(step == 0)
    def _():
        acc_ref[...] = jnp.zeros_like(acc_ref)

    for r in range(d_ref.shape[0] // sub):
        rows = pl.ds(r * sub, sub)
        z = dot(m_ref[rows, :], wup_ref[...]).astype(BF16).astype(F32)
        t = gelu_tanh(z)
        g_ref[rows, :] = ((0.5 * z) * (1.0 + t)).astype(BF16)
        da = dot(d_ref[rows, :], wdown_ref[...], NT).astype(BF16).astype(F32)
        dup_ref[rows, :] = (da * gelu_slope(z, t)).astype(BF16)
        acc_ref[rows, :] += dot(dup_ref[rows, :], wup_ref[...], NT)

    @pl.when(step == pl.num_programs(0) - 1)
    def _():
        load.wait()

        def finish(rows):
            dh = rms_pull(h_ref[rows, :], acc_ref[rows, :].astype(BF16))
            dmid_ref[rows, :] = (d_ref[rows, :].astype(F32) + dh.astype(F32)).astype(BF16)

        in_chunks(d_ref.shape[0], finish)


def params(**kw):
    return pltpu.CompilerParams(dimension_semantics=("arbitrary",), vmem_limit_bytes=VMEM_LIMIT, **kw)


def cost(flops, nbytes, trans=0):
    return pl.CostEstimate(flops=int(flops), bytes_accessed=int(nbytes), transcendentals=int(trans))


def whole(shape):
    return pl.BlockSpec(shape, lambda i: (0,) * len(shape))


def attn_fwd(x, step_emb, layer, wq, wk, wv, wo, mask, seq, scale, tile):
    n, d = x.shape
    row = pl.BlockSpec((tile, d), lambda i: (i, 0))
    return pl.pallas_call(
        functools.partial(attn_fwd_kernel, layer, seq, scale),
        grid=(n // tile,),
        in_specs=[row, whole(step_emb.shape), whole(mask.shape)] + [pl.BlockSpec(memory_space=pl.ANY)] * 4,
        out_specs=[row] * 8 + [pl.BlockSpec((d, tile), lambda i: (0, i))],
        out_shape=[jax.ShapeDtypeStruct((n, d), BF16)] * 8 + [jax.ShapeDtypeStruct((d, n), BF16)],
        scratch_shapes=[pltpu.VMEM(w.shape, BF16) for w in (wq, wk, wv, wo)] + [pltpu.SemaphoreType.DMA((4,))],
        compiler_params=params(),
        cost_estimate=cost(8 * n * d * d, 20 * n * d, n * d),
        name="attn_fwd",
    )(x, step_emb, mask, wq, wk, wv, wo)


def attn_bwd(dmid, q, k, v, xc, wq, wk, wv, wo, mask, seq, scale, tile):
    n, d = xc.shape
    row = pl.BlockSpec((tile, d), lambda i: (i, 0))
    return pl.pallas_call(
        functools.partial(attn_bwd_kernel, seq, scale),
        grid=(n // tile,),
        in_specs=[row] * 5 + [whole(mask.shape)] + [pl.BlockSpec(memory_space=pl.ANY)] * 4,
        out_specs=[row] * 4,
        out_shape=[jax.ShapeDtypeStruct((n, d), BF16)] * 4,
        scratch_shapes=[pltpu.VMEM((tile, d), BF16)] + [pltpu.VMEM(w.shape, BF16) for w in (wo, wq, wk, wv)] + [pltpu.SemaphoreType.DMA((4,))],
        compiler_params=params(),
        cost_estimate=cost(8 * n * d * d, 20 * n * d, n * d),
        name="attn_bwd",
    )(dmid, q, k, v, xc, mask, wo, wq, wk, wv)


def mlp_fwd(m, w_up, w_down, h, tile, sub):
    n, d = m.shape
    f = w_up.shape[1]
    col = pl.BlockSpec((n, tile), lambda i: (0, i))
    return pl.pallas_call(
        functools.partial(mlp_fwd_kernel, sub),
        grid=(f // tile,),
        in_specs=[kept((n, d)), pl.BlockSpec((d, tile), lambda i: (0, i)), pl.BlockSpec((tile, d), lambda i: (i, 0)), pl.BlockSpec(memory_space=pl.ANY)],
        out_specs=[col, col, kept((n, d))],
        out_shape=[jax.ShapeDtypeStruct((n, f), BF16)] * 2 + [jax.ShapeDtypeStruct((n, d), BF16)],
        scratch_shapes=[pltpu.VMEM((n, d), F32), pltpu.VMEM((n, d), BF16), pltpu.SemaphoreType.DMA(())],
        compiler_params=params(),
        cost_estimate=cost(4 * n * d * f, 4 * n * f, n * f),
        name="mlp_fwd",
    )(m, w_up, w_down, h)


def mlp_last(m, d_out, w_up, w_down, h, tile, sub):
    n, d = d_out.shape
    f = w_up.shape[1]
    col = pl.BlockSpec((n, tile), lambda i: (0, i))
    return pl.pallas_call(
        functools.partial(mlp_last_kernel, sub),
        grid=(f // tile,),
        in_specs=[kept((n, d)), kept((n, d)), pl.BlockSpec((d, tile), lambda i: (0, i)), pl.BlockSpec((tile, d), lambda i: (i, 0)),
                  pl.BlockSpec(memory_space=pl.ANY)],
        out_specs=[col, col, kept((n, d))],
        out_shape=[jax.ShapeDtypeStruct((n, f), BF16)] * 2 + [jax.ShapeDtypeStruct((n, d), BF16)],
        scratch_shapes=[pltpu.VMEM((n, d), F32), pltpu.VMEM((n, d), BF16), pltpu.SemaphoreType.DMA(())],
        compiler_params=params(),
        cost_estimate=cost(6 * n * d * f, 4 * n * f, n * f),
        name="mlp_last",
    )(m, d_out, w_up, w_down, h)


def peer_of(me, power):
    return me + power * (1 - 2 * ((me // power) % 2))


def enter_barrier(me):
    barrier = pltpu.get_barrier_semaphore()
    for power in (1, 2, 4, 8):
        pl.semaphore_signal(barrier, inc=1, device_id=(peer_of(me, power),), device_id_type=MESH)
    pl.semaphore_wait(barrier, 4)


def stream_scratch(half, width, slots):
    return [pltpu.VMEM((slots, half // k, width), F32) for k in (1, 2, 4, 8)] + [
        pltpu.SemaphoreType.DMA((4, slots)), pltpu.SemaphoreType.DMA((4, slots))]


def put(ref, value):
    ref[0] = value


def reduce_stage(s, j, shift, half, g_ref, sink, bufs, me):
    h0, h1, h2, h3, send_sem, recv_sem = bufs
    slots = h0.shape[0]
    slot, g = j % slots, g_ref.at[j % g_ref.shape[0]]
    core = me % 2
    powers, bits = [], []
    for k in range(3):
        r = (j + k + shift) % 3
        powers.append(2 + r + r * r)
        bits.append((me // powers[k]) % 2)
    held = (g, h0.at[slot], h1.at[slot], h2.at[slot], h3.at[slot])
    keep = (half * core,) + tuple((half >> (k + 1)) * bits[k] for k in range(3))
    away = (half * (1 - core),) + tuple((half >> (k + 1)) * (1 - bits[k]) for k in range(3))

    def part(ref, start, size):
        return ref.at[pl.ds(pl.multiple_of(start, 8), size)]

    def copy(k):
        peer = peer_of(me, 1) if k == 0 else peer_of(me, powers[k - 1])
        return pltpu.make_async_remote_copy(
            src_ref=part(held[k], away[k], half >> k), dst_ref=held[k + 1], send_sem=send_sem.at[k, slot],
            recv_sem=recv_sem.at[k, slot], device_id=(peer,), device_id_type=MESH)

    if s > 0:
        before = copy(s - 1)
        before.wait_recv()
        before.wait_send()
        own = held[s - 1][pl.ds(pl.multiple_of(keep[s - 1], 8), half >> (s - 1)), :]
        if s == 4:
            sink(j, held[4][...] + own)
        else:
            held[s][...] = held[s][...] + own
    if s < 4:
        copy(s).start()


def reduce_step(i, lags, streams, me):
    for n, *stream in streams:
        for s in (4, 3, 2, 1, 0):
            j = i - lags[s]

            @pl.when((j >= 0) & (j < n))
            def _():
                reduce_stage(s, j, *stream, me)


def mlp_grads_kernel(n, sub, d0_hbm, d1_hbm, m0t_hbm, m1t_hbm, z_ref, g0_ref, g1_ref, dup1_ref, wdown_ref,
                     share_ref, du_ref, gd_ref, gu_ref, d0_ref, d1_ref, m0t_ref, m1t_ref, sems, *bufs):
    me = lax.axis_index('data')
    i = pl.program_id(0)
    load = loads((d0_hbm, d1_hbm, m0t_hbm, m1t_hbm), (d0_ref, d1_ref, m0t_ref, m1t_ref), sems)

    def share_up(j, share):
        piece, width = share_ref.shape[1], share.shape[1]
        for k in range(share.shape[0] // piece):
            share_ref[1, :, k * width:(k + 1) * width] = share[k * piece:(k + 1) * piece, :]

    down = (0, gd_ref.shape[1] // 2, gd_ref, lambda j, share: put(share_ref, share), bufs[:6])
    up = (2, gu_ref.shape[1] // 2, gu_ref, share_up, bufs[6:])

    def exchange(*stages):
        for stream, s, lag in stages:
            j = i - lag

            @pl.when((j >= 0) & (j < n))
            def _():
                reduce_stage(s, j, *stream, me)

    @pl.when(i == 0)
    def _():
        for c in load:
            c.start()
        enter_barrier(me)
        for c in load[:2]:
            c.wait()

    @pl.when(i < n)
    def _():
        gd_ref[i % 2] = dot(g0_ref[...], d0_ref[...], TN) + dot(g1_ref[...], d1_ref[...], TN)

    exchange((up, 1, 1), (down, 4, 4), (down, 3, 3), (down, 2, 2), (down, 0, 0))
    at_step(0, *(c.wait for c in load[2:]))

    @pl.when(i < n)
    def _():
        for r in range(d0_ref.shape[0] // sub):
            rows = pl.ds(r * sub, sub)
            da = dot(d0_ref[rows, :], wdown_ref[...], NT).astype(BF16).astype(F32)
            z = z_ref[rows, :].astype(F32)
            du_ref[rows, :] = (da * gelu_slope(z, gelu_tanh(z))).astype(BF16)
        gu_ref[i % 2] = dot(m0t_ref[...], du_ref[...]) + dot(m1t_ref[...], dup1_ref[...])

    exchange((up, 4, 4), (up, 3, 3), (up, 2, 2), (down, 1, 0), (up, 0, 0))


def mlp_back_kernel(sub, du_ref, wup_ref, d_hbm, h_hbm, dmid_ref, acc_ref, d_ref, h_ref, sems):
    step = pl.program_id(0)
    load = loads((d_hbm, h_hbm), (d_ref, h_ref), sems)
    at_step(0, *(c.start for c in load))

    @pl.when(step == 0)
    def _():
        acc_ref[...] = jnp.zeros_like(acc_ref)

    for r in range(du_ref.shape[0] // sub):
        rows = pl.ds(r * sub, sub)
        acc_ref[rows, :] += dot(du_ref[rows, :], wup_ref[...], NT)

    @pl.when(step == pl.num_programs(0) - 1)
    def _():
        for c in load:
            c.wait()

        def finish(rows):
            dh = rms_pull(h_ref[rows, :], acc_ref[rows, :].astype(BF16))
            dmid_ref[rows, :] = (d_ref[rows, :].astype(F32) + dh.astype(F32)).astype(BF16)

        in_chunks(d_ref.shape[0], finish)


def attn_grads_kernel(n, lags, *refs):
    xs, (u0, u1, m0, m1), out_ref, g_ref, bufs = refs[:8], refs[8:12], refs[12], refs[13], refs[14:]
    me = lax.axis_index('data')
    i = pl.program_id(0)

    @pl.when(i == 0)
    def _():
        enter_barrier(me)

    per = n // 4
    for w in range(4):
        @pl.when((i >= w * per) & (i < (w + 1) * per))
        def _():
            y0, y1 = (u0, u1) if w < 3 else (m0, m1)
            g_ref[i % 4] = dot(xs[2 * w][...], y0[...], TN) + dot(xs[2 * w + 1][...], y1[...], TN)

    reduce_step(i, lags, ((n, 0, g_ref.shape[1] // 2, g_ref, lambda j, share: put(out_ref, share), bufs),), me)


MLP_LAG, MLP_SLOTS = 4, 6
ATTN_LAGS, ATTN_SLOTS = (0, 2, 4, 6, 8), 8


def kept(shape):
    return pl.BlockSpec(shape, lambda i: (0,) * len(shape), pipeline_mode=pl.Buffered(1))


def mlp_grads(ds, mts, z, gs, dup1, w_down, tile, sub):
    rows, d = ds[0].shape
    n = w_down.shape[0] // tile
    at = lambda i: jnp.minimum(i, n - 1)
    col = pl.BlockSpec((rows, tile), lambda i: (0, at(i)))
    anywhere = pl.BlockSpec(memory_space=pl.ANY)
    piece = tile // 16
    return pl.pallas_call(
        functools.partial(mlp_grads_kernel, n, sub),
        grid=(n + MLP_LAG,),
        in_specs=[anywhere] * 4 + [col] * 4 + [pl.BlockSpec((tile, d), lambda i: (at(i), 0))],
        out_specs=[pl.BlockSpec((2, piece, d), lambda i: (jnp.maximum(i - MLP_LAG, 0), 0, 0)), col],
        out_shape=[jax.ShapeDtypeStruct((2 * n, piece, d), F32), jax.ShapeDtypeStruct((rows, n * tile), BF16)],
        scratch_shapes=[pltpu.VMEM((2, tile, d), F32), pltpu.VMEM((2, d, tile), F32)] + [pltpu.VMEM(a.shape, BF16) for a in (*ds, *mts)] + [
            pltpu.SemaphoreType.DMA((4,))] + stream_scratch(tile // 2, d, MLP_SLOTS) + stream_scratch(d // 2, tile, MLP_SLOTS),
        compiler_params=pltpu.CompilerParams(dimension_semantics=("arbitrary",), collective_id=0, has_side_effects=True,
                                             vmem_limit_bytes=VMEM_LIMIT),
        cost_estimate=cost(10 * rows * d * n * tile, 10 * rows * n * tile),
        name="mlp_grads",
    )(*ds, *mts, z, *gs, dup1, w_down)


def mlp_back(du, w_up, d_out, h, tile, sub):
    n, d = d_out.shape
    f = w_up.shape[1]
    anywhere = pl.BlockSpec(memory_space=pl.ANY)
    return pl.pallas_call(
        functools.partial(mlp_back_kernel, sub),
        grid=(f // tile,),
        in_specs=[pl.BlockSpec((n, tile), lambda i: (0, i)), pl.BlockSpec((d, tile), lambda i: (0, i)), anywhere, anywhere],
        out_specs=kept((n, d)),
        out_shape=jax.ShapeDtypeStruct((n, d), BF16),
        scratch_shapes=[pltpu.VMEM((n, d), F32), pltpu.VMEM((n, d), BF16), pltpu.VMEM((n, d), BF16), pltpu.SemaphoreType.DMA((2,))],
        compiler_params=params(),
        cost_estimate=cost(2 * n * d * f, 2 * n * f),
        name="mlp_back",
    )(du, w_up, d_out, h)


def attn_grads(xs, ys, tile):
    rows, d = ys[0].shape
    per = d // tile
    n = 4 * per
    cols = [pl.BlockSpec((rows, tile), lambda i, w=w: (0, jnp.clip(i - w * per, 0, per - 1))) for w in range(4) for _ in range(2)]
    return pl.pallas_call(
        functools.partial(attn_grads_kernel, n, ATTN_LAGS),
        grid=(n + ATTN_LAGS[4],),
        in_specs=cols + [kept((rows, d))] * 4,
        out_specs=pl.BlockSpec((1, tile // 16, d), lambda i: (jnp.maximum(i - ATTN_LAGS[4], 0), 0, 0)),
        out_shape=jax.ShapeDtypeStruct((n, tile // 16, d), F32),
        scratch_shapes=[pltpu.VMEM((4, tile, d), F32)] + stream_scratch(tile // 2, d, ATTN_SLOTS),
        compiler_params=pltpu.CompilerParams(dimension_semantics=("arbitrary",), collective_id=1, has_side_effects=True,
                                             vmem_limit_bytes=VMEM_LIMIT),
        cost_estimate=cost(16 * rows * d * d, 24 * rows * d),
        name="attn_grads",
    )(*[x for pair in xs for x in pair], *ys)


def put_in_place(j, shift, in_ref, out_ref, bands):
    half = out_ref.shape[0] // 2
    piece, width = in_ref.shape[1], out_ref.shape[1]

    def variant(v):
        for dev in range(16):
            bits = [(dev >> (1 + (v + k) % 3)) & 1 for k in range(3)]
            at = half * (dev & 1) + sum((half >> (k + 1)) * bits[k] for k in range(3))
            for k in range(bands):
                out_ref[at + k * piece:at + (k + 1) * piece, :] = in_ref[dev, :, k * width:(k + 1) * width]

    if isinstance(j, int):
        variant((j + shift) % 3)
    else:
        for v in range(3):
            pl.when((j + shift) % 3 == v)(functools.partial(variant, v))


def place_mlp_kernel(group, in_ref, down_ref, up_ref):
    high, width = down_ref.shape[0] // group, up_ref.shape[1] // group
    for c in range(group):
        j = pl.program_id(0) * group + c
        put_in_place(j, 0, in_ref.at[:, 2 * c], down_ref.at[pl.ds(c * high, high)], 1)
        put_in_place(j, 2, in_ref.at[:, 2 * c + 1], up_ref.at[:, pl.ds(c * width, width)], up_ref.shape[0] // (16 * in_ref.shape[2]))


def place_mlp(shares, n, tile, group):
    _, _, piece, d = shares.shape
    return pl.pallas_call(
        functools.partial(place_mlp_kernel, group),
        grid=(n // group,),
        in_specs=[pl.BlockSpec((16, 2 * group, piece, d), lambda i: (0, i, 0, 0))],
        out_specs=[pl.BlockSpec((group * tile, d), lambda i: (i, 0)), pl.BlockSpec((d, group * tile), lambda i: (0, i))],
        out_shape=[jax.ShapeDtypeStruct((n * tile, d), F32), jax.ShapeDtypeStruct((d, n * tile), F32)],
        compiler_params=params(),
        cost_estimate=cost(shares.size // 2, 8 * shares.size),
        name="place_mlp",
    )(shares)


def place_rows_kernel(first, turn, per, in_ref, *refs):
    outs, (in_buf, out_buf, in_sem, out_sem) = refs[:-4], refs[-4:]
    depth, high = in_buf.shape[0], out_buf.shape[1]
    total = per * len(outs)

    def fetch(t):
        return pltpu.make_async_copy(in_ref.at[:, first + t], in_buf.at[t % depth], in_sem.at[t % depth])

    def store(t):
        at = t % per * high
        return pltpu.make_async_copy(out_buf.at[t % depth], outs[t // per].at[pl.ds(at, high)], out_sem.at[t % depth])

    for t in range(min(depth, total)):
        fetch(t).start()
    for t in range(total):
        fetch(t).wait()
        if t >= depth:
            store(t - depth).wait()
        put_in_place(turn + t, 0, in_buf.at[t % depth], out_buf.at[t % depth], 1)
        store(t).start()
        if t + depth < total:
            fetch(t + depth).start()
    for t in range(max(total - depth, 0), total):
        store(t).wait()


def place_rows(shares, first, turn, per, n_out, depth):
    _, _, piece, d = shares.shape
    anywhere = pl.BlockSpec(memory_space=pl.ANY)
    return pl.pallas_call(
        functools.partial(place_rows_kernel, first, turn, per),
        in_specs=[anywhere],
        out_specs=[anywhere] * n_out,
        out_shape=[jax.ShapeDtypeStruct((per * 16 * piece, d), F32)] * n_out,
        scratch_shapes=[pltpu.VMEM((depth, 16, piece, d), F32), pltpu.VMEM((depth, 16 * piece, d), F32),
                        pltpu.SemaphoreType.DMA((depth,)), pltpu.SemaphoreType.DMA((depth,))],
        compiler_params=pltpu.CompilerParams(vmem_limit_bytes=VMEM_LIMIT),
        cost_estimate=cost(per * n_out * piece * d * 16, per * n_out * piece * d * 128),
        name="place_rows",
    )(shares)


def solution(mesh):
    batch_spec = P('data', None, None)

    def per_device(x_loc, g_loc, step_emb, w_q, w_k, w_v, w_o, w_up, w_down):
        d, n_heads, head = w_q.shape
        scale = head ** -0.5
        n_seq, seq, _ = x_loc.shape
        n = n_seq * seq
        wq, wk, wv = (w.transpose(1, 2, 0).reshape(n_heads * head, d) for w in (w_q, w_k, w_v))
        wo = w_o.reshape(n_heads * head, d)
        mask = np.kron(np.eye(4), np.ones((64, 64))).astype(BF16)

        def attn_back(dmid, *acts):
            return attn_bwd(dmid, *acts, wq, wk, wv, wo, mask, seq, scale, 512)

        x0, u0, q0, k0, v0, mix0, h0, m0, mt0 = attn_fwd(x_loc.reshape(n, d), step_emb, 0, wq, wk, wv, wo, mask, seq, scale, 512)
        z0, g0, x = mlp_fwd(m0, w_up, w_down, h0, 1024, 512)
        x1, u1, q1, k1, v1, mix1, h1, m1, mt1 = attn_fwd(x, step_emb, 1, wq, wk, wv, wo, mask, seq, scale, 512)
        do1 = g_loc.reshape(n, d)
        g1, dup1, dmid1 = mlp_last(m1, do1, w_up, w_down, h1, 1024, 512)
        dq1, dk1, dv1, do0 = attn_back(dmid1, q1, k1, v1, x1)
        s_mlp, dup0 = mlp_grads((do0, do1), (mt0, mt1), z0, (g0, g1), dup1, w_down, 256, 256)
        n_tiles, n_blocks = w_up.shape[1] // 256, d // 256
        a_mlp = lax.all_gather(s_mlp, 'data')
        dmid0 = mlp_back(dup0, w_up, do0, h0, 1024, 512)
        dq0, dk0, dv0, d_out = attn_back(dmid0, q0, k0, v0, x0)
        s_attn = attn_grads([(dq0, dq1), (dk0, dk1), (dv0, dv1), (mix0, mix1)], (u0, u1, dmid0, dmid1), 256)
        a_attn = lax.all_gather(s_attn, 'data')
        g_down, g_up = place_mlp(a_mlp, n_tiles, 256, 2)
        g_q, g_k, g_v, g_o = place_rows(a_attn, 0, 0, n_blocks, 4, 6)
        heads = lambda a: a.reshape(n_heads, head, d).transpose(2, 0, 1)
        return heads(g_q), heads(g_k), heads(g_v), g_o.reshape(w_o.shape), g_up, g_down, d_out.reshape(x_loc.shape)

    return jax.shard_map(per_device, mesh=mesh, in_specs=(batch_spec, batch_spec, P(), P(), P(), P(), P(), P(), P()), out_specs=(P(), P(), P(), P(), P(), P(), batch_spec), check_vma=False)
```

```python
import functools
import math

import jax
import jax.numpy as jnp
import numpy as np
from jax import lax
from jax.experimental import pallas as pl
from jax.experimental.pallas import tpu as pltpu
from jax.sharding import PartitionSpec as P


NORM_EPS = 1e-6
GELU_C = math.sqrt(2.0 / math.pi)
GELU_A = 0.044715
BF16 = jnp.bfloat16
F32 = jnp.float32
VMEM_LIMIT = 60 * 1024 * 1024

NN = (((1,), (0,)), ((), ()))
NT = (((1,), (1,)), ((), ()))
TN = (((0,), (0,)), ((), ()))
MESH = pl.DeviceIdType.MESH


def dot(a, b, dims=NN):
    return lax.dot_general(a, b, dims, preferred_element_type=F32)


def rms_scale(x_f32):
    return lax.rsqrt(jnp.mean(x_f32 * x_f32, axis=-1, keepdims=True) + NORM_EPS)


def rms_pull(x_bf16, d_bf16):
    x = x_bf16.astype(F32)
    d = d_bf16.astype(F32)
    r = rms_scale(x)
    dot_dx = jnp.mean(d * x, axis=-1, keepdims=True)
    return (d * r - x * (r * r * r * dot_dx)).astype(BF16)


def gelu_tanh(z):
    return jnp.tanh(GELU_C * (z + GELU_A * (z * z * z)))


def gelu_slope(z, t):
    return 0.5 * (1.0 + t) + (0.5 * z) * ((1.0 - t * t) * (GELU_C * (1.0 + (3.0 * GELU_A) * (z * z))))


def block_diag(a, mask):
    return jnp.concatenate([a, a, a, a], axis=0) * mask


def diag_blocks(full, seq, lane_lo):
    left = jnp.where(lane_lo, full[0:seq, 0:128], full[seq:2 * seq, 0:128])
    right = jnp.where(lane_lo, full[2 * seq:3 * seq, 128:256], full[3 * seq:4 * seq, 128:256])
    return jnp.concatenate([left, right], axis=1)


def softmax_t(scores_t, scale):
    s = scores_t * scale
    e = jnp.exp(s - jnp.max(s, axis=0, keepdims=True))
    return e / jnp.sum(e, axis=0, keepdims=True)


def in_chunks(n, body, rows=32):
    def step(i, _):
        body(pl.ds(pl.multiple_of(i * rows, rows), rows))
        return 0

    lax.fori_loop(0, n // rows, step, 0, unroll=2)


def loads(refs, bufs, sems):
    return [pltpu.make_async_copy(r, b, sems.at[k]) for k, (r, b) in enumerate(zip(refs, bufs))]


def at_step(step, *actions):
    @pl.when(pl.program_id(0) == step)
    def _():
        for act in actions:
            act()


def attn_fwd_kernel(layer, seq, scale, x_ref, e_ref, mask_ref, wq_hbm, wk_hbm, wv_hbm, wo_hbm,
                    xc_ref, u_ref, q_ref, k_ref, v_ref, mix_ref, h_ref, m_ref, mt_ref, wq_ref, wk_ref, wv_ref, wo_ref, sems):
    load = loads((wq_hbm, wk_hbm, wv_hbm, wo_hbm), (wq_ref, wk_ref, wv_ref, wo_ref), sems)
    at_step(0, *(c.start for c in load))
    n_rows = x_ref.shape[0]
    blocks = [pl.ds(r * (n_rows // 2), n_rows // 2) for r in range(2)]
    at_step(0, load[0].wait, load[1].wait)
    for k, rows in enumerate(blocks):
        x = (x_ref[rows, :].astype(F32) + e_ref[layer:layer + 1, :].astype(F32)).astype(BF16)
        xc_ref[rows, :] = x
        x_f32 = x.astype(F32)
        u_ref[rows, :] = (x_f32 * rms_scale(x_f32)).astype(BF16)
        for w_ref, o_ref in ((wq_ref, q_ref), (wk_ref, k_ref), (wv_ref, v_ref)):
            if k == 0 and w_ref is wv_ref:
                at_step(0, load[2].wait, load[3].wait)
            o_ref[rows, :] = dot(u_ref[rows, :], w_ref[...], NT).astype(BF16)

    n_groups = x_ref.shape[1] // 256
    lane_lo = lax.broadcasted_iota(jnp.int32, (seq, 128), 1) < 64

    def one_seq(s):
        rows = pl.ds(s * seq, seq)
        cols = [pl.ds(g * 256, 256) for g in range(n_groups)]
        mask = mask_ref[...]
        st = [dot(k_ref[rows, c], block_diag(q_ref[rows, c], mask), NT).astype(BF16).astype(F32) for c in cols]
        pb = [softmax_t(t, scale).astype(BF16) for t in st]
        for c, p in zip(cols, pb):
            mix_ref[rows, c] = diag_blocks(dot(p, v_ref[rows, c], TN), seq, lane_lo).astype(BF16)

    for s in range(x_ref.shape[0] // seq):
        one_seq(s)
    for rows in blocks:
        h = (xc_ref[rows, :].astype(F32) + dot(mix_ref[rows, :], wo_ref[...]).astype(BF16).astype(F32)).astype(BF16)
        h_ref[rows, :] = h
        h_f32 = h.astype(F32)
        m_ref[rows, :] = (h_f32 * rms_scale(h_f32)).astype(BF16)
    mt_ref[...] = m_ref[...].T


def attn_bwd_kernel(seq, scale, dmid_ref, q_ref, k_ref, v_ref, xc_ref, mask_ref, wo_hbm, wq_hbm, wk_hbm, wv_hbm,
                    dq_ref, dk_ref, dv_ref, dprev_ref, dmix_ref, wo_ref, wq_ref, wk_ref, wv_ref, sems):
    load = loads((wo_hbm, wq_hbm, wk_hbm, wv_hbm), (wo_ref, wq_ref, wk_ref, wv_ref), sems)
    at_step(0, *(c.start for c in load), load[0].wait)
    dmix_ref[...] = dot(dmid_ref[...], wo_ref[...], NT).astype(BF16)
    n_groups = xc_ref.shape[1] // 256
    lane_lo = lax.broadcasted_iota(jnp.int32, (seq, 128), 1) < 64

    def one_seq(s, _):
        rows = pl.ds(pl.multiple_of(s * seq, seq), seq)
        cols = [pl.ds(g * 256, 256) for g in range(n_groups)]
        mask = mask_ref[...]
        qbd = [block_diag(q_ref[rows, c], mask) for c in cols]
        dbd = [block_diag(dmix_ref[rows, c], mask) for c in cols]
        st = [dot(k_ref[rows, c], t, NT).astype(BF16).astype(F32) for c, t in zip(cols, qbd)]
        dp = [dot(v_ref[rows, c], t, NT).astype(BF16).astype(F32) for c, t in zip(cols, dbd)]
        p = [softmax_t(t, scale) for t in st]
        for c, a, t in zip(cols, p, dbd):
            dv_ref[rows, c] = dot(a.astype(BF16), t).astype(BF16)
        ds = [((a * (t - jnp.sum(a * t, axis=0, keepdims=True))) * scale).astype(BF16) for a, t in zip(p, dp)]
        for c, a, t in zip(cols, ds, qbd):
            dk_ref[rows, c] = dot(a, t).astype(BF16)
            dq_ref[rows, c] = diag_blocks(dot(a, k_ref[rows, c], TN), seq, lane_lo).astype(BF16)
        return 0

    lax.fori_loop(0, xc_ref.shape[0] // seq, one_seq, 0, unroll=4)
    at_step(0, *(c.wait for c in load[1:]))
    n_rows = xc_ref.shape[0]
    for rows in [pl.ds(r * (n_rows // 2), n_rows // 2) for r in range(2)]:
        du = dot(dq_ref[rows, :], wq_ref[...]) + dot(dk_ref[rows, :], wk_ref[...]) + dot(dv_ref[rows, :], wv_ref[...])
        dx = rms_pull(xc_ref[rows, :], du.astype(BF16))
        dprev_ref[rows, :] = (dmid_ref[rows, :].astype(F32) + dx.astype(F32)).astype(BF16)


def mlp_fwd_kernel(sub, m_ref, wup_ref, wdown_ref, h_hbm, z_ref, g_ref, y_ref, acc_ref, h_ref, sem):
    step = pl.program_id(0)
    load = pltpu.make_async_copy(h_hbm, h_ref, sem)
    at_step(0, load.start)

    @pl.when(step == 0)
    def _():
        acc_ref[...] = jnp.zeros_like(acc_ref)

    for r in range(m_ref.shape[0] // sub):
        rows = pl.ds(r * sub, sub)
        zb = dot(m_ref[rows, :], wup_ref[...]).astype(BF16)
        z_ref[rows, :] = zb
        z = zb.astype(F32)
        g = ((0.5 * z) * (1.0 + gelu_tanh(z))).astype(BF16)
        g_ref[rows, :] = g
        acc_ref[rows, :] += dot(g, wdown_ref[...])

    @pl.when(step == pl.num_programs(0) - 1)
    def _():
        load.wait()

        def finish(rows):
            y = acc_ref[rows, :].astype(BF16)
            y_ref[rows, :] = (h_ref[rows, :].astype(F32) + y.astype(F32)).astype(BF16)

        in_chunks(m_ref.shape[0], finish)


def mlp_last_kernel(sub, m_ref, d_ref, wup_ref, wdown_ref, h_hbm, g_ref, dup_ref, dmid_ref, acc_ref, h_ref, sem):
    step = pl.program_id(0)
    load = pltpu.make_async_copy(h_hbm, h_ref, sem)
    at_step(0, load.start)

    @pl.when(step == 0)
    def _():
        acc_ref[...] = jnp.zeros_like(acc_ref)

    for r in range(d_ref.shape[0] // sub):
        rows = pl.ds(r * sub, sub)
        z = dot(m_ref[rows, :], wup_ref[...]).astype(BF16).astype(F32)
        t = gelu_tanh(z)
        g_ref[rows, :] = ((0.5 * z) * (1.0 + t)).astype(BF16)
        da = dot(d_ref[rows, :], wdown_ref[...], NT).astype(BF16).astype(F32)
        dup_ref[rows, :] = (da * gelu_slope(z, t)).astype(BF16)
        acc_ref[rows, :] += dot(dup_ref[rows, :], wup_ref[...], NT)

    @pl.when(step == pl.num_programs(0) - 1)
    def _():
        load.wait()

        def finish(rows):
            dh = rms_pull(h_ref[rows, :], acc_ref[rows, :].astype(BF16))
            dmid_ref[rows, :] = (d_ref[rows, :].astype(F32) + dh.astype(F32)).astype(BF16)

        in_chunks(d_ref.shape[0], finish)


def params(**kw):
    return pltpu.CompilerParams(dimension_semantics=("arbitrary",), vmem_limit_bytes=VMEM_LIMIT, **kw)


def cost(flops, nbytes, trans=0):
    return pl.CostEstimate(flops=int(flops), bytes_accessed=int(nbytes), transcendentals=int(trans))


def whole(shape):
    return pl.BlockSpec(shape, lambda i: (0,) * len(shape))


def attn_fwd(x, step_emb, layer, wq, wk, wv, wo, mask, seq, scale, tile):
    n, d = x.shape
    row = pl.BlockSpec((tile, d), lambda i: (i, 0))
    return pl.pallas_call(
        functools.partial(attn_fwd_kernel, layer, seq, scale),
        grid=(n // tile,),
        in_specs=[row, whole(step_emb.shape), whole(mask.shape)] + [pl.BlockSpec(memory_space=pl.ANY)] * 4,
        out_specs=[row] * 8 + [pl.BlockSpec((d, tile), lambda i: (0, i))],
        out_shape=[jax.ShapeDtypeStruct((n, d), BF16)] * 8 + [jax.ShapeDtypeStruct((d, n), BF16)],
        scratch_shapes=[pltpu.VMEM(w.shape, BF16) for w in (wq, wk, wv, wo)] + [pltpu.SemaphoreType.DMA((4,))],
        compiler_params=params(),
        cost_estimate=cost(8 * n * d * d, 20 * n * d, n * d),
        name="attn_fwd",
    )(x, step_emb, mask, wq, wk, wv, wo)


def attn_bwd(dmid, q, k, v, xc, wq, wk, wv, wo, mask, seq, scale, tile):
    n, d = xc.shape
    row = pl.BlockSpec((tile, d), lambda i: (i, 0))
    return pl.pallas_call(
        functools.partial(attn_bwd_kernel, seq, scale),
        grid=(n // tile,),
        in_specs=[row] * 5 + [whole(mask.shape)] + [pl.BlockSpec(memory_space=pl.ANY)] * 4,
        out_specs=[row] * 4,
        out_shape=[jax.ShapeDtypeStruct((n, d), BF16)] * 4,
        scratch_shapes=[pltpu.VMEM((tile, d), BF16)] + [pltpu.VMEM(w.shape, BF16) for w in (wo, wq, wk, wv)] + [pltpu.SemaphoreType.DMA((4,))],
        compiler_params=params(),
        cost_estimate=cost(8 * n * d * d, 20 * n * d, n * d),
        name="attn_bwd",
    )(dmid, q, k, v, xc, mask, wo, wq, wk, wv)


def mlp_fwd(m, w_up, w_down, h, tile, sub):
    n, d = m.shape
    f = w_up.shape[1]
    col = pl.BlockSpec((n, tile), lambda i: (0, i))
    return pl.pallas_call(
        functools.partial(mlp_fwd_kernel, sub),
        grid=(f // tile,),
        in_specs=[kept((n, d)), pl.BlockSpec((d, tile), lambda i: (0, i)), pl.BlockSpec((tile, d), lambda i: (i, 0)), pl.BlockSpec(memory_space=pl.ANY)],
        out_specs=[col, col, kept((n, d))],
        out_shape=[jax.ShapeDtypeStruct((n, f), BF16)] * 2 + [jax.ShapeDtypeStruct((n, d), BF16)],
        scratch_shapes=[pltpu.VMEM((n, d), F32), pltpu.VMEM((n, d), BF16), pltpu.SemaphoreType.DMA(())],
        compiler_params=params(),
        cost_estimate=cost(4 * n * d * f, 4 * n * f, n * f),
        name="mlp_fwd",
    )(m, w_up, w_down, h)


def mlp_last(m, d_out, w_up, w_down, h, tile, sub):
    n, d = d_out.shape
    f = w_up.shape[1]
    col = pl.BlockSpec((n, tile), lambda i: (0, i))
    return pl.pallas_call(
        functools.partial(mlp_last_kernel, sub),
        grid=(f // tile,),
        in_specs=[kept((n, d)), kept((n, d)), pl.BlockSpec((d, tile), lambda i: (0, i)), pl.BlockSpec((tile, d), lambda i: (i, 0)),
                  pl.BlockSpec(memory_space=pl.ANY)],
        out_specs=[col, col, kept((n, d))],
        out_shape=[jax.ShapeDtypeStruct((n, f), BF16)] * 2 + [jax.ShapeDtypeStruct((n, d), BF16)],
        scratch_shapes=[pltpu.VMEM((n, d), F32), pltpu.VMEM((n, d), BF16), pltpu.SemaphoreType.DMA(())],
        compiler_params=params(),
        cost_estimate=cost(6 * n * d * f, 4 * n * f, n * f),
        name="mlp_last",
    )(m, d_out, w_up, w_down, h)


def peer_of(me, power):
    return me + power * (1 - 2 * ((me // power) % 2))


def enter_barrier(me):
    barrier = pltpu.get_barrier_semaphore()
    for power in (1, 2, 4, 8):
        pl.semaphore_signal(barrier, inc=1, device_id=(peer_of(me, power),), device_id_type=MESH)
    pl.semaphore_wait(barrier, 4)


def stream_scratch(half, width, slots):
    return [pltpu.VMEM((slots, half // k, width), F32) for k in (1, 2, 4, 8)] + [
        pltpu.SemaphoreType.DMA((4, slots)), pltpu.SemaphoreType.DMA((4, slots))]


def put(ref, value):
    ref[0] = value


def reduce_stage(s, j, shift, half, g_ref, sink, bufs, me):
    h0, h1, h2, h3, send_sem, recv_sem = bufs
    slots = h0.shape[0]
    slot, g = j % slots, g_ref.at[j % g_ref.shape[0]]
    core = me % 2
    powers, bits = [], []
    for k in range(3):
        r = (j + k + shift) % 3
        powers.append(2 + r + r * r)
        bits.append((me // powers[k]) % 2)
    held = (g, h0.at[slot], h1.at[slot], h2.at[slot], h3.at[slot])
    keep = (half * core,) + tuple((half >> (k + 1)) * bits[k] for k in range(3))
    away = (half * (1 - core),) + tuple((half >> (k + 1)) * (1 - bits[k]) for k in range(3))

    def part(ref, start, size):
        return ref.at[pl.ds(pl.multiple_of(start, 8), size)]

    def copy(k):
        peer = peer_of(me, 1) if k == 0 else peer_of(me, powers[k - 1])
        return pltpu.make_async_remote_copy(
            src_ref=part(held[k], away[k], half >> k), dst_ref=held[k + 1], send_sem=send_sem.at[k, slot],
            recv_sem=recv_sem.at[k, slot], device_id=(peer,), device_id_type=MESH)

    if s > 0:
        before = copy(s - 1)
        before.wait_recv()
        before.wait_send()
        own = held[s - 1][pl.ds(pl.multiple_of(keep[s - 1], 8), half >> (s - 1)), :]
        if s == 4:
            sink(j, held[4][...] + own)
        else:
            held[s][...] = held[s][...] + own
    if s < 4:
        copy(s).start()


def reduce_step(i, lags, streams, me):
    for n, *stream in streams:
        for s in (4, 3, 2, 1, 0):
            j = i - lags[s]

            @pl.when((j >= 0) & (j < n))
            def _():
                reduce_stage(s, j, *stream, me)


def mlp_grads_kernel(n, sub, d0_hbm, d1_hbm, m0t_hbm, m1t_hbm, z_ref, g0_ref, g1_ref, dup1_ref, wdown_ref,
                     share_ref, du_ref, gd_ref, gu_ref, d0_ref, d1_ref, m0t_ref, m1t_ref, sems, *bufs):
    me = lax.axis_index('data')
    i = pl.program_id(0)
    load = loads((d0_hbm, d1_hbm, m0t_hbm, m1t_hbm), (d0_ref, d1_ref, m0t_ref, m1t_ref), sems)

    def share_up(j, share):
        piece, width = share_ref.shape[1], share.shape[1]
        for k in range(share.shape[0] // piece):
            share_ref[1, :, k * width:(k + 1) * width] = share[k * piece:(k + 1) * piece, :]

    down = (0, gd_ref.shape[1] // 2, gd_ref, lambda j, share: put(share_ref, share), bufs[:6])
    up = (2, gu_ref.shape[1] // 2, gu_ref, share_up, bufs[6:])

    def exchange(*stages):
        for stream, s, lag in stages:
            j = i - lag

            @pl.when((j >= 0) & (j < n))
            def _():
                reduce_stage(s, j, *stream, me)

    @pl.when(i == 0)
    def _():
        for c in load:
            c.start()
        enter_barrier(me)
        for c in load[:2]:
            c.wait()

    @pl.when(i < n)
    def _():
        gd_ref[i % 2] = dot(g0_ref[...], d0_ref[...], TN) + dot(g1_ref[...], d1_ref[...], TN)

    exchange((up, 1, 1), (down, 4, 6), (down, 3, 5), (down, 2, 3), (down, 0, 0))
    at_step(0, *(c.wait for c in load[2:]))

    @pl.when(i < n)
    def _():
        for r in range(d0_ref.shape[0] // sub):
            rows = pl.ds(r * sub, sub)
            da = dot(d0_ref[rows, :], wdown_ref[...], NT).astype(BF16).astype(F32)
            z = z_ref[rows, :].astype(F32)
            du_ref[rows, :] = (da * gelu_slope(z, gelu_tanh(z))).astype(BF16)
        gu_ref[i % 2] = dot(m0t_ref[...], du_ref[...]) + dot(m1t_ref[...], dup1_ref[...])

    exchange((up, 4, 6), (up, 3, 5), (up, 2, 3), (down, 1, 0), (up, 0, 0))


def mlp_back_kernel(sub, du_ref, wup_ref, d_hbm, h_hbm, dmid_ref, acc_ref, d_ref, h_ref, sems):
    step = pl.program_id(0)
    load = loads((d_hbm, h_hbm), (d_ref, h_ref), sems)
    at_step(0, *(c.start for c in load))

    @pl.when(step == 0)
    def _():
        acc_ref[...] = jnp.zeros_like(acc_ref)

    for r in range(du_ref.shape[0] // sub):
        rows = pl.ds(r * sub, sub)
        acc_ref[rows, :] += dot(du_ref[rows, :], wup_ref[...], NT)

    @pl.when(step == pl.num_programs(0) - 1)
    def _():
        for c in load:
            c.wait()

        def finish(rows):
            dh = rms_pull(h_ref[rows, :], acc_ref[rows, :].astype(BF16))
            dmid_ref[rows, :] = (d_ref[rows, :].astype(F32) + dh.astype(F32)).astype(BF16)

        in_chunks(d_ref.shape[0], finish)


def attn_grads_kernel(n, lags, *refs):
    xs, (u0, u1, m0, m1), out_ref, g_ref, bufs = refs[:8], refs[8:12], refs[12], refs[13], refs[14:]
    me = lax.axis_index('data')
    i = pl.program_id(0)

    @pl.when(i == 0)
    def _():
        enter_barrier(me)

    per = n // 4
    for w in range(4):
        @pl.when((i >= w * per) & (i < (w + 1) * per))
        def _():
            y0, y1 = (u0, u1) if w < 3 else (m0, m1)
            g_ref[i % 4] = dot(xs[2 * w][...], y0[...], TN) + dot(xs[2 * w + 1][...], y1[...], TN)

    reduce_step(i, lags, ((n, 0, g_ref.shape[1] // 2, g_ref, lambda j, share: put(out_ref, share), bufs),), me)


MLP_LAG, MLP_SLOTS = 6, 8
ATTN_LAGS, ATTN_SLOTS = (0, 1, 4, 6, 8), 12


def kept(shape):
    return pl.BlockSpec(shape, lambda i: (0,) * len(shape), pipeline_mode=pl.Buffered(1))


def mlp_grads(ds, mts, z, gs, dup1, w_down, tile, sub):
    rows, d = ds[0].shape
    n = w_down.shape[0] // tile
    at = lambda i: jnp.minimum(i, n - 1)
    col = pl.BlockSpec((rows, tile), lambda i: (0, at(i)))
    anywhere = pl.BlockSpec(memory_space=pl.ANY)
    piece = tile // 16
    return pl.pallas_call(
        functools.partial(mlp_grads_kernel, n, sub),
        grid=(n + MLP_LAG,),
        in_specs=[anywhere] * 4 + [col] * 4 + [pl.BlockSpec((tile, d), lambda i: (at(i), 0))],
        out_specs=[pl.BlockSpec((2, piece, d), lambda i: (jnp.maximum(i - MLP_LAG, 0), 0, 0)), col],
        out_shape=[jax.ShapeDtypeStruct((2 * n, piece, d), F32), jax.ShapeDtypeStruct((rows, n * tile), BF16)],
        scratch_shapes=[pltpu.VMEM((2, tile, d), F32), pltpu.VMEM((2, d, tile), F32)] + [pltpu.VMEM(a.shape, BF16) for a in (*ds, *mts)] + [
            pltpu.SemaphoreType.DMA((4,))] + stream_scratch(tile // 2, d, MLP_SLOTS) + stream_scratch(d // 2, tile, MLP_SLOTS),
        compiler_params=pltpu.CompilerParams(dimension_semantics=("arbitrary",), collective_id=0, has_side_effects=True,
                                             vmem_limit_bytes=VMEM_LIMIT),
        cost_estimate=cost(10 * rows * d * n * tile, 10 * rows * n * tile),
        name="mlp_grads",
    )(*ds, *mts, z, *gs, dup1, w_down)


def mlp_back(du, w_up, d_out, h, tile, sub):
    n, d = d_out.shape
    f = w_up.shape[1]
    anywhere = pl.BlockSpec(memory_space=pl.ANY)
    return pl.pallas_call(
        functools.partial(mlp_back_kernel, sub),
        grid=(f // tile,),
        in_specs=[pl.BlockSpec((n, tile), lambda i: (0, i)), pl.BlockSpec((d, tile), lambda i: (0, i)), anywhere, anywhere],
        out_specs=kept((n, d)),
        out_shape=jax.ShapeDtypeStruct((n, d), BF16),
        scratch_shapes=[pltpu.VMEM((n, d), F32), pltpu.VMEM((n, d), BF16), pltpu.VMEM((n, d), BF16), pltpu.SemaphoreType.DMA((2,))],
        compiler_params=params(),
        cost_estimate=cost(2 * n * d * f, 2 * n * f),
        name="mlp_back",
    )(du, w_up, d_out, h)


def attn_grads(xs, ys, tile):
    rows, d = ys[0].shape
    per = d // tile
    n = 4 * per
    cols = [pl.BlockSpec((rows, tile), lambda i, w=w: (0, jnp.clip(i - w * per, 0, per - 1))) for w in range(4) for _ in range(2)]
    return pl.pallas_call(
        functools.partial(attn_grads_kernel, n, ATTN_LAGS),
        grid=(n + ATTN_LAGS[4],),
        in_specs=cols + [kept((rows, d))] * 4,
        out_specs=pl.BlockSpec((1, tile // 16, d), lambda i: (jnp.maximum(i - ATTN_LAGS[4], 0), 0, 0)),
        out_shape=jax.ShapeDtypeStruct((n, tile // 16, d), F32),
        scratch_shapes=[pltpu.VMEM((4, tile, d), F32)] + stream_scratch(tile // 2, d, ATTN_SLOTS),
        compiler_params=pltpu.CompilerParams(dimension_semantics=("arbitrary",), collective_id=1, has_side_effects=True,
                                             vmem_limit_bytes=VMEM_LIMIT),
        cost_estimate=cost(16 * rows * d * d, 24 * rows * d),
        name="attn_grads",
    )(*[x for pair in xs for x in pair], *ys)


def put_in_place(j, shift, in_ref, out_ref, bands):
    half = out_ref.shape[0] // 2
    piece, width = in_ref.shape[1], out_ref.shape[1]

    def variant(v):
        for dev in range(16):
            bits = [(dev >> (1 + (v + k) % 3)) & 1 for k in range(3)]
            at = half * (dev & 1) + sum((half >> (k + 1)) * bits[k] for k in range(3))
            for k in range(bands):
                out_ref[at + k * piece:at + (k + 1) * piece, :] = in_ref[dev, :, k * width:(k + 1) * width]

    if isinstance(j, int):
        variant((j + shift) % 3)
    else:
        for v in range(3):
            pl.when((j + shift) % 3 == v)(functools.partial(variant, v))


def place_mlp_kernel(group, in_ref, down_ref, up_ref):
    high, width = down_ref.shape[0] // group, up_ref.shape[1] // group
    for c in range(group):
        j = pl.program_id(0) * group + c
        put_in_place(j, 0, in_ref.at[:, 2 * c], down_ref.at[pl.ds(c * high, high)], 1)
        put_in_place(j, 2, in_ref.at[:, 2 * c + 1], up_ref.at[:, pl.ds(c * width, width)], up_ref.shape[0] // (16 * in_ref.shape[2]))


def place_mlp(shares, n, tile, group):
    _, _, piece, d = shares.shape
    return pl.pallas_call(
        functools.partial(place_mlp_kernel, group),
        grid=(n // group,),
        in_specs=[pl.BlockSpec((16, 2 * group, piece, d), lambda i: (0, i, 0, 0))],
        out_specs=[pl.BlockSpec((group * tile, d), lambda i: (i, 0)), pl.BlockSpec((d, group * tile), lambda i: (0, i))],
        out_shape=[jax.ShapeDtypeStruct((n * tile, d), F32), jax.ShapeDtypeStruct((d, n * tile), F32)],
        compiler_params=params(),
        cost_estimate=cost(shares.size // 2, 8 * shares.size),
        name="place_mlp",
    )(shares)


def place_rows_kernel(first, turn, per, in_ref, *refs):
    outs, (in_buf, out_buf, in_sem, out_sem) = refs[:-4], refs[-4:]
    depth, high = in_buf.shape[0], out_buf.shape[1]
    total = per * len(outs)

    def fetch(t):
        return pltpu.make_async_copy(in_ref.at[:, first + t], in_buf.at[t % depth], in_sem.at[t % depth])

    def store(t):
        at = t % per * high
        return pltpu.make_async_copy(out_buf.at[t % depth], outs[t // per].at[pl.ds(at, high)], out_sem.at[t % depth])

    for t in range(min(depth, total)):
        fetch(t).start()
    for t in range(total):
        fetch(t).wait()
        if t >= depth:
            store(t - depth).wait()
        put_in_place(turn + t, 0, in_buf.at[t % depth], out_buf.at[t % depth], 1)
        store(t).start()
        if t + depth < total:
            fetch(t + depth).start()
    for t in range(max(total - depth, 0), total):
        store(t).wait()


def place_rows(shares, first, turn, per, n_out, depth):
    _, _, piece, d = shares.shape
    anywhere = pl.BlockSpec(memory_space=pl.ANY)
    return pl.pallas_call(
        functools.partial(place_rows_kernel, first, turn, per),
        in_specs=[anywhere],
        out_specs=[anywhere] * n_out,
        out_shape=[jax.ShapeDtypeStruct((per * 16 * piece, d), F32)] * n_out,
        scratch_shapes=[pltpu.VMEM((depth, 16, piece, d), F32), pltpu.VMEM((depth, 16 * piece, d), F32),
                        pltpu.SemaphoreType.DMA((depth,)), pltpu.SemaphoreType.DMA((depth,))],
        compiler_params=pltpu.CompilerParams(vmem_limit_bytes=VMEM_LIMIT),
        cost_estimate=cost(per * n_out * piece * d * 16, per * n_out * piece * d * 128),
        name="place_rows",
    )(shares)


def solution(mesh):
    batch_spec = P('data', None, None)

    def per_device(x_loc, g_loc, step_emb, w_q, w_k, w_v, w_o, w_up, w_down):
        d, n_heads, head = w_q.shape
        scale = head ** -0.5
        n_seq, seq, _ = x_loc.shape
        n = n_seq * seq
        wq, wk, wv = (w.transpose(1, 2, 0).reshape(n_heads * head, d) for w in (w_q, w_k, w_v))
        wo = w_o.reshape(n_heads * head, d)
        mask = np.kron(np.eye(4), np.ones((64, 64))).astype(BF16)

        def attn_back(dmid, *acts):
            return attn_bwd(dmid, *acts, wq, wk, wv, wo, mask, seq, scale, 512)

        x0, u0, q0, k0, v0, mix0, h0, m0, mt0 = attn_fwd(x_loc.reshape(n, d), step_emb, 0, wq, wk, wv, wo, mask, seq, scale, 512)
        z0, g0, x = mlp_fwd(m0, w_up, w_down, h0, 1024, 512)
        x1, u1, q1, k1, v1, mix1, h1, m1, mt1 = attn_fwd(x, step_emb, 1, wq, wk, wv, wo, mask, seq, scale, 512)
        do1 = g_loc.reshape(n, d)
        g1, dup1, dmid1 = mlp_last(m1, do1, w_up, w_down, h1, 1024, 512)
        dq1, dk1, dv1, do0 = attn_back(dmid1, q1, k1, v1, x1)
        s_mlp, dup0 = mlp_grads((do0, do1), (mt0, mt1), z0, (g0, g1), dup1, w_down, 256, 256)
        n_tiles, n_blocks = w_up.shape[1] // 256, d // 256
        a_mlp = lax.all_gather(s_mlp, 'data')
        dmid0 = mlp_back(dup0, w_up, do0, h0, 1024, 512)
        dq0, dk0, dv0, d_out = attn_back(dmid0, q0, k0, v0, x0)
        s_attn = attn_grads([(dq0, dq1), (dk0, dk1), (dv0, dv1), (mix0, mix1)], (u0, u1, dmid0, dmid1), 256)
        a_attn = lax.all_gather(s_attn, 'data')
        g_down, g_up = place_mlp(a_mlp, n_tiles, 256, 2)
        g_q, g_k, g_v, g_o = place_rows(a_attn, 0, 0, n_blocks, 4, 6)
        heads = lambda a: a.reshape(n_heads, head, d).transpose(2, 0, 1)
        return heads(g_q), heads(g_k), heads(g_v), g_o.reshape(w_o.shape), g_up, g_down, d_out.reshape(x_loc.shape)

    return jax.shard_map(per_device, mesh=mesh, in_specs=(batch_spec, batch_spec, P(), P(), P(), P(), P(), P(), P()), out_specs=(P(), P(), P(), P(), P(), P(), batch_spec), check_vma=False)
```
